32 devices in a mesh: pz: 4 (over z), py: 8 (over y, x, core).
Axes of the slice: x: 2, y: 2, z: 4, core: 2. Of those that a mesh axis runs over, the one named last changes fastest.
Arguments:
- populations: float32 [19, 256, 64, 256], P(None, None, 'py', 'pz')
- relax_time: float32 [], replicated
- body_force: float32 [3], replicated
Outputs:
- output 1: float32 [19, 256, 64, 256], P(None, None, 'py', 'pz')
- output 2: float32 [256, 64, 256], P(None, 'py', 'pz')
- output 3: float32 [3, 256, 64, 256], P(None, None, 'py', 'pz')
All inputs are finite; a program needn't handle non-finite values.
Results may differ from the reference program's by a relative error of at most 0.001.
Values sent between devices are 32-bit elements.
A program may use at most 1 GiB of HBM per device.

```python
import jax
import jax.numpy as jnp

NX = 256
NY = 64
NZ = 256
SHARD_Y = 8
SHARD_Z = 64
STEPS = 4

VELOCITIES = ((0, 0, 0), (1, 0, 0), (-1, 0, 0), (0, 1, 0), (0, -1, 0), (0, 0, 1), (0, 0, -1), (1, 1, 0), (-1, -1, 0), (1, -1, 0), (-1, 1, 0), (1, 0, 1), (-1, 0, -1), (1, 0, -1), (-1, 0, 1), (0, 1, 1), (0, -1, -1), (0, 1, -1), (0, -1, 1))
WEIGHTS = (1.0 / 3.0,) + (1.0 / 18.0,) * 6 + (1.0 / 36.0,) * 12


def moments(populations, relax_time, body_force):
    density = jnp.sum(populations, axis=0)
    velocity = []
    for axis_id in range(3):
        plus_part = sum(populations[pop_id] for pop_id in range(19) if VELOCITIES[pop_id][axis_id] == 1)
        minus_part = sum(populations[pop_id] for pop_id in range(19) if VELOCITIES[pop_id][axis_id] == -1)
        velocity.append((plus_part - minus_part + body_force[axis_id] * relax_time) / density)
    return density, velocity


def equilibrium(density, velocity):
    speed_sq = velocity[0] * velocity[0] + velocity[1] * velocity[1] + velocity[2] * velocity[2]
    base_term = 1.0 - 1.5 * speed_sq
    result = []
    for pop_id in range(19):
        projection = sum(velocity[axis_id] * shift for axis_id, shift in enumerate(VELOCITIES[pop_id]) if shift != 0)
        result.append(WEIGHTS[pop_id] * density * (base_term + 3.0 * projection + 4.5 * projection * projection))
    return result


def collide(populations, relax_time, body_force):
    density, velocity = moments(populations, relax_time, body_force)
    feq_list = equilibrium(density, velocity)
    relax_rate = 1.0 / relax_time
    return [populations[pop_id] - (populations[pop_id] - feq_list[pop_id]) * relax_rate for pop_id in range(19)]


def propagate(collided):
    return jnp.stack([jnp.roll(collided[pop_id], VELOCITIES[pop_id], axis=(0, 1, 2)) for pop_id in range(19)])


def setup_inputs(seed: int = 0) -> dict:
    keys = jax.random.split(jax.random.key(seed), 7)
    grid_x = jnp.arange(NX, dtype=jnp.float32)[:, None, None]
    grid_y = jnp.arange(NY, dtype=jnp.float32)[None, :, None]
    grid_z = jnp.arange(NZ, dtype=jnp.float32)[None, None, :]
    phase = 2.0 * jnp.pi * jax.random.uniform(keys[0], (), jnp.float32)
    shear = 0.05 * jnp.sin(2.0 * jnp.pi * grid_z / NZ + phase)
    width_yz = max(2.0, 0.5 * min(SHARD_Y, SHARD_Z))
    width_x = max(2.0, NX / 8.0)
    dist_sq = ((grid_x - NX / 2.0) / width_x) ** 2 + ((grid_y - SHARD_Y + 0.5) / width_yz) ** 2 + ((grid_z - SHARD_Z + 0.5) / width_yz) ** 2
    pulse_amp = 0.1 + 0.1 * jax.random.uniform(keys[1], (), jnp.float32)
    density = 1.0 + pulse_amp * jnp.exp(-0.5 * dist_sq) + 0.02 * jax.random.normal(keys[2], (NX, NY, NZ), jnp.float32)
    noise_u = 0.01 * jax.random.normal(keys[3], (3, NX, NY, NZ), jnp.float32)
    velocity = [noise_u[0] + shear, noise_u[1], noise_u[2]]
    jitter = 1.0 + 0.1 * jax.random.normal(keys[4], (19, NX, NY, NZ), jnp.float32)
    populations = jnp.stack(equilibrium(density, velocity)) * jitter
    relax_time = 0.6 + 0.2 * jax.random.uniform(keys[5], (), jnp.float32)
    body_force = 0.004 * jax.random.normal(keys[6], (3,), jnp.float32)
    return {"populations": populations, "relax_time": relax_time, "body_force": body_force}


def reference(populations, relax_time, body_force):
    state = populations
    for step_id in range(STEPS):
        state = propagate(collide(state, relax_time, body_force))
    density, velocity = moments(state, relax_time, body_force)
    return state, density, jnp.stack(velocity)
```

```python
import functools

import jax
import jax.numpy as jnp
from jax import lax
from jax.experimental import pallas as pl
from jax.experimental.pallas import tpu as pltpu
from jax.sharding import PartitionSpec as P

STEPS = 4
VELOCITIES = ((0, 0, 0), (1, 0, 0), (-1, 0, 0), (0, 1, 0), (0, -1, 0), (0, 0, 1), (0, 0, -1), (1, 1, 0), (-1, -1, 0), (1, -1, 0), (-1, 1, 0), (1, 0, 1), (-1, 0, -1), (1, 0, -1), (-1, 0, 1), (0, 1, 1), (0, -1, -1), (0, 1, -1), (0, -1, 1))
ORDER = (17, 3, 7, 10, 15, 5, 11, 14, 18, 4, 8, 9, 16, 6, 12, 13, 0, 1, 2)
SLOT = {pop_id: slot for slot, pop_id in enumerate(ORDER)}
MESH = pl.DeviceIdType.MESH
LANES = 128
ROWS = 8
COPIES = 16


def moment_sums(load):
    rest = load(0)
    total = rest
    diff = {}
    for plus in range(1, 19, 2):
        upper, lower = load(plus), load(plus + 1)
        total = total + (upper + lower)
        diff[plus] = upper - lower
    mom_x = (diff[1] + diff[7]) + (diff[9] + (diff[11] + diff[13]))
    mom_y = (diff[3] + diff[7]) - (diff[9] - (diff[15] + diff[17]))
    mom_z = (diff[5] + diff[11]) - (diff[13] - (diff[15] - diff[17]))
    return total, (mom_x, mom_y, mom_z)


def tile_terms(load, force, rate36):
    density, momentum = moment_sums(load)
    inverse = 1.0 / density
    half = [(momentum[axis] + force[axis]) * inverse * 1.5 for axis in range(3)]
    square = half[0] * half[0] + half[1] * half[1] + half[2] * half[2]
    scale = density * rate36
    even = scale * (1.0 - square * (2.0 / 3.0))
    twice = scale + scale
    odd = [twice * half[axis] for axis in range(3)]
    return even, odd, half


def relaxed(load, terms, keep, plus):
    even, odd, half = terms
    axes = [(axis, shift) for axis, shift in enumerate(VELOCITIES[plus]) if shift != 0]
    if len(axes) == 1:
        axis = axes[0][0]
        odd_part = odd[axis] + odd[axis]
        even_part = (even + even) + odd_part * half[axis]
    else:
        (first, _), (second, sign) = axes
        if sign > 0:
            odd_part = odd[first] + odd[second]
            projection = half[first] + half[second]
        else:
            odd_part = odd[first] - odd[second]
            projection = half[first] - half[second]
        even_part = even + odd_part * projection
    return load(plus) * keep + (even_part + odd_part), load(plus + 1) * keep + (even_part - odd_part)


def rolled(halves, shift, lane):
    if shift == 0:
        return halves
    moved = [pltpu.roll(part, shift % LANES, 1) for part in halves]
    edge = lane == (0 if shift > 0 else LANES - 1)
    return [jnp.where(edge, moved[1], moved[0]), jnp.where(edge, moved[0], moved[1])]


def step_kernel(size_y, size_z, ny, nz, tau_ref, force_ref, field_ref, out_ref, stage, other, load_sem, send_sem, recv_sem):
    me_y, me_z = lax.axis_index("py"), lax.axis_index("pz")
    up_y, down_y = lax.rem(me_y + 1, size_y), lax.rem(me_y + size_y - 1, size_y)
    up_z, down_z = lax.rem(me_z + 1, size_z), lax.rem(me_z + size_z - 1, size_z)

    def device(dev_y, dev_z):
        return {"py": dev_y, "pz": dev_z}

    barrier = pltpu.get_barrier_semaphore()
    neighbours = [device(dy, dz) for dy in (down_y, me_y, up_y) for dz in (down_z, me_z, up_z)]
    del neighbours[4]
    for neighbour in neighbours:
        pl.semaphore_signal(barrier, inc=1, device_id=neighbour, device_id_type=MESH)

    plane_order = [0, ny - 1] + list(range(1, ny - 1))
    loads = {y: pltpu.make_async_copy(field_ref.at[:, y], stage.at[:, y], load_sem.at[y]) for y in plane_order}
    for y in plane_order:
        loads[y].start()

    tau = jnp.full((ROWS, LANES), tau_ref[0], jnp.float32)
    rate = 1.0 / tau
    keep = 1.0 - rate
    rate36 = rate * (1.0 / 36.0)
    force = [tau * force_ref[axis] for axis in range(3)]
    lane = lax.broadcasted_iota(jnp.int32, (ROWS, LANES), 1)
    first_row, last_row = ROWS, ROWS + nz - 1
    buffers = (other, out_ref)
    tiles = nz // ROWS

    def collide_tile(step, y, tile):
        row = pl.multiple_of(tile * ROWS, ROWS)
        target = buffers[step % 2]
        source = buffers[(step + 1) % 2]

        def load(half, pop_id):
            if step == 0:
                return stage[pop_id, y, pl.ds(row, ROWS), pl.ds(half * LANES, LANES)]
            return source[SLOT[pop_id], y + 1 - VELOCITIES[pop_id][1], half, pl.ds(row + ROWS, ROWS), :]

        def store(pop_id, halves):
            shift_x, _, shift_z = VELOCITIES[pop_id]
            halves = rolled(halves, shift_x, lane)
            for half in range(2):
                target[SLOT[pop_id], y + 1, half, pl.ds(row + (ROWS + shift_z), ROWS), :] = halves[half]

        loaders = [functools.partial(load, half) for half in range(2)]
        terms = [tile_terms(loaders[half], force, rate36) for half in range(2)]
        store(0, [loaders[half](0) * keep + terms[half][0] * 12.0 for half in range(2)])
        for plus in range(1, 19, 2):
            pairs = [relaxed(loaders[half], terms[half], keep, plus) for half in range(2)]
            store(plus, [pair[0] for pair in pairs])
            store(plus + 1, [pair[1] for pair in pairs])

    def copies(step):
        state = buffers[step % 2]
        parity = step % 2
        result = []

        def add(source, target, dev_y, dev_z):
            number = len(result)
            result.append(pltpu.make_async_remote_copy(
                src_ref=source, dst_ref=target, send_sem=send_sem.at[parity, number], recv_sem=recv_sem.at[parity, number],
                device_id=device(dev_y, dev_z), device_id_type=MESH))

        inner = pl.ds(first_row, nz)
        without_first, without_last = pl.ds(first_row + 1, nz - 1), pl.ds(first_row, nz - 1)
        for slots, rows in ((pl.ds(1, 3), inner), (pl.ds(4, 1), without_first), (pl.ds(0, 1), without_last)):
            add(state.at[slots, ny, :, rows, :], state.at[slots, 0, :, rows, :], up_y, me_z)
        for slots, rows in ((pl.ds(9, 3), inner), (pl.ds(8, 1), without_first), (pl.ds(12, 1), without_last)):
            add(state.at[slots, 1, :, rows, :], state.at[slots, ny + 1, :, rows, :], down_y, me_z)
        all_planes, lower_planes, upper_planes = pl.ds(1, ny), pl.ds(1, ny - 1), pl.ds(2, ny - 1)
        out_up, out_down = pl.ds(last_row + 1, 1), pl.ds(first_row - 1, 1)
        in_up, in_down = pl.ds(first_row, 1), pl.ds(last_row, 1)
        for slots, planes in ((pl.ds(5, 3), all_planes), (pl.ds(4, 1), lower_planes), (pl.ds(8, 1), upper_planes)):
            add(state.at[slots, planes, :, out_up, :], state.at[slots, planes, :, in_up, :], me_y, up_z)
        for slots, planes in ((pl.ds(13, 3), all_planes), (pl.ds(0, 1), lower_planes), (pl.ds(12, 1), upper_planes)):
            add(state.at[slots, planes, :, out_down, :], state.at[slots, planes, :, in_down, :], me_y, down_z)
        add(state.at[4, ny, :, out_up, :], state.at[4, 0, :, in_up, :], up_y, up_z)
        add(state.at[0, ny, :, out_down, :], state.at[0, 0, :, in_down, :], up_y, down_z)
        add(state.at[8, 1, :, out_up, :], state.at[8, ny + 1, :, in_up, :], down_y, up_z)
        add(state.at[12, 1, :, out_down, :], state.at[12, ny + 1, :, in_down, :], down_y, down_z)
        return result

    def over(count, body):
        def run(index, carry):
            body(index)
            return carry
        lax.fori_loop(0, count, run, 0)

    started = [copies(step) for step in range(STEPS)]
    for step in range(STEPS):
        if step == 0:
            loads[0].wait()
            loads[ny - 1].wait()
        else:
            for copy in started[step - 1]:
                copy.wait_recv()
        if step >= 2:
            for copy in started[step - 2]:
                copy.wait_send()
        over(2 * tiles, lambda index: collide_tile(step, (index // tiles) * (ny - 1), index % tiles))
        if step == 0:
            pl.semaphore_wait(barrier, len(neighbours))
        for copy in started[step][:6]:
            copy.start()
        if step == 0:
            for y in range(1, ny - 1):
                loads[y].wait()
        over(2 * (ny - 2), lambda index: collide_tile(step, 1 + index // 2, (index % 2) * (tiles - 1)))
        for copy in started[step][6:]:
            copy.start()
        over((ny - 2) * (tiles - 2), lambda index: collide_tile(step, 1 + index // (tiles - 2), 1 + index % (tiles - 2)))
    for copy in started[STEPS - 1]:
        copy.wait_recv()
    for step in (STEPS - 2, STEPS - 1):
        for copy in started[step]:
            copy.wait_send()


def output_kernel(ny, nz, tau_ref, force_ref, state, field_ref, density_ref, velocity_ref, moments, field_sem, moment_sem):
    field_copies = []
    for pop_id in range(19):
        shift_y = VELOCITIES[pop_id][1]
        for half in range(2):
            field_copies.append(pltpu.make_async_copy(
                state.at[SLOT[pop_id], pl.ds(1 - shift_y, ny), half, pl.ds(ROWS, nz), :],
                field_ref.at[pop_id, :, :, pl.ds(half * LANES, LANES)], field_sem.at[2 * pop_id + half]))
    for copy in field_copies:
        copy.start()
    tau = jnp.full((ROWS, LANES), tau_ref[0], jnp.float32)
    force = [tau * force_ref[axis] for axis in range(3)]
    tiles = nz // ROWS
    moment_copies = []
    for y in range(ny):
        def tile_moments(tile, carry):
            row = pl.multiple_of(tile * ROWS, ROWS)
            for half in range(2):
                def load(pop_id):
                    return state[SLOT[pop_id], y + 1 - VELOCITIES[pop_id][1], half, pl.ds(row + ROWS, ROWS), :]
                density, momentum = moment_sums(load)
                inverse = 1.0 / density
                place = (y, pl.ds(row, ROWS), pl.ds(half * LANES, LANES))
                moments[(0, *place)] = density
                for axis in range(3):
                    moments[(1 + axis, *place)] = (momentum[axis] + force[axis]) * inverse
            return carry
        lax.fori_loop(0, tiles, tile_moments, 0)
        moment_copies.append(pltpu.make_async_copy(moments.at[0, y], density_ref.at[y], moment_sem.at[0, y]))
        moment_copies.append(pltpu.make_async_copy(moments.at[pl.ds(1, 3), y], velocity_ref.at[:, y], moment_sem.at[1, y]))
        moment_copies[-2].start()
        moment_copies[-1].start()
    for copy in field_copies + moment_copies:
        copy.wait()


def solution(mesh):
    size_y = mesh.shape["py"]
    size_z = mesh.shape["pz"]
    field_spec = P(None, None, "py", "pz")

    def local_steps(populations, relax_time, body_force):
        field = jnp.transpose(populations, (0, 2, 3, 1))
        _, ny, nz, nx = field.shape
        tau = jnp.reshape(relax_time, (1,))
        state_shape = (19, ny + 2, 2, nz + 2 * ROWS, LANES)
        smem = pl.BlockSpec(memory_space=pltpu.SMEM)
        vmem = pl.BlockSpec(memory_space=pltpu.VMEM)
        anywhere = pl.BlockSpec(memory_space=pl.ANY)
        state = pl.pallas_call(
            functools.partial(step_kernel, size_y, size_z, ny, nz),
            name="lattice_steps",
            out_shape=pltpu.VMEM(state_shape, jnp.float32),
            in_specs=[smem, smem, anywhere],
            out_specs=vmem,
            scratch_shapes=[
                pltpu.VMEM((19, ny, nz, nx), jnp.float32),
                pltpu.VMEM(state_shape, jnp.float32),
                pltpu.SemaphoreType.DMA((ny,)),
                pltpu.SemaphoreType.DMA((2, COPIES)),
                pltpu.SemaphoreType.DMA((2, COPIES)),
            ],
            compiler_params=pltpu.CompilerParams(collective_id=0, has_side_effects=True, vmem_limit_bytes=44 * 2**20),
        )(tau, body_force, field)
        final, density, velocity = pl.pallas_call(
            functools.partial(output_kernel, ny, nz),
            name="lattice_output",
            out_shape=(
                jax.ShapeDtypeStruct((19, ny, nz, nx), jnp.float32),
                jax.ShapeDtypeStruct((ny, nz, nx), jnp.float32),
                jax.ShapeDtypeStruct((3, ny, nz, nx), jnp.float32),
            ),
            in_specs=[smem, smem, vmem],
            out_specs=(anywhere, anywhere, anywhere),
            scratch_shapes=[
                pltpu.VMEM((4, ny, nz, nx), jnp.float32),
                pltpu.SemaphoreType.DMA((38,)),
                pltpu.SemaphoreType.DMA((2, ny)),
            ],
            compiler_params=pltpu.CompilerParams(vmem_limit_bytes=24 * 2**20),
        )(tau, body_force, state)
        return jnp.transpose(final, (0, 3, 1, 2)), jnp.transpose(density, (2, 0, 1)), jnp.transpose(velocity, (0, 3, 1, 2))

    return jax.shard_map(local_steps, mesh=mesh, in_specs=(field_spec, P(), P()), out_specs=(field_spec, P(None, "py", "pz"), field_spec), check_vma=False)
```

```python
import functools

import jax
import jax.numpy as jnp
from jax import lax
from jax.experimental import pallas as pl
from jax.experimental.pallas import tpu as pltpu
from jax.sharding import PartitionSpec as P

STEPS = 4
VELOCITIES = ((0, 0, 0), (1, 0, 0), (-1, 0, 0), (0, 1, 0), (0, -1, 0), (0, 0, 1), (0, 0, -1), (1, 1, 0), (-1, -1, 0), (1, -1, 0), (-1, 1, 0), (1, 0, 1), (-1, 0, -1), (1, 0, -1), (-1, 0, 1), (0, 1, 1), (0, -1, -1), (0, 1, -1), (0, -1, 1))
ORDER = (17, 3, 7, 10, 15, 5, 11, 14, 18, 4, 8, 9, 16, 6, 12, 13, 0, 1, 2)
SLOT = {pop_id: slot for slot, pop_id in enumerate(ORDER)}
MESH = pl.DeviceIdType.MESH
LANES = 128
ROWS = 8
EDGE_COPIES = 7


def moment_sums(load):
    rest = load(0)
    total = rest
    diff = {}
    for plus in range(1, 19, 2):
        upper, lower = load(plus), load(plus + 1)
        total = total + (upper + lower)
        diff[plus] = upper - lower
    mom_x = (diff[1] + diff[7]) + (diff[9] + (diff[11] + diff[13]))
    mom_y = (diff[3] + diff[7]) - (diff[9] - (diff[15] + diff[17]))
    mom_z = (diff[5] + diff[11]) - (diff[13] - (diff[15] - diff[17]))
    return total, (mom_x, mom_y, mom_z)


def tile_terms(load, force, rate36):
    density, momentum = moment_sums(load)
    inverse = 1.0 / density
    half = [(momentum[axis] + force[axis]) * inverse * 1.5 for axis in range(3)]
    square = half[0] * half[0] + half[1] * half[1] + half[2] * half[2]
    scale = density * rate36
    even = scale * (1.0 - square * (2.0 / 3.0))
    twice = scale + scale
    odd = [twice * half[axis] for axis in range(3)]
    return even, odd, half


def relaxed(load, terms, keep, plus):
    even, odd, half = terms
    axes = [(axis, shift) for axis, shift in enumerate(VELOCITIES[plus]) if shift != 0]
    if len(axes) == 1:
        axis = axes[0][0]
        odd_part = odd[axis] + odd[axis]
        even_part = (even + even) + odd_part * half[axis]
    else:
        (first, _), (second, sign) = axes
        if sign > 0:
            odd_part = odd[first] + odd[second]
            projection = half[first] + half[second]
        else:
            odd_part = odd[first] - odd[second]
            projection = half[first] - half[second]
        even_part = even + odd_part * projection
    return load(plus) * keep + (even_part + odd_part), load(plus + 1) * keep + (even_part - odd_part)


def rolled(halves, shift, lane):
    if shift == 0:
        return halves
    moved = [pltpu.roll(part, shift % LANES, 1) for part in halves]
    edge = lane == (0 if shift > 0 else LANES - 1)
    return [jnp.where(edge, moved[1], moved[0]), jnp.where(edge, moved[0], moved[1])]


def step_kernel(size_y, size_z, ny, nz, tau_ref, force_ref, field_ref, out_ref, stage, other, load_sem, face_send, face_recv, edge_send, edge_recv):
    me_y, me_z = lax.axis_index("py"), lax.axis_index("pz")
    up_y, down_y = lax.rem(me_y + 1, size_y), lax.rem(me_y + size_y - 1, size_y)
    up_z, down_z = lax.rem(me_z + 1, size_z), lax.rem(me_z + size_z - 1, size_z)

    def device(dev_y, dev_z):
        return {"py": dev_y, "pz": dev_z}

    barrier = pltpu.get_barrier_semaphore()
    neighbours = [device(dy, dz) for dy in (down_y, me_y, up_y) for dz in (down_z, me_z, up_z)]
    del neighbours[4]
    for neighbour in neighbours:
        pl.semaphore_signal(barrier, inc=1, device_id=neighbour, device_id_type=MESH)

    plane_order = [0, ny - 1] + list(range(1, ny - 1))
    loads = {y: pltpu.make_async_copy(field_ref.at[:, y], stage.at[:, y], load_sem.at[y]) for y in plane_order}
    for y in plane_order:
        loads[y].start()

    tau = jnp.full((ROWS, LANES), tau_ref[0], jnp.float32)
    rate = 1.0 / tau
    keep = 1.0 - rate
    rate36 = rate * (1.0 / 36.0)
    force = [tau * force_ref[axis] for axis in range(3)]
    lane = lax.broadcasted_iota(jnp.int32, (ROWS, LANES), 1)
    buffers = (other, out_ref)
    tiles = nz // ROWS

    def collide_tile(step, y, tile):
        row = pl.multiple_of(tile * ROWS, ROWS)
        target = buffers[step % 2]
        source = buffers[(step + 1) % 2]

        def load(half, pop_id):
            if step == 0:
                return stage[pop_id, y, pl.ds(row, ROWS), pl.ds(half * LANES, LANES)]
            _, shift_y, shift_z = VELOCITIES[pop_id]
            return source[SLOT[pop_id], y + 1 - shift_y, half, pl.ds(row + (ROWS - shift_z), ROWS), :]

        def store(pop_id, halves):
            halves = rolled(halves, VELOCITIES[pop_id][0], lane)
            for half in range(2):
                target[SLOT[pop_id], y + 1, half, pl.ds(row + ROWS, ROWS), :] = halves[half]

        loaders = [functools.partial(load, half) for half in range(2)]
        terms = [tile_terms(loaders[half], force, rate36) for half in range(2)]
        store(0, [loaders[half](0) * keep + terms[half][0] * 12.0 for half in range(2)])
        for plus in range(1, 19, 2):
            pairs = [relaxed(loaders[half], terms[half], keep, plus) for half in range(2)]
            store(plus, [pair[0] for pair in pairs])
            store(plus + 1, [pair[1] for pair in pairs])

    def faces(step, tile):
        state, parity = buffers[step % 2], step % 2
        rows = pl.ds(pl.multiple_of(tile * ROWS + ROWS, ROWS), ROWS)
        result = []
        for face, (slots, source, target, dev_y) in enumerate(((pl.ds(0, 5), ny, 0, up_y), (pl.ds(8, 5), 1, ny + 1, down_y))):
            result.append(pltpu.make_async_remote_copy(
                src_ref=state.at[slots, source, :, rows, :], dst_ref=state.at[slots, target, :, rows, :],
                send_sem=face_send.at[parity, face, tile], recv_sem=face_recv.at[parity, face, tile],
                device_id=device(dev_y, me_z), device_id_type=MESH))
        return result

    def edges(step):
        state, parity = buffers[step % 2], step % 2
        planes = pl.ds(1, ny)
        low, high, below, above = (pl.ds(row, 1) for row in (ROWS, ROWS + nz - 1, ROWS - 1, ROWS + nz))
        parts = (
            (0, ny, low, 0, above, up_y, down_z),
            (12, 1, low, ny + 1, above, down_y, down_z),
            (pl.ds(12, 4), planes, low, planes, above, me_y, down_z),
            (0, planes, low, planes, above, me_y, down_z),
            (4, ny, high, 0, below, up_y, up_z),
            (8, 1, high, ny + 1, below, down_y, up_z),
            (pl.ds(4, 5), planes, high, planes, below, me_y, up_z),
        )
        return [pltpu.make_async_remote_copy(
            src_ref=state.at[slots, source, :, source_row, :], dst_ref=state.at[slots, target, :, target_row, :],
            send_sem=edge_send.at[parity, number], recv_sem=edge_recv.at[parity, number],
            device_id=device(dev_y, dev_z), device_id_type=MESH)
            for number, (slots, source, source_row, target, target_row, dev_y, dev_z) in enumerate(parts)]

    def over(start, stop, body):
        def run(index, carry):
            body(index)
            return carry
        lax.fori_loop(start, stop, run, 0)

    all_edges = [edges(step) for step in range(STEPS)]
    for step in range(STEPS):
        now = all_edges[step]
        if step == 0:
            loads[0].wait()
            loads[ny - 1].wait()

        def await_piece(tile):
            for copy in faces(step - 1, tile):
                copy.wait_recv()

        def place(position):
            upward = position % 2 == 0
            tile = jnp.where(upward, position // 2, tiles - 1 - position // 2)
            if step > 0:
                @pl.when(position < 2)
                def _():
                    await_piece(tile)
                @pl.when(position < tiles - 2)
                def _():
                    await_piece(jnp.where(upward, tile + 1, tile - 1))
                @pl.when(position == 0)
                def _():
                    for copy in all_edges[step - 1][:4]:
                        copy.wait_recv()
                    for copy in all_edges[step - 1][4:]:
                        copy.wait_recv()
            if step >= 2:
                for copy in faces(step - 2, tile):
                    copy.wait_send()
                @pl.when(position == 0)
                def _():
                    for copy in all_edges[step - 2]:
                        copy.wait_send()
            over(0, 2, lambda index: collide_tile(step, index * (ny - 1), tile))
            if step == 0:
                @pl.when(position == 0)
                def _():
                    pl.semaphore_wait(barrier, len(neighbours))
            for number in range(2):
                @pl.when(position == number)
                def _():
                    for copy in (now[0:2], now[4:6])[number]:
                        copy.start()
            for copy in faces(step, tile):
                copy.start()
            if step == 0:
                @pl.when(position == 0)
                def _():
                    for y in range(1, ny - 1):
                        loads[y].wait()
            over(1, ny - 1, lambda index: collide_tile(step, index, tile))
            for number in range(2):
                @pl.when(position == number)
                def _():
                    for copy in (now[2:4], now[6:7])[number]:
                        copy.start()

        over(0, tiles, place)

    def await_last(tile):
        for copy in faces(STEPS - 1, tile):
            copy.wait_recv()
        for step in (STEPS - 2, STEPS - 1):
            for copy in faces(step, tile):
                copy.wait_send()

    over(0, tiles, await_last)
    for copy in all_edges[STEPS - 1]:
        copy.wait_recv()
    for step in (STEPS - 2, STEPS - 1):
        for copy in all_edges[step]:
            copy.wait_send()


def output_kernel(ny, nz, tau_ref, force_ref, state, field_ref, density_ref, velocity_ref, moments, field_sem, moment_sem):
    field_copies = []
    for pop_id in range(19):
        _, shift_y, shift_z = VELOCITIES[pop_id]
        for half in range(2):
            field_copies.append(pltpu.make_async_copy(
                state.at[SLOT[pop_id], pl.ds(1 - shift_y, ny), half, pl.ds(ROWS - shift_z, nz), :],
                field_ref.at[pop_id, :, :, pl.ds(half * LANES, LANES)], field_sem.at[2 * pop_id + half]))
    for copy in field_copies:
        copy.start()
    tau = jnp.full((ROWS, LANES), tau_ref[0], jnp.float32)
    force = [tau * force_ref[axis] for axis in range(3)]
    tiles = nz // ROWS
    moment_copies = []
    for y in range(ny):
        def tile_moments(tile, carry):
            row = pl.multiple_of(tile * ROWS, ROWS)
            for half in range(2):
                def load(pop_id):
                    _, shift_y, shift_z = VELOCITIES[pop_id]
                    return state[SLOT[pop_id], y + 1 - shift_y, half, pl.ds(row + (ROWS - shift_z), ROWS), :]
                density, momentum = moment_sums(load)
                inverse = 1.0 / density
                place = (y, pl.ds(row, ROWS), pl.ds(half * LANES, LANES))
                moments[(0, *place)] = density
                for axis in range(3):
                    moments[(1 + axis, *place)] = (momentum[axis] + force[axis]) * inverse
            return carry
        lax.fori_loop(0, tiles, tile_moments, 0)
        moment_copies.append(pltpu.make_async_copy(moments.at[0, y], density_ref.at[y], moment_sem.at[0, y]))
        moment_copies.append(pltpu.make_async_copy(moments.at[pl.ds(1, 3), y], velocity_ref.at[:, y], moment_sem.at[1, y]))
        moment_copies[-2].start()
        moment_copies[-1].start()
    for copy in field_copies + moment_copies:
        copy.wait()


def solution(mesh):
    size_y = mesh.shape["py"]
    size_z = mesh.shape["pz"]
    field_spec = P(None, None, "py", "pz")

    def local_steps(populations, relax_time, body_force):
        field = jnp.transpose(populations, (0, 2, 3, 1))
        _, ny, nz, nx = field.shape
        tau = jnp.reshape(relax_time, (1,))
        state_shape = (19, ny + 2, 2, nz + 2 * ROWS, LANES)
        smem = pl.BlockSpec(memory_space=pltpu.SMEM)
        vmem = pl.BlockSpec(memory_space=pltpu.VMEM)
        anywhere = pl.BlockSpec(memory_space=pl.ANY)
        state = pl.pallas_call(
            functools.partial(step_kernel, size_y, size_z, ny, nz),
            name="lattice_steps",
            out_shape=pltpu.VMEM(state_shape, jnp.float32),
            in_specs=[smem, smem, anywhere],
            out_specs=vmem,
            scratch_shapes=[
                pltpu.VMEM((19, ny, nz, nx), jnp.float32),
                pltpu.VMEM(state_shape, jnp.float32),
                pltpu.SemaphoreType.DMA((ny,)),
                pltpu.SemaphoreType.DMA((2, 2, nz // ROWS)),
                pltpu.SemaphoreType.DMA((2, 2, nz // ROWS)),
                pltpu.SemaphoreType.DMA((2, EDGE_COPIES)),
                pltpu.SemaphoreType.DMA((2, EDGE_COPIES)),
            ],
            compiler_params=pltpu.CompilerParams(collective_id=0, has_side_effects=True, vmem_limit_bytes=44 * 2**20),
        )(tau, body_force, field)
        final, density, velocity = pl.pallas_call(
            functools.partial(output_kernel, ny, nz),
            name="lattice_output",
            out_shape=(
                jax.ShapeDtypeStruct((19, ny, nz, nx), jnp.float32),
                jax.ShapeDtypeStruct((ny, nz, nx), jnp.float32),
                jax.ShapeDtypeStruct((3, ny, nz, nx), jnp.float32),
            ),
            in_specs=[smem, smem, vmem],
            out_specs=(anywhere, anywhere, anywhere),
            scratch_shapes=[
                pltpu.VMEM((4, ny, nz, nx), jnp.float32),
                pltpu.SemaphoreType.DMA((38,)),
                pltpu.SemaphoreType.DMA((2, ny)),
            ],
            compiler_params=pltpu.CompilerParams(vmem_limit_bytes=24 * 2**20),
        )(tau, body_force, state)
        return jnp.transpose(final, (0, 3, 1, 2)), jnp.transpose(density, (2, 0, 1)), jnp.transpose(velocity, (0, 3, 1, 2))

    return jax.shard_map(local_steps, mesh=mesh, in_specs=(field_spec, P(), P()), out_specs=(field_spec, P(None, "py", "pz"), field_spec), check_vma=False)
```

```python
import functools

import jax
import jax.numpy as jnp
from jax import lax
from jax.experimental import pallas as pl
from jax.experimental.pallas import tpu as pltpu
from jax.sharding import PartitionSpec as P

STEPS = 4
VELOCITIES = ((0, 0, 0), (1, 0, 0), (-1, 0, 0), (0, 1, 0), (0, -1, 0), (0, 0, 1), (0, 0, -1), (1, 1, 0), (-1, -1, 0), (1, -1, 0), (-1, 1, 0), (1, 0, 1), (-1, 0, -1), (1, 0, -1), (-1, 0, 1), (0, 1, 1), (0, -1, -1), (0, 1, -1), (0, -1, 1))
ORDER = (17, 3, 7, 10, 15, 5, 11, 14, 18, 4, 8, 9, 16, 6, 12, 13, 0, 1, 2)
SLOT = {pop_id: slot for slot, pop_id in enumerate(ORDER)}
MESH = pl.DeviceIdType.MESH
LANES = 128
ROWS = 8
EDGE_COPIES = 7


def moment_sums(load):
    rest = load(0)
    total = rest
    diff = {}
    for plus in range(1, 19, 2):
        upper, lower = load(plus), load(plus + 1)
        total = total + (upper + lower)
        diff[plus] = upper - lower
    mom_x = (diff[1] + diff[7]) + (diff[9] + (diff[11] + diff[13]))
    mom_y = (diff[3] + diff[7]) - (diff[9] - (diff[15] + diff[17]))
    mom_z = (diff[5] + diff[11]) - (diff[13] - (diff[15] - diff[17]))
    return total, (mom_x, mom_y, mom_z)


def tile_terms(load, force, rate36):
    density, momentum = moment_sums(load)
    inverse = 1.0 / density
    half = [(momentum[axis] + force[axis]) * inverse * 1.5 for axis in range(3)]
    square = half[0] * half[0] + half[1] * half[1] + half[2] * half[2]
    scale = density * rate36
    even = scale * (1.0 - square * (2.0 / 3.0))
    twice = scale + scale
    odd = [twice * half[axis] for axis in range(3)]
    return even, odd, half


def relaxed(load, terms, keep, plus):
    even, odd, half = terms
    axes = [(axis, shift) for axis, shift in enumerate(VELOCITIES[plus]) if shift != 0]
    if len(axes) == 1:
        axis = axes[0][0]
        odd_part = odd[axis] + odd[axis]
        even_part = (even + even) + odd_part * half[axis]
    else:
        (first, _), (second, sign) = axes
        if sign > 0:
            odd_part = odd[first] + odd[second]
            projection = half[first] + half[second]
        else:
            odd_part = odd[first] - odd[second]
            projection = half[first] - half[second]
        even_part = even + odd_part * projection
    return load(plus) * keep + (even_part + odd_part), load(plus + 1) * keep + (even_part - odd_part)


def rolled(halves, shift, lane):
    if shift == 0:
        return halves
    moved = [pltpu.roll(part, shift % LANES, 1) for part in halves]
    edge = lane == (0 if shift > 0 else LANES - 1)
    return [jnp.where(edge, moved[1], moved[0]), jnp.where(edge, moved[0], moved[1])]


def step_kernel(size_y, size_z, ny, nz, tau_in, force_in, field_ref, out_ref, stage, other, tau_ref, force_ref, param_sem, load_sem, first_sem, face_send, face_recv, edge_send, edge_recv):
    me_y, me_z = lax.axis_index("py"), lax.axis_index("pz")
    up_y, down_y = lax.rem(me_y + 1, size_y), lax.rem(me_y + size_y - 1, size_y)
    up_z, down_z = lax.rem(me_z + 1, size_z), lax.rem(me_z + size_z - 1, size_z)

    def device(dev_y, dev_z):
        return {"py": dev_y, "pz": dev_z}

    barrier = pltpu.get_barrier_semaphore()
    neighbours = [device(dy, dz) for dy in (down_y, me_y, up_y) for dz in (down_z, me_z, up_z)]
    del neighbours[4]
    for neighbour in neighbours:
        pl.semaphore_signal(barrier, inc=1, device_id=neighbour, device_id_type=MESH)

    tiles = nz // ROWS
    params = [pltpu.make_async_copy(tau_in, tau_ref, param_sem.at[0]), pltpu.make_async_copy(force_in, force_ref, param_sem.at[1])]
    for copy in params:
        copy.start()

    def first_loads(tile):
        rows = pl.ds(pl.multiple_of(tile * ROWS, ROWS), ROWS)
        return [pltpu.make_async_copy(field_ref.at[:, y, rows], stage.at[:, y, rows], first_sem.at[face, tile]) for face, y in enumerate((0, ny - 1))]

    for position in range(tiles):
        for copy in first_loads(position // 2 if position % 2 == 0 else tiles - 1 - position // 2):
            copy.start()
    loads = [pltpu.make_async_copy(field_ref.at[:, y], stage.at[:, y], load_sem.at[y]) for y in range(1, ny - 1)]
    for copy in loads:
        copy.start()
    for copy in params:
        copy.wait()

    tau = jnp.full((ROWS, LANES), tau_ref[0], jnp.float32)
    rate = 1.0 / tau
    keep = 1.0 - rate
    rate36 = rate * (1.0 / 36.0)
    force = [tau * force_ref[axis] for axis in range(3)]
    lane = lax.broadcasted_iota(jnp.int32, (ROWS, LANES), 1)
    buffers = (other, out_ref)

    def collide_tile(step, y, tile):
        row = pl.multiple_of(tile * ROWS, ROWS)
        target = buffers[step % 2]
        source = buffers[(step + 1) % 2]

        def load(half, pop_id):
            if step == 0:
                return stage[pop_id, y, pl.ds(row, ROWS), pl.ds(half * LANES, LANES)]
            _, shift_y, shift_z = VELOCITIES[pop_id]
            return source[SLOT[pop_id], y + 1 - shift_y, half, pl.ds(row + (ROWS - shift_z), ROWS), :]

        def store(pop_id, halves):
            halves = rolled(halves, VELOCITIES[pop_id][0], lane)
            for half in range(2):
                target[SLOT[pop_id], y + 1, half, pl.ds(row + ROWS, ROWS), :] = halves[half]

        loaders = [functools.partial(load, half) for half in range(2)]
        terms = [tile_terms(loaders[half], force, rate36) for half in range(2)]
        store(0, [loaders[half](0) * keep + terms[half][0] * 12.0 for half in range(2)])
        for plus in range(1, 19, 2):
            pairs = [relaxed(loaders[half], terms[half], keep, plus) for half in range(2)]
            store(plus, [pair[0] for pair in pairs])
            store(plus + 1, [pair[1] for pair in pairs])

    def faces(step, tile):
        state, parity = buffers[step % 2], step % 2
        rows = pl.ds(pl.multiple_of(tile * ROWS + ROWS, ROWS), ROWS)
        result = []
        for face, (slots, source, target, dev_y) in enumerate(((pl.ds(0, 5), ny, 0, up_y), (pl.ds(8, 5), 1, ny + 1, down_y))):
            result.append(pltpu.make_async_remote_copy(
                src_ref=state.at[slots, source, :, rows, :], dst_ref=state.at[slots, target, :, rows, :],
                send_sem=face_send.at[parity, face, tile], recv_sem=face_recv.at[parity, face, tile],
                device_id=device(dev_y, me_z), device_id_type=MESH))
        return result

    def edges(step):
        state, parity = buffers[step % 2], step % 2
        planes = pl.ds(1, ny)
        low, high, below, above = (pl.ds(row, 1) for row in (ROWS, ROWS + nz - 1, ROWS - 1, ROWS + nz))
        parts = (
            (0, ny, low, 0, above, up_y, down_z),
            (12, 1, low, ny + 1, above, down_y, down_z),
            (pl.ds(12, 4), planes, low, planes, above, me_y, down_z),
            (0, planes, low, planes, above, me_y, down_z),
            (4, ny, high, 0, below, up_y, up_z),
            (8, 1, high, ny + 1, below, down_y, up_z),
            (pl.ds(4, 5), planes, high, planes, below, me_y, up_z),
        )
        return [pltpu.make_async_remote_copy(
            src_ref=state.at[slots, source, :, source_row, :], dst_ref=state.at[slots, target, :, target_row, :],
            send_sem=edge_send.at[parity, number], recv_sem=edge_recv.at[parity, number],
            device_id=device(dev_y, dev_z), device_id_type=MESH)
            for number, (slots, source, source_row, target, target_row, dev_y, dev_z) in enumerate(parts)]

    def over(start, stop, body, unroll=False):
        def run(index, carry):
            body(index)
            return carry
        lax.fori_loop(start, stop, run, 0, unroll=unroll)

    all_edges = [edges(step) for step in range(STEPS)]
    for step in range(STEPS):
        now = all_edges[step]
        def await_piece(tile):
            for copy in faces(step - 1, tile):
                copy.wait_recv()

        def place(position):
            upward = position % 2 == 0
            tile = jnp.where(upward, position // 2, tiles - 1 - position // 2)
            if step == 0:
                for copy in first_loads(tile):
                    copy.wait()
            if step > 0:
                @pl.when(position < 2)
                def _():
                    await_piece(tile)
                @pl.when(position < tiles - 2)
                def _():
                    await_piece(jnp.where(upward, tile + 1, tile - 1))
                @pl.when(position == 0)
                def _():
                    for copy in all_edges[step - 1][:4]:
                        copy.wait_recv()
                    for copy in all_edges[step - 1][4:]:
                        copy.wait_recv()
            if step >= 2:
                for copy in faces(step - 2, tile):
                    copy.wait_send()
                @pl.when(position == 0)
                def _():
                    for copy in all_edges[step - 2]:
                        copy.wait_send()
            over(0, 2, lambda index: collide_tile(step, index * (ny - 1), tile), True)
            if step == 0:
                @pl.when(position == 0)
                def _():
                    pl.semaphore_wait(barrier, len(neighbours))
            for number in range(2):
                @pl.when(position == number)
                def _():
                    for copy in (now[0:2], now[4:6])[number]:
                        copy.start()
            for copy in faces(step, tile):
                copy.start()
            if step == 0:
                @pl.when(position == 0)
                def _():
                    for copy in loads:
                        copy.wait()
            over(1, ny - 1, lambda index: collide_tile(step, index, tile), True)
            for number in range(2):
                @pl.when(position == number)
                def _():
                    for copy in (now[2:4], now[6:7])[number]:
                        copy.start()

        over(0, tiles, place)

    def await_last(tile):
        for copy in faces(STEPS - 1, tile):
            copy.wait_recv()
        for step in (STEPS - 2, STEPS - 1):
            for copy in faces(step, tile):
                copy.wait_send()

    over(0, tiles, await_last)
    for copy in all_edges[STEPS - 1]:
        copy.wait_recv()
    for step in (STEPS - 2, STEPS - 1):
        for copy in all_edges[step]:
            copy.wait_send()


def output_kernel(ny, nz, tau_in, force_in, state, field_ref, density_ref, velocity_ref, moments, tau_ref, force_ref, param_sem, field_sem, moment_sem):
    params = [pltpu.make_async_copy(tau_in, tau_ref, param_sem.at[0]), pltpu.make_async_copy(force_in, force_ref, param_sem.at[1])]
    for copy in params:
        copy.start()
    field_copies = []
    for pop_id in range(19):
        _, shift_y, shift_z = VELOCITIES[pop_id]
        for half in range(2):
            field_copies.append(pltpu.make_async_copy(
                state.at[SLOT[pop_id], pl.ds(1 - shift_y, ny), half, pl.ds(ROWS - shift_z, nz), :],
                field_ref.at[pop_id, :, :, pl.ds(half * LANES, LANES)], field_sem.at[2 * pop_id + half]))
    for copy in field_copies:
        copy.start()
    for copy in params:
        copy.wait()
    tau = jnp.full((ROWS, LANES), tau_ref[0], jnp.float32)
    force = [tau * force_ref[axis] for axis in range(3)]
    tiles = nz // ROWS
    moment_copies = []
    for y in range(ny):
        def tile_moments(tile, carry):
            row = pl.multiple_of(tile * ROWS, ROWS)
            for half in range(2):
                def load(pop_id):
                    _, shift_y, shift_z = VELOCITIES[pop_id]
                    return state[SLOT[pop_id], y + 1 - shift_y, half, pl.ds(row + (ROWS - shift_z), ROWS), :]
                density, momentum = moment_sums(load)
                inverse = 1.0 / density
                place = (y, pl.ds(row, ROWS), pl.ds(half * LANES, LANES))
                moments[(0, *place)] = density
                for axis in range(3):
                    moments[(1 + axis, *place)] = (momentum[axis] + force[axis]) * inverse
            return carry
        lax.fori_loop(0, tiles, tile_moments, 0)
        moment_copies.append(pltpu.make_async_copy(moments.at[0, y], density_ref.at[y], moment_sem.at[0, y]))
        moment_copies.append(pltpu.make_async_copy(moments.at[pl.ds(1, 3), y], velocity_ref.at[:, y], moment_sem.at[1, y]))
        moment_copies[-2].start()
        moment_copies[-1].start()
    for copy in field_copies + moment_copies:
        copy.wait()


def solution(mesh):
    size_y = mesh.shape["py"]
    size_z = mesh.shape["pz"]
    field_spec = P(None, None, "py", "pz")

    def local_steps(populations, relax_time, body_force):
        field = jnp.transpose(populations, (0, 2, 3, 1))
        _, ny, nz, nx = field.shape
        tau = jnp.reshape(relax_time, (1,))
        state_shape = (19, ny + 2, 2, nz + 2 * ROWS, LANES)
        vmem = pl.BlockSpec(memory_space=pltpu.VMEM)
        anywhere = pl.BlockSpec(memory_space=pl.ANY)
        state = pl.pallas_call(
            functools.partial(step_kernel, size_y, size_z, ny, nz),
            name="lattice_steps",
            out_shape=pltpu.VMEM(state_shape, jnp.float32),
            in_specs=[anywhere, anywhere, anywhere],
            out_specs=vmem,
            scratch_shapes=[
                pltpu.VMEM((19, ny, nz, nx), jnp.float32),
                pltpu.VMEM(state_shape, jnp.float32),
                pltpu.SMEM((1,), jnp.float32),
                pltpu.SMEM((3,), jnp.float32),
                pltpu.SemaphoreType.DMA((2,)),
                pltpu.SemaphoreType.DMA((ny,)),
                pltpu.SemaphoreType.DMA((2, nz // ROWS)),
                pltpu.SemaphoreType.DMA((2, 2, nz // ROWS)),
                pltpu.SemaphoreType.DMA((2, 2, nz // ROWS)),
                pltpu.SemaphoreType.DMA((2, EDGE_COPIES)),
                pltpu.SemaphoreType.DMA((2, EDGE_COPIES)),
            ],
            compiler_params=pltpu.CompilerParams(collective_id=0, has_side_effects=True, vmem_limit_bytes=44 * 2**20),
        )(tau, body_force, field)
        final, density, velocity = pl.pallas_call(
            functools.partial(output_kernel, ny, nz),
            name="lattice_output",
            out_shape=(
                jax.ShapeDtypeStruct((19, ny, nz, nx), jnp.float32),
                jax.ShapeDtypeStruct((ny, nz, nx), jnp.float32),
                jax.ShapeDtypeStruct((3, ny, nz, nx), jnp.float32),
            ),
            in_specs=[anywhere, anywhere, vmem],
            out_specs=(anywhere, anywhere, anywhere),
            scratch_shapes=[
                pltpu.VMEM((4, ny, nz, nx), jnp.float32),
                pltpu.SMEM((1,), jnp.float32),
                pltpu.SMEM((3,), jnp.float32),
                pltpu.SemaphoreType.DMA((2,)),
                pltpu.SemaphoreType.DMA((38,)),
                pltpu.SemaphoreType.DMA((2, ny)),
            ],
            compiler_params=pltpu.CompilerParams(vmem_limit_bytes=24 * 2**20),
        )(tau, body_force, state)
        return jnp.transpose(final, (0, 3, 1, 2)), jnp.transpose(density, (2, 0, 1)), jnp.transpose(velocity, (0, 3, 1, 2))

    return jax.shard_map(local_steps, mesh=mesh, in_specs=(field_spec, P(), P()), out_specs=(field_spec, P(None, "py", "pz"), field_spec), check_vma=False)
```

```python
import functools

import jax
import jax.numpy as jnp
from jax import lax
from jax.experimental import pallas as pl
from jax.experimental.pallas import tpu as pltpu
from jax.sharding import PartitionSpec as P

STEPS = 4
VELOCITIES = ((0, 0, 0), (1, 0, 0), (-1, 0, 0), (0, 1, 0), (0, -1, 0), (0, 0, 1), (0, 0, -1), (1, 1, 0), (-1, -1, 0), (1, -1, 0), (-1, 1, 0), (1, 0, 1), (-1, 0, -1), (1, 0, -1), (-1, 0, 1), (0, 1, 1), (0, -1, -1), (0, 1, -1), (0, -1, 1))
ORDER = (17, 3, 7, 10, 15, 5, 11, 14, 18, 4, 8, 9, 16, 6, 12, 13, 0, 1, 2)
SLOT = {pop_id: slot for slot, pop_id in enumerate(ORDER)}
MESH = pl.DeviceIdType.MESH
LANES = 128
ROWS = 8
EDGE_COPIES = 7


def moment_sums(load):
    rest = load(0)
    total = rest
    diff = {}
    for plus in range(1, 19, 2):
        upper, lower = load(plus), load(plus + 1)
        total = total + (upper + lower)
        diff[plus] = upper - lower
    mom_x = (diff[1] + diff[7]) + (diff[9] + (diff[11] + diff[13]))
    mom_y = (diff[3] + diff[7]) - (diff[9] - (diff[15] + diff[17]))
    mom_z = (diff[5] + diff[11]) - (diff[13] - (diff[15] - diff[17]))
    return total, (mom_x, mom_y, mom_z)


def tile_terms(load, force, rate36):
    density, momentum = moment_sums(load)
    inverse = 1.0 / density
    half = [(momentum[axis] + force[axis]) * inverse * 1.5 for axis in range(3)]
    square = half[0] * half[0] + half[1] * half[1] + half[2] * half[2]
    scale = density * rate36
    even = scale * (1.0 - square * (2.0 / 3.0))
    twice = scale + scale
    odd = [twice * half[axis] for axis in range(3)]
    return even, odd, half


def relaxed(load, terms, keep, plus):
    even, odd, half = terms
    axes = [(axis, shift) for axis, shift in enumerate(VELOCITIES[plus]) if shift != 0]
    if len(axes) == 1:
        axis = axes[0][0]
        odd_part = odd[axis] + odd[axis]
        even_part = (even + even) + odd_part * half[axis]
    else:
        (first, _), (second, sign) = axes
        if sign > 0:
            odd_part = odd[first] + odd[second]
            projection = half[first] + half[second]
        else:
            odd_part = odd[first] - odd[second]
            projection = half[first] - half[second]
        even_part = even + odd_part * projection
    return load(plus) * keep + (even_part + odd_part), load(plus + 1) * keep + (even_part - odd_part)


def rolled(halves, shift, lane):
    if shift == 0:
        return halves
    moved = [pltpu.roll(part, shift % LANES, 1) for part in halves]
    edge = lane == (0 if shift > 0 else LANES - 1)
    return [jnp.where(edge, moved[1], moved[0]), jnp.where(edge, moved[0], moved[1])]


def step_kernel(size_y, size_z, ny, nz, tau_in, force_in, field_ref, stage, density_ref, velocity_ref, buffer_0, buffer_1, tau_ref, force_ref, param_sem, load_sem, first_sem, face_send, face_recv, edge_send, edge_recv):
    me_y, me_z = lax.axis_index("py"), lax.axis_index("pz")
    up_y, down_y = lax.rem(me_y + 1, size_y), lax.rem(me_y + size_y - 1, size_y)
    up_z, down_z = lax.rem(me_z + 1, size_z), lax.rem(me_z + size_z - 1, size_z)

    def device(dev_y, dev_z):
        return {"py": dev_y, "pz": dev_z}

    barrier = pltpu.get_barrier_semaphore()
    neighbours = [device(dy, dz) for dy in (down_y, me_y, up_y) for dz in (down_z, me_z, up_z)]
    del neighbours[4]
    for neighbour in neighbours:
        pl.semaphore_signal(barrier, inc=1, device_id=neighbour, device_id_type=MESH)

    tiles = nz // ROWS
    params = [pltpu.make_async_copy(tau_in, tau_ref, param_sem.at[0]), pltpu.make_async_copy(force_in, force_ref, param_sem.at[1])]
    for copy in params:
        copy.start()

    def first_loads(tile):
        rows = pl.ds(pl.multiple_of(tile * ROWS, ROWS), ROWS)
        return [pltpu.make_async_copy(field_ref.at[:, y, rows], stage.at[:, y, rows], first_sem.at[face, tile]) for face, y in enumerate((0, ny - 1))]

    for position in range(tiles):
        for copy in first_loads(position // 2 if position % 2 == 0 else tiles - 1 - position // 2):
            copy.start()
    loads = [pltpu.make_async_copy(field_ref.at[:, y], stage.at[:, y], load_sem.at[y]) for y in range(1, ny - 1)]
    for copy in loads:
        copy.start()
    for copy in params:
        copy.wait()

    tau = jnp.full((ROWS, LANES), tau_ref[0], jnp.float32)
    rate = 1.0 / tau
    keep = 1.0 - rate
    rate36 = rate * (1.0 / 36.0)
    force = [tau * force_ref[axis] for axis in range(3)]
    lane = lax.broadcasted_iota(jnp.int32, (ROWS, LANES), 1)
    buffers = (buffer_0, buffer_1)

    def collide_tile(step, y, tile):
        row = pl.multiple_of(tile * ROWS, ROWS)
        target = buffers[step % 2]
        source = buffers[(step + 1) % 2]

        def load(half, pop_id):
            if step == 0:
                return stage[pop_id, y, pl.ds(row, ROWS), pl.ds(half * LANES, LANES)]
            _, shift_y, shift_z = VELOCITIES[pop_id]
            return source[SLOT[pop_id], y + 1 - shift_y, half, pl.ds(row + (ROWS - shift_z), ROWS), :]

        def store(pop_id, halves):
            halves = rolled(halves, VELOCITIES[pop_id][0], lane)
            for half in range(2):
                target[SLOT[pop_id], y + 1, half, pl.ds(row + ROWS, ROWS), :] = halves[half]

        loaders = [functools.partial(load, half) for half in range(2)]
        terms = [tile_terms(loaders[half], force, rate36) for half in range(2)]
        store(0, [loaders[half](0) * keep + terms[half][0] * 12.0 for half in range(2)])
        for plus in range(1, 19, 2):
            pairs = [relaxed(loaders[half], terms[half], keep, plus) for half in range(2)]
            store(plus, [pair[0] for pair in pairs])
            store(plus + 1, [pair[1] for pair in pairs])

    def faces(step, tile):
        state, parity = buffers[step % 2], step % 2
        rows = pl.ds(pl.multiple_of(tile * ROWS + ROWS, ROWS), ROWS)
        result = []
        for face, (slots, source, target, dev_y) in enumerate(((pl.ds(0, 5), ny, 0, up_y), (pl.ds(8, 5), 1, ny + 1, down_y))):
            result.append(pltpu.make_async_remote_copy(
                src_ref=state.at[slots, source, :, rows, :], dst_ref=state.at[slots, target, :, rows, :],
                send_sem=face_send.at[parity, face, tile], recv_sem=face_recv.at[parity, face, tile],
                device_id=device(dev_y, me_z), device_id_type=MESH))
        return result

    def edges(step):
        state, parity = buffers[step % 2], step % 2
        planes = pl.ds(1, ny)
        low, high, below, above = (pl.ds(row, 1) for row in (ROWS, ROWS + nz - 1, ROWS - 1, ROWS + nz))
        parts = (
            (0, ny, low, 0, above, up_y, down_z),
            (12, 1, low, ny + 1, above, down_y, down_z),
            (pl.ds(12, 4), planes, low, planes, above, me_y, down_z),
            (0, planes, low, planes, above, me_y, down_z),
            (4, ny, high, 0, below, up_y, up_z),
            (8, 1, high, ny + 1, below, down_y, up_z),
            (pl.ds(4, 5), planes, high, planes, below, me_y, up_z),
        )
        return [pltpu.make_async_remote_copy(
            src_ref=state.at[slots, source, :, source_row, :], dst_ref=state.at[slots, target, :, target_row, :],
            send_sem=edge_send.at[parity, number], recv_sem=edge_recv.at[parity, number],
            device_id=device(dev_y, dev_z), device_id_type=MESH)
            for number, (slots, source, source_row, target, target_row, dev_y, dev_z) in enumerate(parts)]

    def over(start, stop, body, unroll=False):
        def run(index, carry):
            body(index)
            return carry
        lax.fori_loop(start, stop, run, 0, unroll=unroll)

    def finish_tile(y, tile):
        row = pl.multiple_of(tile * ROWS, ROWS)
        source = buffers[(STEPS - 1) % 2]
        for half in range(2):
            place = (y, pl.ds(row, ROWS), pl.ds(half * LANES, LANES))

            def load(pop_id):
                _, shift_y, shift_z = VELOCITIES[pop_id]
                value = source[SLOT[pop_id], y + 1 - shift_y, half, pl.ds(row + (ROWS - shift_z), ROWS), :]
                stage[(pop_id, *place)] = value
                return value

            density, momentum = moment_sums(load)
            density_ref[place] = density
            for axis in range(3):
                velocity_ref[(axis, *place)] = (momentum[axis] + force[axis]) / density

    def tile_at(position):
        return jnp.where(position % 2 == 0, position // 2, tiles - 1 - position // 2)

    def at_position(position, number, copies):
        @pl.when(position == number)
        def _():
            for copy in copies:
                copy.start()

    all_edges = [edges(step) for step in range(STEPS)]

    def collide_faces(step, tile):
        over(0, 2, lambda index: collide_tile(step, index * (ny - 1), tile), True)

    def collide_inner(step, tile):
        over(1, ny - 1, lambda index: collide_tile(step, index, tile), True)

    def start_faces(step, position, tile):
        at_position(position, 0, all_edges[step][0:2])
        at_position(position, 1, all_edges[step][4:6])
        for copy in faces(step, tile):
            copy.start()

    def start_rows(step, position):
        at_position(position, 0, all_edges[step][2:4])
        at_position(position, 1, all_edges[step][6:7])

    def await_pieces(step, position, tile):
        def await_piece(number):
            for copy in faces(step, number):
                copy.wait_recv()

        @pl.when(position < 2)
        def _():
            await_piece(tile)
        @pl.when(position < tiles - 2)
        def _():
            await_piece(jnp.where(position % 2 == 0, tile + 1, tile - 1))

    def first_faces(position):
        tile = tile_at(position)
        for copy in first_loads(tile):
            copy.wait()
        collide_faces(0, tile)
        @pl.when(position == 0)
        def _():
            pl.semaphore_wait(barrier, len(neighbours))
        start_faces(0, position, tile)

    def first_inner(position):
        collide_inner(0, tile_at(position))
        start_rows(0, position)

    over(0, tiles, first_faces)
    for copy in loads:
        copy.wait()
    over(0, tiles, first_inner)

    for step in range(1, STEPS):
        def place(position):
            tile = tile_at(position)
            await_pieces(step - 1, position, tile)
            @pl.when(position == 0)
            def _():
                for copy in all_edges[step - 1]:
                    copy.wait_recv()
            if step >= 2:
                for copy in faces(step - 2, tile):
                    copy.wait_send()
                @pl.when(position == 0)
                def _():
                    for copy in all_edges[step - 2]:
                        copy.wait_send()
            collide_faces(step, tile)
            start_faces(step, position, tile)
            collide_inner(step, tile)
            start_rows(step, position)

        over(0, tiles, place)

    last = STEPS - 1
    for copy in all_edges[last]:
        copy.wait_recv()
    over(0, tiles, lambda tile: over(1, ny - 1, lambda y: finish_tile(y, tile)))

    def finish_faces(position):
        tile = tile_at(position)
        await_pieces(last, position, tile)
        over(0, 2, lambda index: finish_tile(index * (ny - 1), tile))

    over(0, tiles, finish_faces)

    def await_sends(tile):
        for step in (last - 1, last):
            for copy in faces(step, tile):
                copy.wait_send()

    over(0, tiles, await_sends)
    for step in (last - 1, last):
        for copy in all_edges[step]:
            copy.wait_send()


def output_kernel(final_in, density_in, velocity_in, final_ref, density_ref, velocity_ref, final_sem, moment_sem):
    copies = [pltpu.make_async_copy(final_in.at[pop_id], final_ref.at[pop_id], final_sem.at[pop_id]) for pop_id in range(19)]
    copies.append(pltpu.make_async_copy(density_in, density_ref, moment_sem.at[0]))
    copies.append(pltpu.make_async_copy(velocity_in, velocity_ref, moment_sem.at[1]))
    for copy in copies:
        copy.start()
    for copy in copies:
        copy.wait()


def solution(mesh):
    size_y = mesh.shape["py"]
    size_z = mesh.shape["pz"]
    field_spec = P(None, None, "py", "pz")

    def local_steps(populations, relax_time, body_force):
        field = jnp.transpose(populations, (0, 2, 3, 1))
        _, ny, nz, nx = field.shape
        tau = jnp.reshape(relax_time, (1,))
        state_shape = (19, ny + 2, 2, nz + 2 * ROWS, LANES)
        vmem = pl.BlockSpec(memory_space=pltpu.VMEM)
        anywhere = pl.BlockSpec(memory_space=pl.ANY)
        results = pl.pallas_call(
            functools.partial(step_kernel, size_y, size_z, ny, nz),
            name="lattice_steps",
            out_shape=(
                pltpu.VMEM((19, ny, nz, nx), jnp.float32),
                pltpu.VMEM((ny, nz, nx), jnp.float32),
                pltpu.VMEM((3, ny, nz, nx), jnp.float32),
            ),
            in_specs=[anywhere, anywhere, anywhere],
            out_specs=(vmem, vmem, vmem),
            scratch_shapes=[
                pltpu.VMEM(state_shape, jnp.float32),
                pltpu.VMEM(state_shape, jnp.float32),
                pltpu.SMEM((1,), jnp.float32),
                pltpu.SMEM((3,), jnp.float32),
                pltpu.SemaphoreType.DMA((2,)),
                pltpu.SemaphoreType.DMA((ny,)),
                pltpu.SemaphoreType.DMA((2, nz // ROWS)),
                pltpu.SemaphoreType.DMA((2, 2, nz // ROWS)),
                pltpu.SemaphoreType.DMA((2, 2, nz // ROWS)),
                pltpu.SemaphoreType.DMA((2, EDGE_COPIES)),
                pltpu.SemaphoreType.DMA((2, EDGE_COPIES)),
            ],
            compiler_params=pltpu.CompilerParams(collective_id=0, has_side_effects=True, vmem_limit_bytes=46 * 2**20),
        )(tau, body_force, field)
        final, density, velocity = pl.pallas_call(
            output_kernel,
            name="lattice_output",
            out_shape=tuple(jax.ShapeDtypeStruct(result.shape, result.dtype) for result in results),
            in_specs=[vmem, vmem, vmem],
            out_specs=(anywhere, anywhere, anywhere),
            scratch_shapes=[pltpu.SemaphoreType.DMA((19,)), pltpu.SemaphoreType.DMA((2,))],
            compiler_params=pltpu.CompilerParams(vmem_limit_bytes=2**20),
        )(*results)
        return jnp.transpose(final, (0, 3, 1, 2)), jnp.transpose(density, (2, 0, 1)), jnp.transpose(velocity, (0, 3, 1, 2))

    return jax.shard_map(local_steps, mesh=mesh, in_specs=(field_spec, P(), P()), out_specs=(field_spec, P(None, "py", "pz"), field_spec), check_vma=False)
```

```python
import functools

import jax
import jax.numpy as jnp
from jax import lax
from jax.experimental import pallas as pl
from jax.experimental.pallas import tpu as pltpu
from jax.sharding import PartitionSpec as P

STEPS = 4
VELOCITIES = ((0, 0, 0), (1, 0, 0), (-1, 0, 0), (0, 1, 0), (0, -1, 0), (0, 0, 1), (0, 0, -1), (1, 1, 0), (-1, -1, 0), (1, -1, 0), (-1, 1, 0), (1, 0, 1), (-1, 0, -1), (1, 0, -1), (-1, 0, 1), (0, 1, 1), (0, -1, -1), (0, 1, -1), (0, -1, 1))
ORDER = (17, 3, 7, 10, 15, 5, 11, 14, 18, 4, 8, 9, 16, 6, 12, 13, 0, 1, 2)
SLOT = {pop_id: slot for slot, pop_id in enumerate(ORDER)}
MESH = pl.DeviceIdType.MESH
LANES = 128
ROWS = 8
EDGE_COPIES = 7


def moment_sums(load):
    rest = load(0)
    total = rest
    diff = {}
    for plus in range(1, 19, 2):
        upper, lower = load(plus), load(plus + 1)
        total = total + (upper + lower)
        diff[plus] = upper - lower
    mom_x = (diff[1] + diff[7]) + (diff[9] + (diff[11] + diff[13]))
    mom_y = (diff[3] + diff[7]) - (diff[9] - (diff[15] + diff[17]))
    mom_z = (diff[5] + diff[11]) - (diff[13] - (diff[15] - diff[17]))
    return total, (mom_x, mom_y, mom_z)


def tile_terms(load, force, rate36):
    density, momentum = moment_sums(load)
    inverse = 1.0 / density
    half = [(momentum[axis] + force[axis]) * inverse * 1.5 for axis in range(3)]
    square = half[0] * half[0] + half[1] * half[1] + half[2] * half[2]
    scale = density * rate36
    even = scale * (1.0 - square * (2.0 / 3.0))
    twice = scale + scale
    odd = [twice * half[axis] for axis in range(3)]
    return even, odd, half


def relaxed(load, terms, keep, plus):
    even, odd, half = terms
    axes = [(axis, shift) for axis, shift in enumerate(VELOCITIES[plus]) if shift != 0]
    if len(axes) == 1:
        axis = axes[0][0]
        odd_part = odd[axis] + odd[axis]
        even_part = (even + even) + odd_part * half[axis]
    else:
        (first, _), (second, sign) = axes
        if sign > 0:
            odd_part = odd[first] + odd[second]
            projection = half[first] + half[second]
        else:
            odd_part = odd[first] - odd[second]
            projection = half[first] - half[second]
        even_part = even + odd_part * projection
    return load(plus) * keep + (even_part + odd_part), load(plus + 1) * keep + (even_part - odd_part)


def rolled(halves, shift, lane):
    if shift == 0:
        return halves
    moved = [pltpu.roll(part, shift % LANES, 1) for part in halves]
    edge = lane == (0 if shift > 0 else LANES - 1)
    return [jnp.where(edge, moved[1], moved[0]), jnp.where(edge, moved[0], moved[1])]


def step_kernel(size_y, size_z, ny, nz, tau_in, force_in, field_ref, stage, density_ref, velocity_ref, buffer_0, buffer_1, tau_ref, force_ref, param_sem, load_sem, first_sem, face_send, face_recv, edge_send, edge_recv):
    me_y, me_z = lax.axis_index("py"), lax.axis_index("pz")
    up_y, down_y = lax.rem(me_y + 1, size_y), lax.rem(me_y + size_y - 1, size_y)
    up_z, down_z = lax.rem(me_z + 1, size_z), lax.rem(me_z + size_z - 1, size_z)

    def device(dev_y, dev_z):
        return {"py": dev_y, "pz": dev_z}

    barrier = pltpu.get_barrier_semaphore()
    beside = [(dev_y, dev_z) for dev_z in (down_z, up_z) for dev_y in (down_y, me_y, up_y)]

    def signal(dev_y, dev_z):
        pl.semaphore_signal(barrier, inc=1, device_id=device(dev_y, dev_z), device_id_type=MESH)

    signal(up_y, me_z)
    signal(down_y, me_z)
    for dev_y, dev_z in beside:
        @pl.when(jnp.logical_and(me_z != 0, dev_z != 0))
        def _():
            signal(dev_y, dev_z)

    def enter():
        @pl.when(me_z == 0)
        def _():
            pl.semaphore_wait(barrier, 2)
        @pl.when(me_z != 0)
        def _():
            pl.semaphore_wait(barrier, 2 + len(beside))
        for dev_y, dev_z in beside:
            @pl.when(jnp.logical_or(me_z == 0, dev_z == 0))
            def _():
                signal(dev_y, dev_z)

    tiles = nz // ROWS
    params = [pltpu.make_async_copy(tau_in, tau_ref, param_sem.at[0]), pltpu.make_async_copy(force_in, force_ref, param_sem.at[1])]
    for copy in params:
        copy.start()

    def first_loads(tile):
        rows = pl.ds(pl.multiple_of(tile * ROWS, ROWS), ROWS)
        return [pltpu.make_async_copy(field_ref.at[:, y, rows], stage.at[:, y, rows], first_sem.at[face, tile]) for face, y in enumerate((0, ny - 1))]

    def inner_load(tile):
        rows = pl.ds(pl.multiple_of(tile * ROWS, ROWS), ROWS)
        planes = pl.ds(1, ny - 2)
        return pltpu.make_async_copy(field_ref.at[:, planes, rows], stage.at[:, planes, rows], load_sem.at[tile])

    order = [position // 2 if position % 2 == 0 else tiles - 1 - position // 2 for position in range(tiles)]
    for positions in (order[:2], order[2:]):
        for tile in positions:
            for copy in first_loads(tile):
                copy.start()
        for tile in positions:
            inner_load(tile).start()
    for copy in params:
        copy.wait()

    tau = jnp.full((ROWS, LANES), tau_ref[0], jnp.float32)
    rate = 1.0 / tau
    keep = 1.0 - rate
    rate36 = rate * (1.0 / 36.0)
    force = [tau * force_ref[axis] for axis in range(3)]
    lane = lax.broadcasted_iota(jnp.int32, (ROWS, LANES), 1)
    buffers = (buffer_0, buffer_1)

    def collide_tile(step, y, tile):
        row = pl.multiple_of(tile * ROWS, ROWS)
        target = buffers[step % 2]
        source = buffers[(step + 1) % 2]

        def load(half, pop_id):
            if step == 0:
                return stage[pop_id, y, pl.ds(row, ROWS), pl.ds(half * LANES, LANES)]
            _, shift_y, shift_z = VELOCITIES[pop_id]
            return source[SLOT[pop_id], y + 1 - shift_y, half, pl.ds(row + (ROWS - shift_z), ROWS), :]

        def store(pop_id, halves):
            halves = rolled(halves, VELOCITIES[pop_id][0], lane)
            for half in range(2):
                target[SLOT[pop_id], y + 1, half, pl.ds(row + ROWS, ROWS), :] = halves[half]

        loaders = [functools.partial(load, half) for half in range(2)]
        terms = [tile_terms(loaders[half], force, rate36) for half in range(2)]
        store(0, [loaders[half](0) * keep + terms[half][0] * 12.0 for half in range(2)])
        for plus in range(1, 19, 2):
            pairs = [relaxed(loaders[half], terms[half], keep, plus) for half in range(2)]
            store(plus, [pair[0] for pair in pairs])
            store(plus + 1, [pair[1] for pair in pairs])

    def faces(step, tile):
        state, parity = buffers[step % 2], step % 2
        rows = pl.ds(pl.multiple_of(tile * ROWS + ROWS, ROWS), ROWS)
        result = []
        for face, (slots, source, target, dev_y) in enumerate(((pl.ds(0, 5), ny, 0, up_y), (pl.ds(8, 5), 1, ny + 1, down_y))):
            result.append(pltpu.make_async_remote_copy(
                src_ref=state.at[slots, source, :, rows, :], dst_ref=state.at[slots, target, :, rows, :],
                send_sem=face_send.at[parity, face, tile], recv_sem=face_recv.at[parity, face, tile],
                device_id=device(dev_y, me_z), device_id_type=MESH))
        return result

    def edges(step):
        state, parity = buffers[step % 2], step % 2
        planes = pl.ds(1, ny)
        low, high, below, above = (pl.ds(row, 1) for row in (ROWS, ROWS + nz - 1, ROWS - 1, ROWS + nz))
        parts = (
            (0, ny, low, 0, above, up_y, down_z),
            (12, 1, low, ny + 1, above, down_y, down_z),
            (pl.ds(12, 4), planes, low, planes, above, me_y, down_z),
            (0, planes, low, planes, above, me_y, down_z),
            (4, ny, high, 0, below, up_y, up_z),
            (8, 1, high, ny + 1, below, down_y, up_z),
            (pl.ds(4, 5), planes, high, planes, below, me_y, up_z),
        )
        return [pltpu.make_async_remote_copy(
            src_ref=state.at[slots, source, :, source_row, :], dst_ref=state.at[slots, target, :, target_row, :],
            send_sem=edge_send.at[parity, number], recv_sem=edge_recv.at[parity, number],
            device_id=device(dev_y, dev_z), device_id_type=MESH)
            for number, (slots, source, source_row, target, target_row, dev_y, dev_z) in enumerate(parts)]

    def over(start, stop, body, unroll=False):
        def run(index, carry):
            body(index)
            return carry
        lax.fori_loop(start, stop, run, 0, unroll=unroll)

    def finish_tile(y, tile):
        row = pl.multiple_of(tile * ROWS, ROWS)
        source = buffers[(STEPS - 1) % 2]
        for half in range(2):
            place = (y, pl.ds(row, ROWS), pl.ds(half * LANES, LANES))

            def load(pop_id):
                _, shift_y, shift_z = VELOCITIES[pop_id]
                value = source[SLOT[pop_id], y + 1 - shift_y, half, pl.ds(row + (ROWS - shift_z), ROWS), :]
                stage[(pop_id, *place)] = value
                return value

            density, momentum = moment_sums(load)
            density_ref[place] = density
            for axis in range(3):
                velocity_ref[(axis, *place)] = (momentum[axis] + force[axis]) / density

    def tile_at(position):
        return jnp.where(position % 2 == 0, position // 2, tiles - 1 - position // 2)

    def at_position(position, number, copies):
        @pl.when(position == number)
        def _():
            for copy in copies:
                copy.start()

    all_edges = [edges(step) for step in range(STEPS)]

    def collide_faces(step, tile):
        over(0, 2, lambda index: collide_tile(step, index * (ny - 1), tile), True)

    def collide_inner(step, tile):
        over(1, ny - 1, lambda index: collide_tile(step, index, tile), True)

    def start_faces(step, position, tile):
        at_position(position, 0, all_edges[step][0:2])
        at_position(position, 1, all_edges[step][4:6])
        for copy in faces(step, tile):
            copy.start()

    def start_rows(step, position):
        at_position(position, 0, all_edges[step][2:4])
        at_position(position, 1, all_edges[step][6:7])

    def await_pieces(step, position, tile):
        def await_piece(number):
            for copy in faces(step, number):
                copy.wait_recv()

        @pl.when(position < 2)
        def _():
            await_piece(tile)
        @pl.when(position < tiles - 2)
        def _():
            await_piece(jnp.where(position % 2 == 0, tile + 1, tile - 1))

    def first_faces(position):
        tile = tile_at(position)
        for copy in first_loads(tile):
            copy.wait()
        collide_faces(0, tile)
        @pl.when(position == 0)
        def _():
            enter()
        for copy in faces(0, tile):
            copy.start()

    def first_inner(position):
        tile = tile_at(position)
        inner_load(tile).wait()
        collide_inner(0, tile)

    def first_part(position):
        @pl.when(jnp.logical_or(position < 2, jnp.logical_and(position >= 4, position < tiles + 2)))
        def _():
            first_faces(jnp.where(position < 2, position, position - 2))
        @pl.when(jnp.logical_or(jnp.logical_and(position >= 2, position < 4), position >= tiles + 2))
        def _():
            first_inner(jnp.where(position < 4, position - 2, position - tiles))
        @pl.when(position == 3)
        def _():
            @pl.when(me_z == 0)
            def _():
                pl.semaphore_wait(barrier, len(beside))
            for copy in all_edges[0]:
                copy.start()

    over(0, 2 * tiles, first_part)

    for step in range(1, STEPS):
        def place(position):
            tile = tile_at(position)
            await_pieces(step - 1, position, tile)
            @pl.when(position == 0)
            def _():
                for copy in all_edges[step - 1]:
                    copy.wait_recv()
            if step >= 2:
                for copy in faces(step - 2, tile):
                    copy.wait_send()
                @pl.when(position == 0)
                def _():
                    for copy in all_edges[step - 2]:
                        copy.wait_send()
            collide_faces(step, tile)
            start_faces(step, position, tile)
            collide_inner(step, tile)
            start_rows(step, position)

        over(0, tiles, place)

    last = STEPS - 1
    for copy in all_edges[last]:
        copy.wait_recv()
    over(0, tiles, lambda tile: over(1, ny - 1, lambda y: finish_tile(y, tile)))

    def finish_faces(position):
        tile = tile_at(position)
        await_pieces(last, position, tile)
        over(0, 2, lambda index: finish_tile(index * (ny - 1), tile))

    over(0, tiles, finish_faces)

    def await_sends(tile):
        for step in (last - 1, last):
            for copy in faces(step, tile):
                copy.wait_send()

    over(0, tiles, await_sends)
    for step in (last - 1, last):
        for copy in all_edges[step]:
            copy.wait_send()


def output_kernel(final_in, density_in, velocity_in, final_ref, density_ref, velocity_ref, final_sem, moment_sem):
    copies = [pltpu.make_async_copy(final_in.at[pop_id], final_ref.at[pop_id], final_sem.at[pop_id]) for pop_id in range(19)]
    copies.append(pltpu.make_async_copy(density_in, density_ref, moment_sem.at[0]))
    copies.append(pltpu.make_async_copy(velocity_in, velocity_ref, moment_sem.at[1]))
    for copy in copies:
        copy.start()
    for copy in copies:
        copy.wait()


def solution(mesh):
    size_y = mesh.shape["py"]
    size_z = mesh.shape["pz"]
    field_spec = P(None, None, "py", "pz")

    def local_steps(populations, relax_time, body_force):
        field = jnp.transpose(populations, (0, 2, 3, 1))
        _, ny, nz, nx = field.shape
        tau = jnp.reshape(relax_time, (1,))
        state_shape = (19, ny + 2, 2, nz + 2 * ROWS, LANES)
        vmem = pl.BlockSpec(memory_space=pltpu.VMEM)
        anywhere = pl.BlockSpec(memory_space=pl.ANY)
        results = pl.pallas_call(
            functools.partial(step_kernel, size_y, size_z, ny, nz),
            name="lattice_steps",
            out_shape=(
                pltpu.VMEM((19, ny, nz, nx), jnp.float32),
                pltpu.VMEM((ny, nz, nx), jnp.float32),
                pltpu.VMEM((3, ny, nz, nx), jnp.float32),
            ),
            in_specs=[anywhere, anywhere, anywhere],
            out_specs=(vmem, vmem, vmem),
            scratch_shapes=[
                pltpu.VMEM(state_shape, jnp.float32),
                pltpu.VMEM(state_shape, jnp.float32),
                pltpu.SMEM((1,), jnp.float32),
                pltpu.SMEM((3,), jnp.float32),
                pltpu.SemaphoreType.DMA((2,)),
                pltpu.SemaphoreType.DMA((nz // ROWS,)),
                pltpu.SemaphoreType.DMA((2, nz // ROWS)),
                pltpu.SemaphoreType.DMA((2, 2, nz // ROWS)),
                pltpu.SemaphoreType.DMA((2, 2, nz // ROWS)),
                pltpu.SemaphoreType.DMA((2, EDGE_COPIES)),
                pltpu.SemaphoreType.DMA((2, EDGE_COPIES)),
            ],
            compiler_params=pltpu.CompilerParams(collective_id=0, has_side_effects=True, vmem_limit_bytes=46 * 2**20),
        )(tau, body_force, field)
        final, density, velocity = pl.pallas_call(
            output_kernel,
            name="lattice_output",
            out_shape=tuple(jax.ShapeDtypeStruct(result.shape, result.dtype) for result in results),
            in_specs=[vmem, vmem, vmem],
            out_specs=(anywhere, anywhere, anywhere),
            scratch_shapes=[pltpu.SemaphoreType.DMA((19,)), pltpu.SemaphoreType.DMA((2,))],
            compiler_params=pltpu.CompilerParams(vmem_limit_bytes=2**20),
        )(*results)
        return jnp.transpose(final, (0, 3, 1, 2)), jnp.transpose(density, (2, 0, 1)), jnp.transpose(velocity, (0, 3, 1, 2))

    return jax.shard_map(local_steps, mesh=mesh, in_specs=(field_spec, P(), P()), out_specs=(field_spec, P(None, "py", "pz"), field_spec), check_vma=False)
```

```python
import functools

import jax
import jax.numpy as jnp
from jax import lax
from jax.experimental import pallas as pl
from jax.experimental.pallas import tpu as pltpu
from jax.sharding import PartitionSpec as P

STEPS = 4
VELOCITIES = ((0, 0, 0), (1, 0, 0), (-1, 0, 0), (0, 1, 0), (0, -1, 0), (0, 0, 1), (0, 0, -1), (1, 1, 0), (-1, -1, 0), (1, -1, 0), (-1, 1, 0), (1, 0, 1), (-1, 0, -1), (1, 0, -1), (-1, 0, 1), (0, 1, 1), (0, -1, -1), (0, 1, -1), (0, -1, 1))
ORDER = (17, 3, 7, 10, 15, 5, 11, 14, 18, 4, 8, 9, 16, 6, 12, 13, 0, 1, 2)
SLOT = {pop_id: slot for slot, pop_id in enumerate(ORDER)}
MESH = pl.DeviceIdType.MESH
LANES = 128
ROWS = 8
EDGE_COPIES = 7


def moment_sums(load):
    rest = load(0)
    total = rest
    diff = {}
    for plus in range(1, 19, 2):
        upper, lower = load(plus), load(plus + 1)
        total = total + (upper + lower)
        diff[plus] = upper - lower
    mom_x = (diff[1] + diff[7]) + (diff[9] + (diff[11] + diff[13]))
    mom_y = (diff[3] + diff[7]) - (diff[9] - (diff[15] + diff[17]))
    mom_z = (diff[5] + diff[11]) - (diff[13] - (diff[15] - diff[17]))
    return total, (mom_x, mom_y, mom_z)


def tile_terms(load, force, rate36):
    density, momentum = moment_sums(load)
    inverse = 1.0 / density
    half = [(momentum[axis] + force[axis]) * inverse * 1.5 for axis in range(3)]
    square = half[0] * half[0] + half[1] * half[1] + half[2] * half[2]
    scale = density * rate36
    even = scale * (1.0 - square * (2.0 / 3.0))
    twice = scale + scale
    odd = [twice * half[axis] for axis in range(3)]
    return even, odd, half


def relaxed(load, terms, keep, plus):
    even, odd, half = terms
    axes = [(axis, shift) for axis, shift in enumerate(VELOCITIES[plus]) if shift != 0]
    if len(axes) == 1:
        axis = axes[0][0]
        odd_part = odd[axis] + odd[axis]
        even_part = (even + even) + odd_part * half[axis]
    else:
        (first, _), (second, sign) = axes
        if sign > 0:
            odd_part = odd[first] + odd[second]
            projection = half[first] + half[second]
        else:
            odd_part = odd[first] - odd[second]
            projection = half[first] - half[second]
        even_part = even + odd_part * projection
    return load(plus) * keep + (even_part + odd_part), load(plus + 1) * keep + (even_part - odd_part)


def rolled(halves, shift, lane):
    if shift == 0:
        return halves
    moved = [pltpu.roll(part, shift % LANES, 1) for part in halves]
    edge = lane == (0 if shift > 0 else LANES - 1)
    return [jnp.where(edge, moved[1], moved[0]), jnp.where(edge, moved[0], moved[1])]


def step_kernel(size_y, size_z, ny, nz, tau_in, force_in, field_ref, stage, density_ref, velocity_ref, buffer_0, buffer_1, tau_ref, force_ref, param_sem, load_sem, first_sem, face_send, face_recv, edge_send, edge_recv):
    me_y, me_z = lax.axis_index("py"), lax.axis_index("pz")
    up_y, down_y = lax.rem(me_y + 1, size_y), lax.rem(me_y + size_y - 1, size_y)
    up_z, down_z = lax.rem(me_z + 1, size_z), lax.rem(me_z + size_z - 1, size_z)

    def device(dev_y, dev_z):
        return {"py": dev_y, "pz": dev_z}

    barrier = pltpu.get_barrier_semaphore()
    beside = [(dev_y, dev_z) for dev_z in (down_z, up_z) for dev_y in (down_y, me_y, up_y)]

    def signal(dev_y, dev_z):
        pl.semaphore_signal(barrier, inc=1, device_id=device(dev_y, dev_z), device_id_type=MESH)

    signal(up_y, me_z)
    signal(down_y, me_z)
    for dev_y, dev_z in beside:
        @pl.when(jnp.logical_and(me_z != 0, dev_z != 0))
        def _():
            signal(dev_y, dev_z)

    def enter():
        @pl.when(me_z == 0)
        def _():
            pl.semaphore_wait(barrier, 2)
        @pl.when(me_z != 0)
        def _():
            pl.semaphore_wait(barrier, 2 + len(beside))
        for dev_y, dev_z in beside:
            @pl.when(jnp.logical_or(me_z == 0, dev_z == 0))
            def _():
                signal(dev_y, dev_z)

    tiles = nz // ROWS
    params = [pltpu.make_async_copy(tau_in, tau_ref, param_sem.at[0]), pltpu.make_async_copy(force_in, force_ref, param_sem.at[1])]
    for copy in params:
        copy.start()

    def first_loads(tile):
        rows = pl.ds(pl.multiple_of(tile * ROWS, ROWS), ROWS)
        return [pltpu.make_async_copy(field_ref.at[:, y, rows], stage.at[:, y, rows], first_sem.at[face, tile]) for face, y in enumerate((0, ny - 1))]

    def inner_load(tile):
        rows = pl.ds(pl.multiple_of(tile * ROWS, ROWS), ROWS)
        planes = pl.ds(1, ny - 2)
        return pltpu.make_async_copy(field_ref.at[:, planes, rows], stage.at[:, planes, rows], load_sem.at[tile])

    def outwards(position):
        return tiles // 2 - 1 - position // 2 if position % 2 == 0 else tiles // 2 + position // 2

    for position in range(tiles):
        for copy in first_loads(outwards(position)):
            copy.start()
    for position in range(tiles):
        inner_load(outwards(tiles - 1 - position)).start()
    for copy in params:
        copy.wait()

    tau = jnp.full((ROWS, LANES), tau_ref[0], jnp.float32)
    rate = 1.0 / tau
    keep = 1.0 - rate
    rate36 = rate * (1.0 / 36.0)
    force = [tau * force_ref[axis] for axis in range(3)]
    lane = lax.broadcasted_iota(jnp.int32, (ROWS, LANES), 1)
    buffers = (buffer_0, buffer_1)

    def collide_tile(step, y, tile):
        row = pl.multiple_of(tile * ROWS, ROWS)
        target = buffers[step % 2]
        source = buffers[(step + 1) % 2]

        def load(half, pop_id):
            if step == 0:
                return stage[pop_id, y, pl.ds(row, ROWS), pl.ds(half * LANES, LANES)]
            _, shift_y, shift_z = VELOCITIES[pop_id]
            return source[SLOT[pop_id], y + 1 - shift_y, half, pl.ds(row + (ROWS - shift_z), ROWS), :]

        def store(pop_id, halves):
            halves = rolled(halves, VELOCITIES[pop_id][0], lane)
            for half in range(2):
                target[SLOT[pop_id], y + 1, half, pl.ds(row + ROWS, ROWS), :] = halves[half]

        loaders = [functools.partial(load, half) for half in range(2)]
        terms = [tile_terms(loaders[half], force, rate36) for half in range(2)]
        store(0, [loaders[half](0) * keep + terms[half][0] * 12.0 for half in range(2)])
        for plus in range(1, 19, 2):
            pairs = [relaxed(loaders[half], terms[half], keep, plus) for half in range(2)]
            store(plus, [pair[0] for pair in pairs])
            store(plus + 1, [pair[1] for pair in pairs])

    def faces(step, tile):
        state, parity = buffers[step % 2], step % 2
        rows = pl.ds(pl.multiple_of(tile * ROWS + ROWS, ROWS), ROWS)
        result = []
        for face, (slots, source, target, dev_y) in enumerate(((pl.ds(0, 5), ny, 0, up_y), (pl.ds(8, 5), 1, ny + 1, down_y))):
            result.append(pltpu.make_async_remote_copy(
                src_ref=state.at[slots, source, :, rows, :], dst_ref=state.at[slots, target, :, rows, :],
                send_sem=face_send.at[parity, face, tile], recv_sem=face_recv.at[parity, face, tile],
                device_id=device(dev_y, me_z), device_id_type=MESH))
        return result

    def edges(step):
        state, parity = buffers[step % 2], step % 2
        planes = pl.ds(1, ny)
        low, high, below, above = (pl.ds(row, 1) for row in (ROWS, ROWS + nz - 1, ROWS - 1, ROWS + nz))
        parts = (
            (0, ny, low, 0, above, up_y, down_z),
            (12, 1, low, ny + 1, above, down_y, down_z),
            (pl.ds(12, 4), planes, low, planes, above, me_y, down_z),
            (0, planes, low, planes, above, me_y, down_z),
            (4, ny, high, 0, below, up_y, up_z),
            (8, 1, high, ny + 1, below, down_y, up_z),
            (pl.ds(4, 5), planes, high, planes, below, me_y, up_z),
        )
        return [pltpu.make_async_remote_copy(
            src_ref=state.at[slots, source, :, source_row, :], dst_ref=state.at[slots, target, :, target_row, :],
            send_sem=edge_send.at[parity, number], recv_sem=edge_recv.at[parity, number],
            device_id=device(dev_y, dev_z), device_id_type=MESH)
            for number, (slots, source, source_row, target, target_row, dev_y, dev_z) in enumerate(parts)]

    def over(start, stop, body, unroll=False):
        def run(index, carry):
            body(index)
            return carry
        lax.fori_loop(start, stop, run, 0, unroll=unroll)

    def finish_tile(y, tile):
        row = pl.multiple_of(tile * ROWS, ROWS)
        source = buffers[(STEPS - 1) % 2]
        for half in range(2):
            place = (y, pl.ds(row, ROWS), pl.ds(half * LANES, LANES))

            def load(pop_id):
                _, shift_y, shift_z = VELOCITIES[pop_id]
                value = source[SLOT[pop_id], y + 1 - shift_y, half, pl.ds(row + (ROWS - shift_z), ROWS), :]
                stage[(pop_id, *place)] = value
                return value

            density, momentum = moment_sums(load)
            density_ref[place] = density
            for axis in range(3):
                velocity_ref[(axis, *place)] = (momentum[axis] + force[axis]) / density

    def tile_at(position):
        return jnp.where(position % 2 == 0, tiles // 2 - 1 - position // 2, tiles // 2 + position // 2)

    def at_position(position, number, copies):
        @pl.when(position == number)
        def _():
            for copy in copies:
                copy.start()

    all_edges = [edges(step) for step in range(STEPS)]

    def collide_faces(step, tile):
        over(0, 2, lambda index: collide_tile(step, index * (ny - 1), tile), True)

    def collide_inner(step, tile):
        over(1, ny - 1, lambda index: collide_tile(step, index, tile), True)

    def start_faces(step, tile):
        for copy in faces(step, tile):
            copy.start()

    def start_edges(step, position):
        at_position(position, tiles - 2, all_edges[step][:4])
        at_position(position, tiles - 1, all_edges[step][4:])

    def await_pieces(step, position, tile):
        def await_piece(number):
            for copy in faces(step, number):
                copy.wait_recv()

        @pl.when(position == 0)
        def _():
            await_piece(tile)
            await_piece(tile + 1)
        @pl.when(position < tiles - 2)
        def _():
            await_piece(jnp.where(position % 2 == 0, tile - 1, tile + 1))

    def first_faces(position):
        tile = tile_at(position)
        for copy in first_loads(tile):
            copy.wait()
        collide_faces(0, tile)
        @pl.when(position == 0)
        def _():
            enter()
        for copy in faces(0, tile):
            copy.start()

    def first_inner(position):
        tile = tile_at(tiles - 1 - position)
        inner_load(tile).wait()
        collide_inner(0, tile)
        @pl.when(jnp.logical_and(position == 1, me_z != 0))
        def _():
            for copy in all_edges[0]:
                copy.start()

    over(0, tiles, first_faces)
    over(0, tiles, first_inner)

    @pl.when(me_z == 0)
    def _():
        pl.semaphore_wait(barrier, len(beside))
        for copy in all_edges[0]:
            copy.start()

    for step in range(1, STEPS):
        def place(position):
            tile = tile_at(position)
            await_pieces(step - 1, position, tile)
            @pl.when(position == tiles - 2)
            def _():
                for copy in all_edges[step - 1]:
                    copy.wait_recv()
            if step >= 2:
                for copy in faces(step - 2, tile):
                    copy.wait_send()
                @pl.when(position == tiles - 2)
                def _():
                    for copy in all_edges[step - 2]:
                        copy.wait_send()
            collide_faces(step, tile)
            start_faces(step, tile)
            collide_inner(step, tile)
            start_edges(step, position)

        over(0, tiles, place)

    last = STEPS - 1
    def finish_inner(position):
        @pl.when(position == tiles - 2)
        def _():
            for copy in all_edges[last]:
                copy.wait_recv()
        tile = tile_at(position)
        over(1, ny - 1, lambda y: finish_tile(y, tile))

    over(0, tiles, finish_inner)

    def finish_faces(position):
        tile = tile_at(position)
        await_pieces(last, position, tile)
        over(0, 2, lambda index: finish_tile(index * (ny - 1), tile))

    over(0, tiles, finish_faces)

    def await_sends(tile):
        for step in (last - 1, last):
            for copy in faces(step, tile):
                copy.wait_send()

    over(0, tiles, await_sends)
    for step in (last - 1, last):
        for copy in all_edges[step]:
            copy.wait_send()


def output_kernel(final_in, density_in, velocity_in, final_ref, density_ref, velocity_ref, final_sem, moment_sem):
    copies = [pltpu.make_async_copy(final_in.at[pop_id], final_ref.at[pop_id], final_sem.at[pop_id]) for pop_id in range(19)]
    copies.append(pltpu.make_async_copy(density_in, density_ref, moment_sem.at[0]))
    copies.append(pltpu.make_async_copy(velocity_in, velocity_ref, moment_sem.at[1]))
    for copy in copies:
        copy.start()
    for copy in copies:
        copy.wait()


def solution(mesh):
    size_y = mesh.shape["py"]
    size_z = mesh.shape["pz"]
    field_spec = P(None, None, "py", "pz")

    def local_steps(populations, relax_time, body_force):
        field = jnp.transpose(populations, (0, 2, 3, 1))
        _, ny, nz, nx = field.shape
        tau = jnp.reshape(relax_time, (1,))
        state_shape = (19, ny + 2, 2, nz + 2 * ROWS, LANES)
        vmem = pl.BlockSpec(memory_space=pltpu.VMEM)
        anywhere = pl.BlockSpec(memory_space=pl.ANY)
        results = pl.pallas_call(
            functools.partial(step_kernel, size_y, size_z, ny, nz),
            name="lattice_steps",
            out_shape=(
                pltpu.VMEM((19, ny, nz, nx), jnp.float32),
                pltpu.VMEM((ny, nz, nx), jnp.float32),
                pltpu.VMEM((3, ny, nz, nx), jnp.float32),
            ),
            in_specs=[anywhere, anywhere, anywhere],
            out_specs=(vmem, vmem, vmem),
            scratch_shapes=[
                pltpu.VMEM(state_shape, jnp.float32),
                pltpu.VMEM(state_shape, jnp.float32),
                pltpu.SMEM((1,), jnp.float32),
                pltpu.SMEM((3,), jnp.float32),
                pltpu.SemaphoreType.DMA((2,)),
                pltpu.SemaphoreType.DMA((nz // ROWS,)),
                pltpu.SemaphoreType.DMA((2, nz // ROWS)),
                pltpu.SemaphoreType.DMA((2, 2, nz // ROWS)),
                pltpu.SemaphoreType.DMA((2, 2, nz // ROWS)),
                pltpu.SemaphoreType.DMA((2, EDGE_COPIES)),
                pltpu.SemaphoreType.DMA((2, EDGE_COPIES)),
            ],
            compiler_params=pltpu.CompilerParams(collective_id=0, has_side_effects=True, vmem_limit_bytes=46 * 2**20),
        )(tau, body_force, field)
        final, density, velocity = pl.pallas_call(
            output_kernel,
            name="lattice_output",
            out_shape=tuple(jax.ShapeDtypeStruct(result.shape, result.dtype) for result in results),
            in_specs=[vmem, vmem, vmem],
            out_specs=(anywhere, anywhere, anywhere),
            scratch_shapes=[pltpu.SemaphoreType.DMA((19,)), pltpu.SemaphoreType.DMA((2,))],
            compiler_params=pltpu.CompilerParams(vmem_limit_bytes=2**20),
        )(*results)
        return jnp.transpose(final, (0, 3, 1, 2)), jnp.transpose(density, (2, 0, 1)), jnp.transpose(velocity, (0, 3, 1, 2))

    return jax.shard_map(local_steps, mesh=mesh, in_specs=(field_spec, P(), P()), out_specs=(field_spec, P(None, "py", "pz"), field_spec), check_vma=False)
```

```python
import functools

import jax
import jax.numpy as jnp
from jax import lax
from jax.experimental import pallas as pl
from jax.experimental.pallas import tpu as pltpu
from jax.sharding import PartitionSpec as P

STEPS = 4
VELOCITIES = ((0, 0, 0), (1, 0, 0), (-1, 0, 0), (0, 1, 0), (0, -1, 0), (0, 0, 1), (0, 0, -1), (1, 1, 0), (-1, -1, 0), (1, -1, 0), (-1, 1, 0), (1, 0, 1), (-1, 0, -1), (1, 0, -1), (-1, 0, 1), (0, 1, 1), (0, -1, -1), (0, 1, -1), (0, -1, 1))
ORDER = (17, 3, 7, 10, 15, 5, 11, 14, 18, 4, 8, 9, 16, 6, 12, 13, 0, 1, 2)
SLOT = {pop_id: slot for slot, pop_id in enumerate(ORDER)}
MESH = pl.DeviceIdType.MESH
LANES = 128
ROWS = 8
EDGE_COPIES = 7


def moment_sums(load):
    rest = load(0)
    total = rest
    diff = {}
    for plus in range(1, 19, 2):
        upper, lower = load(plus), load(plus + 1)
        total = total + (upper + lower)
        diff[plus] = upper - lower
    mom_x = (diff[1] + diff[7]) + (diff[9] + (diff[11] + diff[13]))
    mom_y = (diff[3] + diff[7]) - (diff[9] - (diff[15] + diff[17]))
    mom_z = (diff[5] + diff[11]) - (diff[13] - (diff[15] - diff[17]))
    return total, (mom_x, mom_y, mom_z)


def tile_terms(load, force, rate36):
    density, momentum = moment_sums(load)
    inverse = 1.0 / density
    half = [(momentum[axis] + force[axis]) * inverse * 1.5 for axis in range(3)]
    square = half[0] * half[0] + half[1] * half[1] + half[2] * half[2]
    scale = density * rate36
    even = scale * (1.0 - square * (2.0 / 3.0))
    twice = scale + scale
    odd = [twice * half[axis] for axis in range(3)]
    return even, odd, half


def relaxed(load, terms, keep, plus):
    even, odd, half = terms
    axes = [(axis, shift) for axis, shift in enumerate(VELOCITIES[plus]) if shift != 0]
    if len(axes) == 1:
        axis = axes[0][0]
        odd_part = odd[axis] + odd[axis]
        even_part = (even + even) + odd_part * half[axis]
    else:
        (first, _), (second, sign) = axes
        if sign > 0:
            odd_part = odd[first] + odd[second]
            projection = half[first] + half[second]
        else:
            odd_part = odd[first] - odd[second]
            projection = half[first] - half[second]
        even_part = even + odd_part * projection
    return load(plus) * keep + (even_part + odd_part), load(plus + 1) * keep + (even_part - odd_part)


def rolled(halves, shift, lane):
    if shift == 0:
        return halves
    moved = [pltpu.roll(part, shift % LANES, 1) for part in halves]
    edge = lane == (0 if shift > 0 else LANES - 1)
    return [jnp.where(edge, moved[1], moved[0]), jnp.where(edge, moved[0], moved[1])]


def step_kernel(size_y, size_z, ny, nz, tau_in, force_in, field_ref, stage, density_ref, velocity_ref, buffer_0, buffer_1, tau_ref, force_ref, param_sem, load_sem, first_sem, face_send, face_recv, edge_send, edge_recv):
    me_y, me_z = lax.axis_index("py"), lax.axis_index("pz")
    up_y, down_y = lax.rem(me_y + 1, size_y), lax.rem(me_y + size_y - 1, size_y)
    up_z, down_z = lax.rem(me_z + 1, size_z), lax.rem(me_z + size_z - 1, size_z)

    def device(dev_y, dev_z):
        return {"py": dev_y, "pz": dev_z}

    barrier = pltpu.get_barrier_semaphore()
    beside = [(dev_y, dev_z) for dev_z in (down_z, up_z) for dev_y in (down_y, me_y, up_y)]

    def signal(dev_y, dev_z):
        pl.semaphore_signal(barrier, inc=1, device_id=device(dev_y, dev_z), device_id_type=MESH)

    signal(up_y, me_z)
    signal(down_y, me_z)
    for dev_y, dev_z in beside:
        @pl.when(jnp.logical_and(me_z != 0, dev_z != 0))
        def _():
            signal(dev_y, dev_z)

    def enter(count, needs_signal):
        pl.semaphore_wait(barrier, count)
        for dev_y, dev_z in beside:
            @pl.when(needs_signal(dev_z))
            def _():
                signal(dev_y, dev_z)

    tiles = nz // ROWS
    params = [pltpu.make_async_copy(tau_in, tau_ref, param_sem.at[0]), pltpu.make_async_copy(force_in, force_ref, param_sem.at[1])]
    for copy in params:
        copy.start()

    def first_loads(tile):
        rows = pl.ds(pl.multiple_of(tile * ROWS, ROWS), ROWS)
        return [pltpu.make_async_copy(field_ref.at[:, y, rows], stage.at[:, y, rows], first_sem.at[face, tile]) for face, y in enumerate((0, ny - 1))]

    def inner_load(tile):
        rows = pl.ds(pl.multiple_of(tile * ROWS, ROWS), ROWS)
        planes = pl.ds(1, ny - 2)
        return pltpu.make_async_copy(field_ref.at[:, planes, rows], stage.at[:, planes, rows], load_sem.at[tile])

    order = [position // 2 if position % 2 == 0 else tiles - 1 - position // 2 for position in range(tiles)]
    for positions in (order[:2], order[2:]):
        for tile in positions:
            for copy in first_loads(tile):
                copy.start()
        for tile in positions:
            inner_load(tile).start()
    for copy in params:
        copy.wait()

    tau = jnp.full((ROWS, LANES), tau_ref[0], jnp.float32)
    rate = 1.0 / tau
    keep = 1.0 - rate
    rate36 = rate * (1.0 / 36.0)
    force = [tau * force_ref[axis] for axis in range(3)]
    lane = lax.broadcasted_iota(jnp.int32, (ROWS, LANES), 1)
    buffers = (buffer_0, buffer_1)

    def collide_tile(step, y, tile):
        row = pl.multiple_of(tile * ROWS, ROWS)
        target = buffers[step % 2]
        source = buffers[(step + 1) % 2]

        def load(half, pop_id):
            if step == 0:
                return stage[pop_id, y, pl.ds(row, ROWS), pl.ds(half * LANES, LANES)]
            _, shift_y, shift_z = VELOCITIES[pop_id]
            return source[SLOT[pop_id], y + 1 - shift_y, half, pl.ds(row + (ROWS - shift_z), ROWS), :]

        def store(pop_id, halves):
            halves = rolled(halves, VELOCITIES[pop_id][0], lane)
            for half in range(2):
                target[SLOT[pop_id], y + 1, half, pl.ds(row + ROWS, ROWS), :] = halves[half]

        loaders = [functools.partial(load, half) for half in range(2)]
        terms = [tile_terms(loaders[half], force, rate36) for half in range(2)]
        store(0, [loaders[half](0) * keep + terms[half][0] * 12.0 for half in range(2)])
        for plus in range(1, 19, 2):
            pairs = [relaxed(loaders[half], terms[half], keep, plus) for half in range(2)]
            store(plus, [pair[0] for pair in pairs])
            store(plus + 1, [pair[1] for pair in pairs])

    def faces(step, tile):
        state, parity = buffers[step % 2], step % 2
        rows = pl.ds(pl.multiple_of(tile * ROWS + ROWS, ROWS), ROWS)
        result = []
        for face, (slots, source, target, dev_y) in enumerate(((pl.ds(0, 5), ny, 0, up_y), (pl.ds(8, 5), 1, ny + 1, down_y))):
            result.append(pltpu.make_async_remote_copy(
                src_ref=state.at[slots, source, :, rows, :], dst_ref=state.at[slots, target, :, rows, :],
                send_sem=face_send.at[parity, face, tile], recv_sem=face_recv.at[parity, face, tile],
                device_id=device(dev_y, me_z), device_id_type=MESH))
        return result

    def edges(step):
        state, parity = buffers[step % 2], step % 2
        planes = pl.ds(1, ny)
        low, high, below, above = (pl.ds(row, 1) for row in (ROWS, ROWS + nz - 1, ROWS - 1, ROWS + nz))
        parts = (
            (0, ny, low, 0, above, up_y, down_z),
            (12, 1, low, ny + 1, above, down_y, down_z),
            (pl.ds(12, 4), planes, low, planes, above, me_y, down_z),
            (0, planes, low, planes, above, me_y, down_z),
            (4, ny, high, 0, below, up_y, up_z),
            (8, 1, high, ny + 1, below, down_y, up_z),
            (pl.ds(4, 5), planes, high, planes, below, me_y, up_z),
        )
        return [pltpu.make_async_remote_copy(
            src_ref=state.at[slots, source, :, source_row, :], dst_ref=state.at[slots, target, :, target_row, :],
            send_sem=edge_send.at[parity, number], recv_sem=edge_recv.at[parity, number],
            device_id=device(dev_y, dev_z), device_id_type=MESH)
            for number, (slots, source, source_row, target, target_row, dev_y, dev_z) in enumerate(parts)]

    def over(start, stop, body, unroll=False):
        def run(index, carry):
            body(index)
            return carry
        lax.fori_loop(start, stop, run, 0, unroll=unroll)

    def finish_tile(y, tile):
        row = pl.multiple_of(tile * ROWS, ROWS)
        source = buffers[(STEPS - 1) % 2]
        for half in range(2):
            place = (y, pl.ds(row, ROWS), pl.ds(half * LANES, LANES))

            def load(pop_id):
                _, shift_y, shift_z = VELOCITIES[pop_id]
                value = source[SLOT[pop_id], y + 1 - shift_y, half, pl.ds(row + (ROWS - shift_z), ROWS), :]
                stage[(pop_id, *place)] = value
                return value

            density, momentum = moment_sums(load)
            density_ref[place] = density
            for axis in range(3):
                velocity_ref[(axis, *place)] = (momentum[axis] + force[axis]) / density

    def tile_at(position):
        return jnp.where(position % 2 == 0, position // 2, tiles - 1 - position // 2)

    def at_position(position, number, copies):
        @pl.when(position == number)
        def _():
            for copy in copies:
                copy.start()

    all_edges = [edges(step) for step in range(STEPS)]

    def collide_faces(step, tile):
        over(0, 2, lambda index: collide_tile(step, index * (ny - 1), tile), True)

    def collide_inner(step, tile):
        over(1, ny - 1, lambda index: collide_tile(step, index, tile), True)

    def start_faces(step, position, tile):
        at_position(position, 0, all_edges[step][0:2])
        at_position(position, 1, all_edges[step][4:6])
        for copy in faces(step, tile):
            copy.start()

    def start_rows(step, position):
        at_position(position, 0, all_edges[step][2:4])
        at_position(position, 1, all_edges[step][6:7])

    def await_pieces(step, position, tile):
        def await_piece(number):
            for copy in faces(step, number):
                copy.wait_recv()

        @pl.when(position < 2)
        def _():
            await_piece(tile)
        @pl.when(position < tiles - 2)
        def _():
            await_piece(jnp.where(position % 2 == 0, tile + 1, tile - 1))

    def first_faces(position):
        tile = tile_at(position)
        for copy in first_loads(tile):
            copy.wait()
        collide_faces(0, tile)
        @pl.when(jnp.logical_and(position == 0, me_z != 0))
        def _():
            enter(2 + len(beside), lambda dev_z: dev_z == 0)
        for copy in faces(0, tile):
            copy.start()

    def first_inner(position):
        tile = tile_at(position)
        inner_load(tile).wait()
        collide_inner(0, tile)

    split = jnp.where(me_z == 0, tiles, 2)

    def first_part(number):
        early = number < 2 * split
        local = jnp.where(early, number, number - 2 * split)
        length = jnp.where(early, split, tiles - split)
        position = jnp.where(early, 0, split) + jnp.where(local < length, local, local - length)
        @pl.when(local < length)
        def _():
            first_faces(position)
        @pl.when(local >= length)
        def _():
            first_inner(position)
        @pl.when(jnp.logical_and(number == 3, me_z != 0))
        def _():
            for copy in all_edges[0]:
                copy.start()

    @pl.when(me_z == 0)
    def _():
        enter(2, lambda dev_z: dev_z != me_z)

    over(0, 2 * tiles, first_part)

    @pl.when(me_z == 0)
    def _():
        pl.semaphore_wait(barrier, len(beside))
        for copy in all_edges[0]:
            copy.start()

    for step in range(1, STEPS):
        def place(position):
            tile = tile_at(position)
            await_pieces(step - 1, position, tile)
            @pl.when(position == 0)
            def _():
                for copy in all_edges[step - 1]:
                    copy.wait_recv()
            if step >= 2:
                for copy in faces(step - 2, tile):
                    copy.wait_send()
                @pl.when(position == 0)
                def _():
                    for copy in all_edges[step - 2]:
                        copy.wait_send()
            collide_faces(step, tile)
            start_faces(step, position, tile)
            collide_inner(step, tile)
            start_rows(step, position)

        over(0, tiles, place)

    last = STEPS - 1
    def finish_inner(position):
        @pl.when(position == tiles - 2)
        def _():
            for copy in all_edges[last]:
                copy.wait_recv()
        tile = tile_at(tiles - 1 - position)
        over(1, ny - 1, lambda y: finish_tile(y, tile))

    over(0, tiles, finish_inner)

    def finish_faces(position):
        tile = tile_at(position)
        await_pieces(last, position, tile)
        over(0, 2, lambda index: finish_tile(index * (ny - 1), tile))

    over(0, tiles, finish_faces)

    def await_sends(tile):
        for step in (last - 1, last):
            for copy in faces(step, tile):
                copy.wait_send()

    over(0, tiles, await_sends)
    for step in (last - 1, last):
        for copy in all_edges[step]:
            copy.wait_send()


def output_kernel(final_in, density_in, velocity_in, final_ref, density_ref, velocity_ref, final_sem, moment_sem):
    copies = [pltpu.make_async_copy(final_in.at[pop_id], final_ref.at[pop_id], final_sem.at[pop_id]) for pop_id in range(19)]
    copies.append(pltpu.make_async_copy(density_in, density_ref, moment_sem.at[0]))
    copies.append(pltpu.make_async_copy(velocity_in, velocity_ref, moment_sem.at[1]))
    for copy in copies:
        copy.start()
    for copy in copies:
        copy.wait()


def solution(mesh):
    size_y = mesh.shape["py"]
    size_z = mesh.shape["pz"]
    field_spec = P(None, None, "py", "pz")

    def local_steps(populations, relax_time, body_force):
        field = jnp.transpose(populations, (0, 2, 3, 1))
        _, ny, nz, nx = field.shape
        tau = jnp.reshape(relax_time, (1,))
        state_shape = (19, ny + 2, 2, nz + 2 * ROWS, LANES)
        vmem = pl.BlockSpec(memory_space=pltpu.VMEM)
        anywhere = pl.BlockSpec(memory_space=pl.ANY)
        results = pl.pallas_call(
            functools.partial(step_kernel, size_y, size_z, ny, nz),
            name="lattice_steps",
            out_shape=(
                pltpu.VMEM((19, ny, nz, nx), jnp.float32),
                pltpu.VMEM((ny, nz, nx), jnp.float32),
                pltpu.VMEM((3, ny, nz, nx), jnp.float32),
            ),
            in_specs=[anywhere, anywhere, anywhere],
            out_specs=(vmem, vmem, vmem),
            scratch_shapes=[
                pltpu.VMEM(state_shape, jnp.float32),
                pltpu.VMEM(state_shape, jnp.float32),
                pltpu.SMEM((1,), jnp.float32),
                pltpu.SMEM((3,), jnp.float32),
                pltpu.SemaphoreType.DMA((2,)),
                pltpu.SemaphoreType.DMA((nz // ROWS,)),
                pltpu.SemaphoreType.DMA((2, nz // ROWS)),
                pltpu.SemaphoreType.DMA((2, 2, nz // ROWS)),
                pltpu.SemaphoreType.DMA((2, 2, nz // ROWS)),
                pltpu.SemaphoreType.DMA((2, EDGE_COPIES)),
                pltpu.SemaphoreType.DMA((2, EDGE_COPIES)),
            ],
            compiler_params=pltpu.CompilerParams(collective_id=0, has_side_effects=True, vmem_limit_bytes=46 * 2**20),
        )(tau, body_force, field)
        final, density, velocity = pl.pallas_call(
            output_kernel,
            name="lattice_output",
            out_shape=tuple(jax.ShapeDtypeStruct(result.shape, result.dtype) for result in results),
            in_specs=[vmem, vmem, vmem],
            out_specs=(anywhere, anywhere, anywhere),
            scratch_shapes=[pltpu.SemaphoreType.DMA((19,)), pltpu.SemaphoreType.DMA((2,))],
            compiler_params=pltpu.CompilerParams(vmem_limit_bytes=2**20),
        )(*results)
        return jnp.transpose(final, (0, 3, 1, 2)), jnp.transpose(density, (2, 0, 1)), jnp.transpose(velocity, (0, 3, 1, 2))

    return jax.shard_map(local_steps, mesh=mesh, in_specs=(field_spec, P(), P()), out_specs=(field_spec, P(None, "py", "pz"), field_spec), check_vma=False)
```

```python
import functools

import jax
import jax.numpy as jnp
from jax import lax
from jax.experimental import pallas as pl
from jax.experimental.pallas import tpu as pltpu
from jax.sharding import PartitionSpec as P

STEPS = 4
VELOCITIES = ((0, 0, 0), (1, 0, 0), (-1, 0, 0), (0, 1, 0), (0, -1, 0), (0, 0, 1), (0, 0, -1), (1, 1, 0), (-1, -1, 0), (1, -1, 0), (-1, 1, 0), (1, 0, 1), (-1, 0, -1), (1, 0, -1), (-1, 0, 1), (0, 1, 1), (0, -1, -1), (0, 1, -1), (0, -1, 1))
ORDER = (17, 3, 7, 10, 15, 5, 11, 14, 18, 4, 8, 9, 16, 6, 12, 13, 0, 1, 2)
SLOT = {pop_id: slot for slot, pop_id in enumerate(ORDER)}
MESH = pl.DeviceIdType.MESH
LANES = 128
ROWS = 8
EDGE_COPIES = 7


def moment_sums(load):
    rest = load(0)
    total = rest
    diff = {}
    for plus in range(1, 19, 2):
        upper, lower = load(plus), load(plus + 1)
        total = total + (upper + lower)
        diff[plus] = upper - lower
    mom_x = (diff[1] + diff[7]) + (diff[9] + (diff[11] + diff[13]))
    mom_y = (diff[3] + diff[7]) - (diff[9] - (diff[15] + diff[17]))
    mom_z = (diff[5] + diff[11]) - (diff[13] - (diff[15] - diff[17]))
    return total, (mom_x, mom_y, mom_z)


def tile_terms(load, force, rate36):
    density, momentum = moment_sums(load)
    inverse = 1.0 / density
    half = [(momentum[axis] + force[axis]) * inverse * 1.5 for axis in range(3)]
    square = half[0] * half[0] + half[1] * half[1] + half[2] * half[2]
    scale = density * rate36
    even = scale * (1.0 - square * (2.0 / 3.0))
    twice = scale + scale
    odd = [twice * half[axis] for axis in range(3)]
    return even, odd, half


def relaxed(load, terms, keep, plus):
    even, odd, half = terms
    axes = [(axis, shift) for axis, shift in enumerate(VELOCITIES[plus]) if shift != 0]
    if len(axes) == 1:
        axis = axes[0][0]
        odd_part = odd[axis] + odd[axis]
        even_part = (even + even) + odd_part * half[axis]
    else:
        (first, _), (second, sign) = axes
        if sign > 0:
            odd_part = odd[first] + odd[second]
            projection = half[first] + half[second]
        else:
            odd_part = odd[first] - odd[second]
            projection = half[first] - half[second]
        even_part = even + odd_part * projection
    return load(plus) * keep + (even_part + odd_part), load(plus + 1) * keep + (even_part - odd_part)


def rolled(halves, shift, lane):
    if shift == 0:
        return halves
    moved = [pltpu.roll(part, shift % LANES, 1) for part in halves]
    edge = lane == (0 if shift > 0 else LANES - 1)
    return [jnp.where(edge, moved[1], moved[0]), jnp.where(edge, moved[0], moved[1])]


def step_kernel(size_y, size_z, ny, nz, tau_in, force_in, field_ref, stage, density_ref, velocity_ref, buffer_0, buffer_1, tau_ref, force_ref, param_sem, load_sem, first_sem, face_send, face_recv, edge_send, edge_recv):
    me_y, me_z = lax.axis_index("py"), lax.axis_index("pz")
    up_y, down_y = lax.rem(me_y + 1, size_y), lax.rem(me_y + size_y - 1, size_y)
    up_z, down_z = lax.rem(me_z + 1, size_z), lax.rem(me_z + size_z - 1, size_z)

    def device(dev_y, dev_z):
        return {"py": dev_y, "pz": dev_z}

    barrier = pltpu.get_barrier_semaphore()
    beside = [(dev_y, dev_z) for dev_z in (down_z, up_z) for dev_y in (down_y, me_y, up_y)]

    def signal(dev_y, dev_z):
        pl.semaphore_signal(barrier, inc=1, device_id=device(dev_y, dev_z), device_id_type=MESH)

    signal(up_y, me_z)
    signal(down_y, me_z)
    for dev_y, dev_z in beside:
        @pl.when(jnp.logical_and(me_z != 0, dev_z != 0))
        def _():
            signal(dev_y, dev_z)

    def enter(count, needs_signal):
        pl.semaphore_wait(barrier, count)
        for dev_y, dev_z in beside:
            @pl.when(needs_signal(dev_z))
            def _():
                signal(dev_y, dev_z)

    tiles = nz // ROWS
    params = [pltpu.make_async_copy(tau_in, tau_ref, param_sem.at[0]), pltpu.make_async_copy(force_in, force_ref, param_sem.at[1])]
    for copy in params:
        copy.start()

    def first_loads(tile):
        rows = pl.ds(pl.multiple_of(tile * ROWS, ROWS), ROWS)
        return [pltpu.make_async_copy(field_ref.at[:, y, rows], stage.at[:, y, rows], first_sem.at[face, tile]) for face, y in enumerate((0, ny - 1))]

    def inner_load(tile):
        rows = pl.ds(pl.multiple_of(tile * ROWS, ROWS), ROWS)
        planes = pl.ds(1, ny - 2)
        return pltpu.make_async_copy(field_ref.at[:, planes, rows], stage.at[:, planes, rows], load_sem.at[tile])

    order = [position // 2 if position % 2 == 0 else tiles - 1 - position // 2 for position in range(tiles)]
    for positions in (order[:2], order[2:]):
        for tile in positions:
            for copy in first_loads(tile):
                copy.start()
        for tile in positions:
            inner_load(tile).start()
    for copy in params:
        copy.wait()

    tau = jnp.full((ROWS, LANES), tau_ref[0], jnp.float32)
    rate = 1.0 / tau
    keep = 1.0 - rate
    rate36 = rate * (1.0 / 36.0)
    force = [tau * force_ref[axis] for axis in range(3)]
    lane = lax.broadcasted_iota(jnp.int32, (ROWS, LANES), 1)
    buffers = (buffer_0, buffer_1)

    def collide_tile(step, y, tile):
        row = pl.multiple_of(tile * ROWS, ROWS)
        target = buffers[step % 2]
        source = buffers[(step + 1) % 2]

        def load(half, pop_id):
            if step == 0:
                return stage[pop_id, y, pl.ds(row, ROWS), pl.ds(half * LANES, LANES)]
            _, shift_y, shift_z = VELOCITIES[pop_id]
            return source[SLOT[pop_id], y + 1 - shift_y, half, pl.ds(row + (ROWS - shift_z), ROWS), :]

        def store(pop_id, halves):
            halves = rolled(halves, VELOCITIES[pop_id][0], lane)
            for half in range(2):
                target[SLOT[pop_id], y + 1, half, pl.ds(row + ROWS, ROWS), :] = halves[half]

        loaders = [functools.partial(load, half) for half in range(2)]
        terms = [tile_terms(loaders[half], force, rate36) for half in range(2)]
        store(0, [loaders[half](0) * keep + terms[half][0] * 12.0 for half in range(2)])
        for plus in range(1, 19, 2):
            pairs = [relaxed(loaders[half], terms[half], keep, plus) for half in range(2)]
            store(plus, [pair[0] for pair in pairs])
            store(plus + 1, [pair[1] for pair in pairs])

    def faces(step, tile):
        state, parity = buffers[step % 2], step % 2
        rows = pl.ds(pl.multiple_of(tile * ROWS + ROWS, ROWS), ROWS)
        result = []
        for face, (slots, source, target, dev_y) in enumerate(((pl.ds(0, 5), ny, 0, up_y), (pl.ds(8, 5), 1, ny + 1, down_y))):
            result.append(pltpu.make_async_remote_copy(
                src_ref=state.at[slots, source, :, rows, :], dst_ref=state.at[slots, target, :, rows, :],
                send_sem=face_send.at[parity, face, tile], recv_sem=face_recv.at[parity, face, tile],
                device_id=device(dev_y, me_z), device_id_type=MESH))
        return result

    def edges(step):
        state, parity = buffers[step % 2], step % 2
        planes = pl.ds(1, ny)
        low, high, below, above = (pl.ds(row, 1) for row in (ROWS, ROWS + nz - 1, ROWS - 1, ROWS + nz))
        parts = (
            (0, ny, low, 0, above, up_y, down_z),
            (12, 1, low, ny + 1, above, down_y, down_z),
            (pl.ds(12, 4), planes, low, planes, above, me_y, down_z),
            (0, planes, low, planes, above, me_y, down_z),
            (4, ny, high, 0, below, up_y, up_z),
            (8, 1, high, ny + 1, below, down_y, up_z),
            (pl.ds(4, 5), planes, high, planes, below, me_y, up_z),
        )
        return [pltpu.make_async_remote_copy(
            src_ref=state.at[slots, source, :, source_row, :], dst_ref=state.at[slots, target, :, target_row, :],
            send_sem=edge_send.at[parity, number], recv_sem=edge_recv.at[parity, number],
            device_id=device(dev_y, dev_z), device_id_type=MESH)
            for number, (slots, source, source_row, target, target_row, dev_y, dev_z) in enumerate(parts)]

    def over(start, stop, body, unroll=False):
        def run(index, carry):
            body(index)
            return carry
        lax.fori_loop(start, stop, run, 0, unroll=unroll)

    def finish_tile(y, tile):
        row = pl.multiple_of(tile * ROWS, ROWS)
        source = buffers[(STEPS - 1) % 2]
        for half in range(2):
            place = (y, pl.ds(row, ROWS), pl.ds(half * LANES, LANES))

            def load(pop_id):
                _, shift_y, shift_z = VELOCITIES[pop_id]
                value = source[SLOT[pop_id], y + 1 - shift_y, half, pl.ds(row + (ROWS - shift_z), ROWS), :]
                stage[(pop_id, *place)] = value
                return value

            density, momentum = moment_sums(load)
            density_ref[place] = density
            for axis in range(3):
                velocity_ref[(axis, *place)] = (momentum[axis] + force[axis]) / density

    def tile_at(position):
        return jnp.where(position % 2 == 0, position // 2, tiles - 1 - position // 2)

    def at_position(position, number, copies):
        @pl.when(position == number)
        def _():
            for copy in copies:
                copy.start()

    all_edges = [edges(step) for step in range(STEPS)]

    def collide_faces(step, tile):
        over(0, 2, lambda index: collide_tile(step, index * (ny - 1), tile), True)

    def collide_inner(step, tile):
        over(1, ny - 1, lambda index: collide_tile(step, index, tile), True)

    def start_faces(step, position, tile):
        at_position(position, 0, all_edges[step][0:2])
        at_position(position, 1, all_edges[step][4:6])
        for copy in faces(step, tile):
            copy.start()

    def start_rows(step, position):
        at_position(position, 0, all_edges[step][2:4])
        at_position(position, 1, all_edges[step][6:7])

    def await_pieces(step, position, tile):
        def await_piece(number):
            for copy in faces(step, number):
                copy.wait_recv()

        @pl.when(position < 2)
        def _():
            await_piece(tile)
        @pl.when(position < tiles - 2)
        def _():
            await_piece(jnp.where(position % 2 == 0, tile + 1, tile - 1))

    def first_faces(position):
        tile = tile_at(position)
        for copy in first_loads(tile):
            copy.wait()
        collide_faces(0, tile)
        @pl.when(jnp.logical_and(position == 0, me_z != 0))
        def _():
            enter(2 + len(beside), lambda dev_z: dev_z == 0)
        for number, corners in enumerate((all_edges[0][0:2], all_edges[0][4:6])):
            @pl.when(jnp.logical_and(position == number, me_z != 0))
            def _():
                for copy in corners:
                    copy.start()
        for copy in faces(0, tile):
            copy.start()

    def first_inner(position):
        tile = tile_at(position)
        inner_load(tile).wait()
        collide_inner(0, tile)

    split = jnp.where(me_z == 0, tiles // 2, 2)

    def first_part(number):
        early = number < 2 * split
        local = jnp.where(early, number, number - 2 * split)
        length = jnp.where(early, split, tiles - split)
        position = jnp.where(early, 0, split) + jnp.where(local < length, local, local - length)
        @pl.when(local < length)
        def _():
            first_faces(position)
        @pl.when(local >= length)
        def _():
            first_inner(position)
        @pl.when(number == 2 * split - 1)
        def _():
            @pl.when(me_z == 0)
            def _():
                pl.semaphore_wait(barrier, len(beside))
                for copy in all_edges[0][0:2] + all_edges[0][4:6]:
                    copy.start()
            for copy in all_edges[0][2:4] + all_edges[0][6:7]:
                copy.start()

    @pl.when(me_z == 0)
    def _():
        enter(2, lambda dev_z: dev_z != me_z)

    over(0, 2 * tiles, first_part)

    for step in range(1, STEPS):
        def place(position):
            tile = tile_at(position)
            await_pieces(step - 1, position, tile)
            @pl.when(position == 0)
            def _():
                for copy in all_edges[step - 1]:
                    copy.wait_recv()
            if step >= 2:
                for copy in faces(step - 2, tile):
                    copy.wait_send()
                @pl.when(position == 0)
                def _():
                    for copy in all_edges[step - 2]:
                        copy.wait_send()
            collide_faces(step, tile)
            start_faces(step, position, tile)
            collide_inner(step, tile)
            start_rows(step, position)

        over(0, tiles, place)

    last = STEPS - 1
    def finish_inner(position):
        @pl.when(position == tiles - 2)
        def _():
            for copy in all_edges[last]:
                copy.wait_recv()
        tile = tile_at(tiles - 1 - position)
        over(1, ny - 1, lambda y: finish_tile(y, tile))

    over(0, tiles, finish_inner)

    def finish_faces(position):
        tile = tile_at(position)
        await_pieces(last, position, tile)
        over(0, 2, lambda index: finish_tile(index * (ny - 1), tile))

    over(0, tiles, finish_faces)

    def await_sends(tile):
        for step in (last - 1, last):
            for copy in faces(step, tile):
                copy.wait_send()

    over(0, tiles, await_sends)
    for step in (last - 1, last):
        for copy in all_edges[step]:
            copy.wait_send()


def output_kernel(final_in, density_in, velocity_in, final_ref, density_ref, velocity_ref, final_sem, moment_sem):
    copies = [pltpu.make_async_copy(final_in.at[pop_id], final_ref.at[pop_id], final_sem.at[pop_id]) for pop_id in range(19)]
    copies.append(pltpu.make_async_copy(density_in, density_ref, moment_sem.at[0]))
    copies.append(pltpu.make_async_copy(velocity_in, velocity_ref, moment_sem.at[1]))
    for copy in copies:
        copy.start()
    for copy in copies:
        copy.wait()


def solution(mesh):
    size_y = mesh.shape["py"]
    size_z = mesh.shape["pz"]
    field_spec = P(None, None, "py", "pz")

    def local_steps(populations, relax_time, body_force):
        field = jnp.transpose(populations, (0, 2, 3, 1))
        _, ny, nz, nx = field.shape
        tau = jnp.reshape(relax_time, (1,))
        state_shape = (19, ny + 2, 2, nz + 2 * ROWS, LANES)
        vmem = pl.BlockSpec(memory_space=pltpu.VMEM)
        anywhere = pl.BlockSpec(memory_space=pl.ANY)
        results = pl.pallas_call(
            functools.partial(step_kernel, size_y, size_z, ny, nz),
            name="lattice_steps",
            out_shape=(
                pltpu.VMEM((19, ny, nz, nx), jnp.float32),
                pltpu.VMEM((ny, nz, nx), jnp.float32),
                pltpu.VMEM((3, ny, nz, nx), jnp.float32),
            ),
            in_specs=[anywhere, anywhere, anywhere],
            out_specs=(vmem, vmem, vmem),
            scratch_shapes=[
                pltpu.VMEM(state_shape, jnp.float32),
                pltpu.VMEM(state_shape, jnp.float32),
                pltpu.SMEM((1,), jnp.float32),
                pltpu.SMEM((3,), jnp.float32),
                pltpu.SemaphoreType.DMA((2,)),
                pltpu.SemaphoreType.DMA((nz // ROWS,)),
                pltpu.SemaphoreType.DMA((2, nz // ROWS)),
                pltpu.SemaphoreType.DMA((2, 2, nz // ROWS)),
                pltpu.SemaphoreType.DMA((2, 2, nz // ROWS)),
                pltpu.SemaphoreType.DMA((2, EDGE_COPIES)),
                pltpu.SemaphoreType.DMA((2, EDGE_COPIES)),
            ],
            compiler_params=pltpu.CompilerParams(collective_id=0, has_side_effects=True, vmem_limit_bytes=46 * 2**20),
        )(tau, body_force, field)
        final, density, velocity = pl.pallas_call(
            output_kernel,
            name="lattice_output",
            out_shape=tuple(jax.ShapeDtypeStruct(result.shape, result.dtype) for result in results),
            in_specs=[vmem, vmem, vmem],
            out_specs=(anywhere, anywhere, anywhere),
            scratch_shapes=[pltpu.SemaphoreType.DMA((19,)), pltpu.SemaphoreType.DMA((2,))],
            compiler_params=pltpu.CompilerParams(vmem_limit_bytes=2**20),
        )(*results)
        return jnp.transpose(final, (0, 3, 1, 2)), jnp.transpose(density, (2, 0, 1)), jnp.transpose(velocity, (0, 3, 1, 2))

    return jax.shard_map(local_steps, mesh=mesh, in_specs=(field_spec, P(), P()), out_specs=(field_spec, P(None, "py", "pz"), field_spec), check_vma=False)
```

```python
import functools

import jax
import jax.numpy as jnp
from jax import lax
from jax.experimental import pallas as pl
from jax.experimental.pallas import tpu as pltpu
from jax.sharding import PartitionSpec as P

STEPS = 4
VELOCITIES = ((0, 0, 0), (1, 0, 0), (-1, 0, 0), (0, 1, 0), (0, -1, 0), (0, 0, 1), (0, 0, -1), (1, 1, 0), (-1, -1, 0), (1, -1, 0), (-1, 1, 0), (1, 0, 1), (-1, 0, -1), (1, 0, -1), (-1, 0, 1), (0, 1, 1), (0, -1, -1), (0, 1, -1), (0, -1, 1))
ORDER = (17, 3, 7, 10, 15, 5, 11, 14, 18, 4, 8, 9, 16, 6, 12, 13, 0, 1, 2)
SLOT = {pop_id: slot for slot, pop_id in enumerate(ORDER)}
MESH = pl.DeviceIdType.MESH
LANES = 128
ROWS = 8
EDGE_COPIES = 7


def moment_sums(load):
    rest = load(0)
    total = rest
    diff = {}
    for plus in range(1, 19, 2):
        upper, lower = load(plus), load(plus + 1)
        total = total + (upper + lower)
        diff[plus] = upper - lower
    mom_x = (diff[1] + diff[7]) + (diff[9] + (diff[11] + diff[13]))
    mom_y = (diff[3] + diff[7]) - (diff[9] - (diff[15] + diff[17]))
    mom_z = (diff[5] + diff[11]) - (diff[13] - (diff[15] - diff[17]))
    return total, (mom_x, mom_y, mom_z)


def tile_terms(load, force, rate36):
    density, momentum = moment_sums(load)
    inverse = 1.0 / density
    half = [(momentum[axis] + force[axis]) * inverse * 1.5 for axis in range(3)]
    square = half[0] * half[0] + half[1] * half[1] + half[2] * half[2]
    scale = density * rate36
    even = scale * (1.0 - square * (2.0 / 3.0))
    twice = scale + scale
    odd = [twice * half[axis] for axis in range(3)]
    return even, odd, half


def relaxed(load, terms, keep, plus):
    even, odd, half = terms
    axes = [(axis, shift) for axis, shift in enumerate(VELOCITIES[plus]) if shift != 0]
    if len(axes) == 1:
        axis = axes[0][0]
        odd_part = odd[axis] + odd[axis]
        even_part = (even + even) + odd_part * half[axis]
    else:
        (first, _), (second, sign) = axes
        if sign > 0:
            odd_part = odd[first] + odd[second]
            projection = half[first] + half[second]
        else:
            odd_part = odd[first] - odd[second]
            projection = half[first] - half[second]
        even_part = even + odd_part * projection
    return load(plus) * keep + (even_part + odd_part), load(plus + 1) * keep + (even_part - odd_part)


def rolled(halves, shift, lane):
    if shift == 0:
        return halves
    moved = [pltpu.roll(part, shift % LANES, 1) for part in halves]
    edge = lane == (0 if shift > 0 else LANES - 1)
    return [jnp.where(edge, moved[1], moved[0]), jnp.where(edge, moved[0], moved[1])]


def step_kernel(size_y, size_z, ny, nz, tau_in, force_in, field_ref, stage, density_ref, velocity_ref, buffer_0, buffer_1, tau_ref, force_ref, param_sem, load_sem, first_sem, face_send, face_recv, edge_send, edge_recv):
    me_y, me_z = lax.axis_index("py"), lax.axis_index("pz")
    up_y, down_y = lax.rem(me_y + 1, size_y), lax.rem(me_y + size_y - 1, size_y)
    up_z, down_z = lax.rem(me_z + 1, size_z), lax.rem(me_z + size_z - 1, size_z)

    def device(dev_y, dev_z):
        return {"py": dev_y, "pz": dev_z}

    barrier = pltpu.get_barrier_semaphore()
    beside = [(dev_y, dev_z) for dev_z in (down_z, up_z) for dev_y in (down_y, me_y, up_y)]

    def signal(dev_y, dev_z):
        pl.semaphore_signal(barrier, inc=1, device_id=device(dev_y, dev_z), device_id_type=MESH)

    signal(up_y, me_z)
    signal(down_y, me_z)
    for dev_y, dev_z in beside:
        @pl.when(jnp.logical_and(me_z != 0, dev_z != 0))
        def _():
            signal(dev_y, dev_z)

    def enter(count, targets):
        pl.semaphore_wait(barrier, count)
        for dev_z in targets:
            signal(me_y, dev_z)

    tiles = nz // ROWS
    params = [pltpu.make_async_copy(tau_in, tau_ref, param_sem.at[0]), pltpu.make_async_copy(force_in, force_ref, param_sem.at[1])]
    for copy in params:
        copy.start()

    def first_loads(tile):
        rows = pl.ds(pl.multiple_of(tile * ROWS, ROWS), ROWS)
        return [pltpu.make_async_copy(field_ref.at[:, y, rows], stage.at[:, y, rows], first_sem.at[face, tile]) for face, y in enumerate((0, ny - 1))]

    def inner_load(tile):
        rows = pl.ds(pl.multiple_of(tile * ROWS, ROWS), ROWS)
        planes = pl.ds(1, ny - 2)
        return pltpu.make_async_copy(field_ref.at[:, planes, rows], stage.at[:, planes, rows], load_sem.at[tile])

    order = [position // 2 if position % 2 == 0 else tiles - 1 - position // 2 for position in range(tiles)]
    for positions in (order[:2], order[2:]):
        for tile in positions:
            for copy in first_loads(tile):
                copy.start()
        for tile in positions:
            inner_load(tile).start()
    for copy in params:
        copy.wait()

    tau = jnp.full((ROWS, LANES), tau_ref[0], jnp.float32)
    rate = 1.0 / tau
    keep = 1.0 - rate
    rate36 = rate * (1.0 / 36.0)
    force = [tau * force_ref[axis] for axis in range(3)]
    lane = lax.broadcasted_iota(jnp.int32, (ROWS, LANES), 1)
    buffers = (buffer_0, buffer_1)

    def collide_tile(step, y, tile):
        row = pl.multiple_of(tile * ROWS, ROWS)
        target = buffers[step % 2]
        source = buffers[(step + 1) % 2]

        def load(half, pop_id):
            if step == 0:
                return stage[pop_id, y, pl.ds(row, ROWS), pl.ds(half * LANES, LANES)]
            _, shift_y, shift_z = VELOCITIES[pop_id]
            return source[SLOT[pop_id], y + 1 - shift_y, half, pl.ds(row + (ROWS - shift_z), ROWS), :]

        def store(pop_id, halves):
            halves = rolled(halves, VELOCITIES[pop_id][0], lane)
            for half in range(2):
                target[SLOT[pop_id], y + 1, half, pl.ds(row + ROWS, ROWS), :] = halves[half]

        loaders = [functools.partial(load, half) for half in range(2)]
        terms = [tile_terms(loaders[half], force, rate36) for half in range(2)]
        store(0, [loaders[half](0) * keep + terms[half][0] * 12.0 for half in range(2)])
        for plus in range(1, 19, 2):
            pairs = [relaxed(loaders[half], terms[half], keep, plus) for half in range(2)]
            store(plus, [pair[0] for pair in pairs])
            store(plus + 1, [pair[1] for pair in pairs])

    def faces(step, tile):
        state, parity = buffers[step % 2], step % 2
        rows = pl.ds(pl.multiple_of(tile * ROWS + ROWS, ROWS), ROWS)
        result = []
        for face, (slots, source, target, dev_y) in enumerate(((pl.ds(0, 5), ny, 0, up_y), (pl.ds(8, 5), 1, ny + 1, down_y))):
            result.append(pltpu.make_async_remote_copy(
                src_ref=state.at[slots, source, :, rows, :], dst_ref=state.at[slots, target, :, rows, :],
                send_sem=face_send.at[parity, face, tile], recv_sem=face_recv.at[parity, face, tile],
                device_id=device(dev_y, me_z), device_id_type=MESH))
        return result

    def edges(step):
        state, parity = buffers[step % 2], step % 2
        planes = pl.ds(1, ny)
        low, high, below, above = (pl.ds(row, 1) for row in (ROWS, ROWS + nz - 1, ROWS - 1, ROWS + nz))
        parts = (
            (0, ny, low, 0, above, up_y, down_z),
            (12, 1, low, ny + 1, above, down_y, down_z),
            (pl.ds(12, 4), planes, low, planes, above, me_y, down_z),
            (0, planes, low, planes, above, me_y, down_z),
            (4, ny, high, 0, below, up_y, up_z),
            (8, 1, high, ny + 1, below, down_y, up_z),
            (pl.ds(4, 5), planes, high, planes, below, me_y, up_z),
        )
        return [pltpu.make_async_remote_copy(
            src_ref=state.at[slots, source, :, source_row, :], dst_ref=state.at[slots, target, :, target_row, :],
            send_sem=edge_send.at[parity, number], recv_sem=edge_recv.at[parity, number],
            device_id=device(dev_y, dev_z), device_id_type=MESH)
            for number, (slots, source, source_row, target, target_row, dev_y, dev_z) in enumerate(parts)]

    def over(start, stop, body, unroll=False):
        def run(index, carry):
            body(index)
            return carry
        lax.fori_loop(start, stop, run, 0, unroll=unroll)

    def finish_tile(y, tile):
        row = pl.multiple_of(tile * ROWS, ROWS)
        source = buffers[(STEPS - 1) % 2]
        for half in range(2):
            place = (y, pl.ds(row, ROWS), pl.ds(half * LANES, LANES))

            def load(pop_id):
                _, shift_y, shift_z = VELOCITIES[pop_id]
                value = source[SLOT[pop_id], y + 1 - shift_y, half, pl.ds(row + (ROWS - shift_z), ROWS), :]
                stage[(pop_id, *place)] = value
                return value

            density, momentum = moment_sums(load)
            density_ref[place] = density
            for axis in range(3):
                velocity_ref[(axis, *place)] = (momentum[axis] + force[axis]) / density

    def tile_at(position):
        return jnp.where(position % 2 == 0, position // 2, tiles - 1 - position // 2)

    def at_position(position, number, copies):
        @pl.when(position == number)
        def _():
            for copy in copies:
                copy.start()

    all_edges = [edges(step) for step in range(STEPS)]

    def collide_faces(step, tile):
        over(0, 2, lambda index: collide_tile(step, index * (ny - 1), tile), True)

    def collide_inner(step, tile):
        over(1, ny - 1, lambda index: collide_tile(step, index, tile), True)

    def start_faces(step, position, tile):
        at_position(position, 0, all_edges[step][0:2])
        at_position(position, 1, all_edges[step][4:6])
        for copy in faces(step, tile):
            copy.start()

    def start_rows(step, position):
        at_position(position, 0, all_edges[step][2:4])
        at_position(position, 1, all_edges[step][6:7])

    def await_pieces(step, position, tile):
        def await_piece(number):
            for copy in faces(step, number):
                copy.wait_recv()

        @pl.when(position < 2)
        def _():
            await_piece(tile)
        @pl.when(position < tiles - 2)
        def _():
            await_piece(jnp.where(position % 2 == 0, tile + 1, tile - 1))

    def first_faces(position):
        tile = tile_at(position)
        for copy in first_loads(tile):
            copy.wait()
        collide_faces(0, tile)
        @pl.when(position == 0)
        def _():
            @pl.when(jnp.logical_and(me_z != 0, jnp.logical_and(down_z != 0, up_z != 0)))
            def _():
                enter(8, ())
            @pl.when(jnp.logical_and(me_z != 0, down_z == 0))
            def _():
                enter(6, (down_z,))
            @pl.when(jnp.logical_and(me_z != 0, up_z == 0))
            def _():
                enter(6, (up_z,))
        for number, corners in enumerate((all_edges[0][0:2], all_edges[0][4:6])):
            @pl.when(jnp.logical_and(position == number, me_z != 0))
            def _():
                for copy in corners:
                    copy.start()
        for copy in faces(0, tile):
            copy.start()

    def first_inner(position):
        tile = tile_at(position)
        inner_load(tile).wait()
        collide_inner(0, tile)

    split = jnp.where(me_z == 0, tiles // 2, 2)

    def first_part(number):
        early = number < 2 * split
        local = jnp.where(early, number, number - 2 * split)
        length = jnp.where(early, split, tiles - split)
        position = jnp.where(early, 0, split) + jnp.where(local < length, local, local - length)
        @pl.when(local < length)
        def _():
            first_faces(position)
        @pl.when(local >= length)
        def _():
            first_inner(position)
        @pl.when(number == 2 * split - 1)
        def _():
            @pl.when(me_z == 0)
            def _():
                pl.semaphore_wait(barrier, 2)
                for copy in all_edges[0][0:2] + all_edges[0][4:6]:
                    copy.start()
            for copy in all_edges[0][2:4] + all_edges[0][6:7]:
                copy.start()

    @pl.when(me_z == 0)
    def _():
        enter(2, (down_z, up_z))

    over(0, 2 * tiles, first_part)

    for step in range(1, STEPS):
        def place(position):
            tile = tile_at(position)
            await_pieces(step - 1, position, tile)
            @pl.when(position == 0)
            def _():
                for copy in all_edges[step - 1]:
                    copy.wait_recv()
            if step >= 2:
                for copy in faces(step - 2, tile):
                    copy.wait_send()
                @pl.when(position == 0)
                def _():
                    for copy in all_edges[step - 2]:
                        copy.wait_send()
            collide_faces(step, tile)
            start_faces(step, position, tile)
            collide_inner(step, tile)
            start_rows(step, position)

        over(0, tiles, place)

    last = STEPS - 1
    def finish_inner(position):
        @pl.when(position == tiles - 2)
        def _():
            for copy in all_edges[last]:
                copy.wait_recv()
        tile = tile_at(tiles - 1 - position)
        over(1, ny - 1, lambda y: finish_tile(y, tile))

    over(0, tiles, finish_inner)

    def finish_faces(position):
        tile = tile_at(position)
        await_pieces(last, position, tile)
        over(0, 2, lambda index: finish_tile(index * (ny - 1), tile))

    over(0, tiles, finish_faces)

    def await_sends(tile):
        for step in (last - 1, last):
            for copy in faces(step, tile):
                copy.wait_send()

    over(0, tiles, await_sends)
    for step in (last - 1, last):
        for copy in all_edges[step]:
            copy.wait_send()


def output_kernel(final_in, density_in, velocity_in, final_ref, density_ref, velocity_ref, final_sem, moment_sem):
    copies = [pltpu.make_async_copy(final_in.at[pop_id], final_ref.at[pop_id], final_sem.at[pop_id]) for pop_id in range(19)]
    copies.append(pltpu.make_async_copy(density_in, density_ref, moment_sem.at[0]))
    copies.append(pltpu.make_async_copy(velocity_in, velocity_ref, moment_sem.at[1]))
    for copy in copies:
        copy.start()
    for copy in copies:
        copy.wait()


def solution(mesh):
    size_y = mesh.shape["py"]
    size_z = mesh.shape["pz"]
    field_spec = P(None, None, "py", "pz")

    def local_steps(populations, relax_time, body_force):
        field = jnp.transpose(populations, (0, 2, 3, 1))
        _, ny, nz, nx = field.shape
        tau = jnp.reshape(relax_time, (1,))
        state_shape = (19, ny + 2, 2, nz + 2 * ROWS, LANES)
        vmem = pl.BlockSpec(memory_space=pltpu.VMEM)
        anywhere = pl.BlockSpec(memory_space=pl.ANY)
        results = pl.pallas_call(
            functools.partial(step_kernel, size_y, size_z, ny, nz),
            name="lattice_steps",
            out_shape=(
                pltpu.VMEM((19, ny, nz, nx), jnp.float32),
                pltpu.VMEM((ny, nz, nx), jnp.float32),
                pltpu.VMEM((3, ny, nz, nx), jnp.float32),
            ),
            in_specs=[anywhere, anywhere, anywhere],
            out_specs=(vmem, vmem, vmem),
            scratch_shapes=[
                pltpu.VMEM(state_shape, jnp.float32),
                pltpu.VMEM(state_shape, jnp.float32),
                pltpu.SMEM((1,), jnp.float32),
                pltpu.SMEM((3,), jnp.float32),
                pltpu.SemaphoreType.DMA((2,)),
                pltpu.SemaphoreType.DMA((nz // ROWS,)),
                pltpu.SemaphoreType.DMA((2, nz // ROWS)),
                pltpu.SemaphoreType.DMA((2, 2, nz // ROWS)),
                pltpu.SemaphoreType.DMA((2, 2, nz // ROWS)),
                pltpu.SemaphoreType.DMA((2, EDGE_COPIES)),
                pltpu.SemaphoreType.DMA((2, EDGE_COPIES)),
            ],
            compiler_params=pltpu.CompilerParams(collective_id=0, has_side_effects=True, vmem_limit_bytes=46 * 2**20),
        )(tau, body_force, field)
        final, density, velocity = pl.pallas_call(
            output_kernel,
            name="lattice_output",
            out_shape=tuple(jax.ShapeDtypeStruct(result.shape, result.dtype) for result in results),
            in_specs=[vmem, vmem, vmem],
            out_specs=(anywhere, anywhere, anywhere),
            scratch_shapes=[pltpu.SemaphoreType.DMA((19,)), pltpu.SemaphoreType.DMA((2,))],
            compiler_params=pltpu.CompilerParams(vmem_limit_bytes=2**20),
        )(*results)
        return jnp.transpose(final, (0, 3, 1, 2)), jnp.transpose(density, (2, 0, 1)), jnp.transpose(velocity, (0, 3, 1, 2))

    return jax.shard_map(local_steps, mesh=mesh, in_specs=(field_spec, P(), P()), out_specs=(field_spec, P(None, "py", "pz"), field_spec), check_vma=False)
```

```python
import functools

import jax
import jax.numpy as jnp
from jax import lax
from jax.experimental import pallas as pl
from jax.experimental.pallas import tpu as pltpu
from jax.sharding import PartitionSpec as P

STEPS = 4
VELOCITIES = ((0, 0, 0), (1, 0, 0), (-1, 0, 0), (0, 1, 0), (0, -1, 0), (0, 0, 1), (0, 0, -1), (1, 1, 0), (-1, -1, 0), (1, -1, 0), (-1, 1, 0), (1, 0, 1), (-1, 0, -1), (1, 0, -1), (-1, 0, 1), (0, 1, 1), (0, -1, -1), (0, 1, -1), (0, -1, 1))
ORDER = (17, 3, 7, 10, 15, 5, 11, 14, 18, 4, 8, 9, 16, 6, 12, 13, 0, 1, 2)
SLOT = {pop_id: slot for slot, pop_id in enumerate(ORDER)}
MESH = pl.DeviceIdType.MESH
LANES = 128
ROWS = 8
EDGE_COPIES = 7


def moment_sums(load):
    rest = load(0)
    total = rest
    diff = {}
    for plus in range(1, 19, 2):
        upper, lower = load(plus), load(plus + 1)
        total = total + (upper + lower)
        diff[plus] = upper - lower
    mom_x = (diff[1] + diff[7]) + (diff[9] + (diff[11] + diff[13]))
    mom_y = (diff[3] + diff[7]) - (diff[9] - (diff[15] + diff[17]))
    mom_z = (diff[5] + diff[11]) - (diff[13] - (diff[15] - diff[17]))
    return total, (mom_x, mom_y, mom_z)


def tile_terms(load, force, rate36):
    density, momentum = moment_sums(load)
    inverse = 1.0 / density
    half = [(momentum[axis] + force[axis]) * inverse * 1.5 for axis in range(3)]
    square = half[0] * half[0] + half[1] * half[1] + half[2] * half[2]
    scale = density * rate36
    even = scale * (1.0 - square * (2.0 / 3.0))
    twice = scale + scale
    odd = [twice * half[axis] for axis in range(3)]
    return even, odd, half


def relaxed(load, terms, keep, plus):
    even, odd, half = terms
    axes = [(axis, shift) for axis, shift in enumerate(VELOCITIES[plus]) if shift != 0]
    if len(axes) == 1:
        axis = axes[0][0]
        odd_part = odd[axis] + odd[axis]
        even_part = (even + even) + odd_part * half[axis]
    else:
        (first, _), (second, sign) = axes
        if sign > 0:
            odd_part = odd[first] + odd[second]
            projection = half[first] + half[second]
        else:
            odd_part = odd[first] - odd[second]
            projection = half[first] - half[second]
        even_part = even + odd_part * projection
    return load(plus) * keep + (even_part + odd_part), load(plus + 1) * keep + (even_part - odd_part)


def rolled(halves, shift, lane):
    if shift == 0:
        return halves
    moved = [pltpu.roll(part, shift % LANES, 1) for part in halves]
    edge = lane == (0 if shift > 0 else LANES - 1)
    return [jnp.where(edge, moved[1], moved[0]), jnp.where(edge, moved[0], moved[1])]


def step_kernel(size_y, size_z, ny, nz, tau_in, force_in, field_ref, stage, density_ref, velocity_ref, buffer_0, buffer_1, tau_ref, force_ref, param_sem, load_sem, first_sem, face_send, face_recv, edge_send, edge_recv):
    me_y, me_z = lax.axis_index("py"), lax.axis_index("pz")
    up_y, down_y = lax.rem(me_y + 1, size_y), lax.rem(me_y + size_y - 1, size_y)
    up_z, down_z = lax.rem(me_z + 1, size_z), lax.rem(me_z + size_z - 1, size_z)

    def device(dev_y, dev_z):
        return {"py": dev_y, "pz": dev_z}

    barrier = pltpu.get_barrier_semaphore()
    even = me_z % 2 == 0
    odd = me_z % 2 == 1

    def signal(dev_y, dev_z):
        pl.semaphore_signal(barrier, inc=1, device_id=device(dev_y, dev_z), device_id_type=MESH)

    signal(up_y, me_z)
    signal(down_y, me_z)

    def enter(count):
        pl.semaphore_wait(barrier, count)
        signal(me_y, down_z)
        signal(me_y, up_z)

    tiles = nz // ROWS
    params = [pltpu.make_async_copy(tau_in, tau_ref, param_sem.at[0]), pltpu.make_async_copy(force_in, force_ref, param_sem.at[1])]
    for copy in params:
        copy.start()

    def first_loads(tile):
        rows = pl.ds(pl.multiple_of(tile * ROWS, ROWS), ROWS)
        return [pltpu.make_async_copy(field_ref.at[:, y, rows], stage.at[:, y, rows], first_sem.at[face, tile]) for face, y in enumerate((0, ny - 1))]

    def inner_load(tile):
        rows = pl.ds(pl.multiple_of(tile * ROWS, ROWS), ROWS)
        planes = pl.ds(1, ny - 2)
        return pltpu.make_async_copy(field_ref.at[:, planes, rows], stage.at[:, planes, rows], load_sem.at[tile])

    order = [position // 2 if position % 2 == 0 else tiles - 1 - position // 2 for position in range(tiles)]
    for positions in (order[:2], order[2:]):
        for tile in positions:
            for copy in first_loads(tile):
                copy.start()
        for tile in positions:
            inner_load(tile).start()
    for copy in params:
        copy.wait()

    tau = jnp.full((ROWS, LANES), tau_ref[0], jnp.float32)
    rate = 1.0 / tau
    keep = 1.0 - rate
    rate36 = rate * (1.0 / 36.0)
    force = [tau * force_ref[axis] for axis in range(3)]
    lane = lax.broadcasted_iota(jnp.int32, (ROWS, LANES), 1)
    buffers = (buffer_0, buffer_1)

    def collide_tile(step, y, tile):
        row = pl.multiple_of(tile * ROWS, ROWS)
        target = buffers[step % 2]
        source = buffers[(step + 1) % 2]

        def load(half, pop_id):
            if step == 0:
                return stage[pop_id, y, pl.ds(row, ROWS), pl.ds(half * LANES, LANES)]
            _, shift_y, shift_z = VELOCITIES[pop_id]
            return source[SLOT[pop_id], y + 1 - shift_y, half, pl.ds(row + (ROWS - shift_z), ROWS), :]

        def store(pop_id, halves):
            halves = rolled(halves, VELOCITIES[pop_id][0], lane)
            for half in range(2):
                target[SLOT[pop_id], y + 1, half, pl.ds(row + ROWS, ROWS), :] = halves[half]

        loaders = [functools.partial(load, half) for half in range(2)]
        terms = [tile_terms(loaders[half], force, rate36) for half in range(2)]
        store(0, [loaders[half](0) * keep + terms[half][0] * 12.0 for half in range(2)])
        for plus in range(1, 19, 2):
            pairs = [relaxed(loaders[half], terms[half], keep, plus) for half in range(2)]
            store(plus, [pair[0] for pair in pairs])
            store(plus + 1, [pair[1] for pair in pairs])

    def faces(step, tile):
        state, parity = buffers[step % 2], step % 2
        rows = pl.ds(pl.multiple_of(tile * ROWS + ROWS, ROWS), ROWS)
        result = []
        for face, (slots, source, target, dev_y) in enumerate(((pl.ds(0, 5), ny, 0, up_y), (pl.ds(8, 5), 1, ny + 1, down_y))):
            result.append(pltpu.make_async_remote_copy(
                src_ref=state.at[slots, source, :, rows, :], dst_ref=state.at[slots, target, :, rows, :],
                send_sem=face_send.at[parity, face, tile], recv_sem=face_recv.at[parity, face, tile],
                device_id=device(dev_y, me_z), device_id_type=MESH))
        return result

    def edges(step):
        state, parity = buffers[step % 2], step % 2
        planes = pl.ds(1, ny)
        low, high, below, above = (pl.ds(row, 1) for row in (ROWS, ROWS + nz - 1, ROWS - 1, ROWS + nz))
        parts = (
            (0, ny, low, 0, above, up_y, down_z),
            (12, 1, low, ny + 1, above, down_y, down_z),
            (pl.ds(12, 4), planes, low, planes, above, me_y, down_z),
            (0, planes, low, planes, above, me_y, down_z),
            (4, ny, high, 0, below, up_y, up_z),
            (8, 1, high, ny + 1, below, down_y, up_z),
            (pl.ds(4, 5), planes, high, planes, below, me_y, up_z),
        )
        return [pltpu.make_async_remote_copy(
            src_ref=state.at[slots, source, :, source_row, :], dst_ref=state.at[slots, target, :, target_row, :],
            send_sem=edge_send.at[parity, number], recv_sem=edge_recv.at[parity, number],
            device_id=device(dev_y, dev_z), device_id_type=MESH)
            for number, (slots, source, source_row, target, target_row, dev_y, dev_z) in enumerate(parts)]

    def over(start, stop, body, unroll=False):
        def run(index, carry):
            body(index)
            return carry
        lax.fori_loop(start, stop, run, 0, unroll=unroll)

    def finish_tile(y, tile):
        row = pl.multiple_of(tile * ROWS, ROWS)
        source = buffers[(STEPS - 1) % 2]
        for half in range(2):
            place = (y, pl.ds(row, ROWS), pl.ds(half * LANES, LANES))

            def load(pop_id):
                _, shift_y, shift_z = VELOCITIES[pop_id]
                value = source[SLOT[pop_id], y + 1 - shift_y, half, pl.ds(row + (ROWS - shift_z), ROWS), :]
                stage[(pop_id, *place)] = value
                return value

            density, momentum = moment_sums(load)
            density_ref[place] = density
            for axis in range(3):
                velocity_ref[(axis, *place)] = (momentum[axis] + force[axis]) / density

    def tile_at(position):
        return jnp.where(position % 2 == 0, position // 2, tiles - 1 - position // 2)

    def at_position(position, number, copies):
        @pl.when(position == number)
        def _():
            for copy in copies:
                copy.start()

    all_edges = [edges(step) for step in range(STEPS)]

    def collide_faces(step, tile):
        over(0, 2, lambda index: collide_tile(step, index * (ny - 1), tile), True)

    def collide_inner(step, tile):
        over(1, ny - 1, lambda index: collide_tile(step, index, tile), True)

    def start_faces(step, position, tile):
        at_position(position, 0, all_edges[step][0:2])
        at_position(position, 1, all_edges[step][4:6])
        for copy in faces(step, tile):
            copy.start()

    def start_rows(step, position):
        at_position(position, 0, all_edges[step][2:4])
        at_position(position, 1, all_edges[step][6:7])

    def await_pieces(step, position, tile):
        def await_piece(number):
            for copy in faces(step, number):
                copy.wait_recv()

        @pl.when(position < 2)
        def _():
            await_piece(tile)
        @pl.when(position < tiles - 2)
        def _():
            await_piece(jnp.where(position % 2 == 0, tile + 1, tile - 1))

    def first_faces(position):
        tile = tile_at(position)
        for copy in first_loads(tile):
            copy.wait()
        collide_faces(0, tile)
        @pl.when(jnp.logical_and(position == 0, odd))
        def _():
            enter(4)
        for number, corners in enumerate((all_edges[0][0:2], all_edges[0][4:6])):
            @pl.when(jnp.logical_and(position == number, odd))
            def _():
                for copy in corners:
                    copy.start()
        for copy in faces(0, tile):
            copy.start()

    def first_inner(position):
        tile = tile_at(position)
        inner_load(tile).wait()
        collide_inner(0, tile)

    split = jnp.where(even, tiles // 2, 2)

    def first_part(number):
        early = number < 2 * split
        local = jnp.where(early, number, number - 2 * split)
        length = jnp.where(early, split, tiles - split)
        position = jnp.where(early, 0, split) + jnp.where(local < length, local, local - length)
        @pl.when(local < length)
        def _():
            first_faces(position)
        @pl.when(local >= length)
        def _():
            first_inner(position)
        @pl.when(number == 2 * split - 1)
        def _():
            @pl.when(even)
            def _():
                pl.semaphore_wait(barrier, 2)
                for copy in all_edges[0][0:2] + all_edges[0][4:6]:
                    copy.start()
            for copy in all_edges[0][2:4] + all_edges[0][6:7]:
                copy.start()

    @pl.when(even)
    def _():
        enter(2)

    over(0, 2 * tiles, first_part)

    for step in range(1, STEPS):
        def place(position):
            tile = tile_at(position)
            await_pieces(step - 1, position, tile)
            @pl.when(position == 0)
            def _():
                for copy in all_edges[step - 1]:
                    copy.wait_recv()
            if step >= 2:
                for copy in faces(step - 2, tile):
                    copy.wait_send()
                @pl.when(position == 0)
                def _():
                    for copy in all_edges[step - 2]:
                        copy.wait_send()
            collide_faces(step, tile)
            start_faces(step, position, tile)
            collide_inner(step, tile)
            start_rows(step, position)

        over(0, tiles, place)

    last = STEPS - 1
    def finish_inner(position):
        @pl.when(position == tiles - 2)
        def _():
            for copy in all_edges[last]:
                copy.wait_recv()
        tile = tile_at(tiles - 1 - position)
        over(1, ny - 1, lambda y: finish_tile(y, tile))

    over(0, tiles, finish_inner)

    def finish_faces(position):
        tile = tile_at(position)
        await_pieces(last, position, tile)
        over(0, 2, lambda index: finish_tile(index * (ny - 1), tile))

    over(0, tiles, finish_faces)

    def await_sends(tile):
        for step in (last - 1, last):
            for copy in faces(step, tile):
                copy.wait_send()

    over(0, tiles, await_sends)
    for step in (last - 1, last):
        for copy in all_edges[step]:
            copy.wait_send()


def output_kernel(final_in, density_in, velocity_in, final_ref, density_ref, velocity_ref, final_sem, moment_sem):
    copies = [pltpu.make_async_copy(final_in.at[pop_id], final_ref.at[pop_id], final_sem.at[pop_id]) for pop_id in range(19)]
    copies.append(pltpu.make_async_copy(density_in, density_ref, moment_sem.at[0]))
    copies.append(pltpu.make_async_copy(velocity_in, velocity_ref, moment_sem.at[1]))
    for copy in copies:
        copy.start()
    for copy in copies:
        copy.wait()


def solution(mesh):
    size_y = mesh.shape["py"]
    size_z = mesh.shape["pz"]
    field_spec = P(None, None, "py", "pz")

    def local_steps(populations, relax_time, body_force):
        field = jnp.transpose(populations, (0, 2, 3, 1))
        _, ny, nz, nx = field.shape
        tau = jnp.reshape(relax_time, (1,))
        state_shape = (19, ny + 2, 2, nz + 2 * ROWS, LANES)
        vmem = pl.BlockSpec(memory_space=pltpu.VMEM)
        anywhere = pl.BlockSpec(memory_space=pl.ANY)
        results = pl.pallas_call(
            functools.partial(step_kernel, size_y, size_z, ny, nz),
            name="lattice_steps",
            out_shape=(
                pltpu.VMEM((19, ny, nz, nx), jnp.float32),
                pltpu.VMEM((ny, nz, nx), jnp.float32),
                pltpu.VMEM((3, ny, nz, nx), jnp.float32),
            ),
            in_specs=[anywhere, anywhere, anywhere],
            out_specs=(vmem, vmem, vmem),
            scratch_shapes=[
                pltpu.VMEM(state_shape, jnp.float32),
                pltpu.VMEM(state_shape, jnp.float32),
                pltpu.SMEM((1,), jnp.float32),
                pltpu.SMEM((3,), jnp.float32),
                pltpu.SemaphoreType.DMA((2,)),
                pltpu.SemaphoreType.DMA((nz // ROWS,)),
                pltpu.SemaphoreType.DMA((2, nz // ROWS)),
                pltpu.SemaphoreType.DMA((2, 2, nz // ROWS)),
                pltpu.SemaphoreType.DMA((2, 2, nz // ROWS)),
                pltpu.SemaphoreType.DMA((2, EDGE_COPIES)),
                pltpu.SemaphoreType.DMA((2, EDGE_COPIES)),
            ],
            compiler_params=pltpu.CompilerParams(collective_id=0, has_side_effects=True, vmem_limit_bytes=46 * 2**20),
        )(tau, body_force, field)
        final, density, velocity = pl.pallas_call(
            output_kernel,
            name="lattice_output",
            out_shape=tuple(jax.ShapeDtypeStruct(result.shape, result.dtype) for result in results),
            in_specs=[vmem, vmem, vmem],
            out_specs=(anywhere, anywhere, anywhere),
            scratch_shapes=[pltpu.SemaphoreType.DMA((19,)), pltpu.SemaphoreType.DMA((2,))],
            compiler_params=pltpu.CompilerParams(vmem_limit_bytes=2**20),
        )(*results)
        return jnp.transpose(final, (0, 3, 1, 2)), jnp.transpose(density, (2, 0, 1)), jnp.transpose(velocity, (0, 3, 1, 2))

    return jax.shard_map(local_steps, mesh=mesh, in_specs=(field_spec, P(), P()), out_specs=(field_spec, P(None, "py", "pz"), field_spec), check_vma=False)
```

```python
import functools

import jax
import jax.numpy as jnp
from jax import lax
from jax.experimental import pallas as pl
from jax.experimental.pallas import tpu as pltpu
from jax.sharding import PartitionSpec as P

STEPS = 4
VELOCITIES = ((0, 0, 0), (1, 0, 0), (-1, 0, 0), (0, 1, 0), (0, -1, 0), (0, 0, 1), (0, 0, -1), (1, 1, 0), (-1, -1, 0), (1, -1, 0), (-1, 1, 0), (1, 0, 1), (-1, 0, -1), (1, 0, -1), (-1, 0, 1), (0, 1, 1), (0, -1, -1), (0, 1, -1), (0, -1, 1))
ORDER = (17, 3, 7, 10, 15, 5, 11, 14, 18, 4, 8, 9, 16, 6, 12, 13, 0, 1, 2)
SLOT = {pop_id: slot for slot, pop_id in enumerate(ORDER)}
MESH = pl.DeviceIdType.MESH
LANES = 128
ROWS = 8
EDGE_COPIES = 7


def moment_sums(load):
    rest = load(0)
    total = rest
    diff = {}
    for plus in range(1, 19, 2):
        upper, lower = load(plus), load(plus + 1)
        total = total + (upper + lower)
        diff[plus] = upper - lower
    mom_x = (diff[1] + diff[7]) + (diff[9] + (diff[11] + diff[13]))
    mom_y = (diff[3] + diff[7]) - (diff[9] - (diff[15] + diff[17]))
    mom_z = (diff[5] + diff[11]) - (diff[13] - (diff[15] - diff[17]))
    return total, (mom_x, mom_y, mom_z)


def tile_terms(load, force, rate36):
    density, momentum = moment_sums(load)
    inverse = 1.0 / density
    half = [(momentum[axis] + force[axis]) * inverse * 1.5 for axis in range(3)]
    square = half[0] * half[0] + half[1] * half[1] + half[2] * half[2]
    scale = density * rate36
    even = scale * (1.0 - square * (2.0 / 3.0))
    twice = scale + scale
    odd = [twice * half[axis] for axis in range(3)]
    return even, odd, half


def relaxed(load, terms, keep, plus):
    even, odd, half = terms
    axes = [(axis, shift) for axis, shift in enumerate(VELOCITIES[plus]) if shift != 0]
    if len(axes) == 1:
        axis = axes[0][0]
        odd_part = odd[axis] + odd[axis]
        even_part = (even + even) + odd_part * half[axis]
    else:
        (first, _), (second, sign) = axes
        if sign > 0:
            odd_part = odd[first] + odd[second]
            projection = half[first] + half[second]
        else:
            odd_part = odd[first] - odd[second]
            projection = half[first] - half[second]
        even_part = even + odd_part * projection
    return load(plus) * keep + (even_part + odd_part), load(plus + 1) * keep + (even_part - odd_part)


def rolled(halves, shift, lane):
    if shift == 0:
        return halves
    moved = [pltpu.roll(part, shift % LANES, 1) for part in halves]
    edge = lane == (0 if shift > 0 else LANES - 1)
    return [jnp.where(edge, moved[1], moved[0]), jnp.where(edge, moved[0], moved[1])]


def step_kernel(size_y, size_z, ny, nz, tau_in, force_in, field_ref, stage, density_ref, velocity_ref, buffer_0, buffer_1, tau_ref, force_ref, param_sem, load_sem, first_sem, face_send, face_recv, edge_send, edge_recv):
    me_y, me_z = lax.axis_index("py"), lax.axis_index("pz")
    up_y, down_y = lax.rem(me_y + 1, size_y), lax.rem(me_y + size_y - 1, size_y)
    up_z, down_z = lax.rem(me_z + 1, size_z), lax.rem(me_z + size_z - 1, size_z)

    def device(dev_y, dev_z):
        return {"py": dev_y, "pz": dev_z}

    barrier = pltpu.get_barrier_semaphore()
    beside = [(dev_y, dev_z) for dev_z in (down_z, up_z) for dev_y in (down_y, me_y, up_y)]

    def signal(dev_y, dev_z):
        pl.semaphore_signal(barrier, inc=1, device_id=device(dev_y, dev_z), device_id_type=MESH)

    signal(up_y, me_z)
    signal(down_y, me_z)
    for dev_y, dev_z in beside:
        @pl.when(jnp.logical_and(me_z != 0, dev_z != 0))
        def _():
            signal(dev_y, dev_z)

    def enter(count, targets):
        pl.semaphore_wait(barrier, count)
        for dev_z in targets:
            signal(me_y, dev_z)

    tiles = nz // ROWS
    params = [pltpu.make_async_copy(tau_in, tau_ref, param_sem.at[0]), pltpu.make_async_copy(force_in, force_ref, param_sem.at[1])]
    for copy in params:
        copy.start()

    def first_loads(tile):
        rows = pl.ds(pl.multiple_of(tile * ROWS, ROWS), ROWS)
        return [pltpu.make_async_copy(field_ref.at[:, y, rows], stage.at[:, y, rows], first_sem.at[face, tile]) for face, y in enumerate((0, ny - 1))]

    def inner_load(tile):
        rows = pl.ds(pl.multiple_of(tile * ROWS, ROWS), ROWS)
        planes = pl.ds(1, ny - 2)
        return pltpu.make_async_copy(field_ref.at[:, planes, rows], stage.at[:, planes, rows], load_sem.at[tile])

    order = [position // 2 if position % 2 == 0 else tiles - 1 - position // 2 for position in range(tiles)]
    for positions in (order[:2], order[2:]):
        for tile in positions:
            for copy in first_loads(tile):
                copy.start()
        for tile in positions:
            inner_load(tile).start()
    for copy in params:
        copy.wait()

    tau = jnp.full((ROWS, LANES), tau_ref[0], jnp.float32)
    rate = 1.0 / tau
    keep = 1.0 - rate
    rate36 = rate * (1.0 / 36.0)
    force = [tau * force_ref[axis] for axis in range(3)]
    lane = lax.broadcasted_iota(jnp.int32, (ROWS, LANES), 1)
    buffers = (buffer_0, buffer_1)

    def collide_tile(step, y, tile):
        row = pl.multiple_of(tile * ROWS, ROWS)
        target = buffers[step % 2]
        source = buffers[(step + 1) % 2]

        def load(half, pop_id):
            if step == 0:
                return stage[pop_id, y, pl.ds(row, ROWS), pl.ds(half * LANES, LANES)]
            _, shift_y, shift_z = VELOCITIES[pop_id]
            return source[SLOT[pop_id], y + 1 - shift_y, half, pl.ds(row + (ROWS - shift_z), ROWS), :]

        def store(pop_id, halves):
            halves = rolled(halves, VELOCITIES[pop_id][0], lane)
            for half in range(2):
                target[SLOT[pop_id], y + 1, half, pl.ds(row + ROWS, ROWS), :] = halves[half]

        loaders = [functools.partial(load, half) for half in range(2)]
        terms = [tile_terms(loaders[half], force, rate36) for half in range(2)]
        store(0, [loaders[half](0) * keep + terms[half][0] * 12.0 for half in range(2)])
        for plus in range(1, 19, 2):
            pairs = [relaxed(loaders[half], terms[half], keep, plus) for half in range(2)]
            store(plus, [pair[0] for pair in pairs])
            store(plus + 1, [pair[1] for pair in pairs])

    def faces(step, tile):
        state, parity = buffers[step % 2], step % 2
        rows = pl.ds(pl.multiple_of(tile * ROWS + ROWS, ROWS), ROWS)
        result = []
        for face, (slots, source, target, dev_y) in enumerate(((pl.ds(0, 5), ny, 0, up_y), (pl.ds(8, 5), 1, ny + 1, down_y))):
            result.append(pltpu.make_async_remote_copy(
                src_ref=state.at[slots, source, :, rows, :], dst_ref=state.at[slots, target, :, rows, :],
                send_sem=face_send.at[parity, face, tile], recv_sem=face_recv.at[parity, face, tile],
                device_id=device(dev_y, me_z), device_id_type=MESH))
        return result

    def edges(step):
        state, parity = buffers[step % 2], step % 2
        planes = pl.ds(1, ny)
        low, high, below, above = (pl.ds(row, 1) for row in (ROWS, ROWS + nz - 1, ROWS - 1, ROWS + nz))
        parts = (
            (0, ny, low, 0, above, up_y, down_z),
            (12, 1, low, ny + 1, above, down_y, down_z),
            (pl.ds(12, 4), planes, low, planes, above, me_y, down_z),
            (0, planes, low, planes, above, me_y, down_z),
            (4, ny, high, 0, below, up_y, up_z),
            (8, 1, high, ny + 1, below, down_y, up_z),
            (pl.ds(4, 5), planes, high, planes, below, me_y, up_z),
        )
        return [pltpu.make_async_remote_copy(
            src_ref=state.at[slots, source, :, source_row, :], dst_ref=state.at[slots, target, :, target_row, :],
            send_sem=edge_send.at[parity, number], recv_sem=edge_recv.at[parity, number],
            device_id=device(dev_y, dev_z), device_id_type=MESH)
            for number, (slots, source, source_row, target, target_row, dev_y, dev_z) in enumerate(parts)]

    def over(start, stop, body, unroll=False):
        def run(index, carry):
            body(index)
            return carry
        lax.fori_loop(start, stop, run, 0, unroll=unroll)

    def finish_tile(y, tile):
        row = pl.multiple_of(tile * ROWS, ROWS)
        source = buffers[(STEPS - 1) % 2]
        for half in range(2):
            place = (y, pl.ds(row, ROWS), pl.ds(half * LANES, LANES))

            def load(pop_id):
                _, shift_y, shift_z = VELOCITIES[pop_id]
                value = source[SLOT[pop_id], y + 1 - shift_y, half, pl.ds(row + (ROWS - shift_z), ROWS), :]
                stage[(pop_id, *place)] = value
                return value

            density, momentum = moment_sums(load)
            density_ref[place] = density
            for axis in range(3):
                velocity_ref[(axis, *place)] = (momentum[axis] + force[axis]) / density

    def tile_at(position):
        return jnp.where(position % 2 == 0, position // 2, tiles - 1 - position // 2)

    def at_position(position, number, copies):
        @pl.when(position == number)
        def _():
            for copy in copies:
                copy.start()

    all_edges = [edges(step) for step in range(STEPS)]

    def collide_faces(step, tile):
        over(0, 2, lambda index: collide_tile(step, index * (ny - 1), tile), True)

    def collide_inner(step, tile):
        over(1, ny - 1, lambda index: collide_tile(step, index, tile), True)

    def start_faces(step, position, tile):
        at_position(position, 0, all_edges[step][0:2])
        at_position(position, 1, all_edges[step][4:6])
        for copy in faces(step, tile):
            copy.start()

    def start_rows(step, position):
        at_position(position, 0, all_edges[step][2:4])
        at_position(position, 1, all_edges[step][6:7])

    def await_pieces(step, position, tile):
        def await_piece(number):
            for copy in faces(step, number):
                copy.wait_recv()

        @pl.when(position < 2)
        def _():
            await_piece(tile)
        @pl.when(position < tiles - 2)
        def _():
            await_piece(jnp.where(position % 2 == 0, tile + 1, tile - 1))

    def first_faces(position):
        tile = tile_at(position)
        for copy in first_loads(tile):
            copy.wait()
        collide_faces(0, tile)
        @pl.when(position == 0)
        def _():
            @pl.when(jnp.logical_and(me_z != 0, jnp.logical_and(down_z != 0, up_z != 0)))
            def _():
                enter(8, ())
            @pl.when(jnp.logical_and(me_z != 0, down_z == 0))
            def _():
                enter(6, (down_z,))
            @pl.when(jnp.logical_and(me_z != 0, up_z == 0))
            def _():
                enter(6, (up_z,))
        for number, corners in enumerate((all_edges[0][0:2], all_edges[0][4:6])):
            @pl.when(jnp.logical_and(position == number, me_z != 0))
            def _():
                for copy in corners:
                    copy.start()
        for copy in faces(0, tile):
            copy.start()

    def first_inner(position):
        tile = tile_at(position)
        inner_load(tile).wait()
        collide_inner(0, tile)

    split = jnp.where(me_z == 0, tiles // 2, 2)

    def first_part(number):
        early = number < 2 * split
        local = jnp.where(early, number, number - 2 * split)
        length = jnp.where(early, split, tiles - split)
        position = jnp.where(early, 0, split) + jnp.where(local < length, local, local - length)
        @pl.when(local < length)
        def _():
            first_faces(position)
        @pl.when(local >= length)
        def _():
            first_inner(position)
        @pl.when(number == 2 * split - 1)
        def _():
            @pl.when(me_z == 0)
            def _():
                pl.semaphore_wait(barrier, 2)
                for copy in all_edges[0][0:2] + all_edges[0][4:6]:
                    copy.start()
            for copy in all_edges[0][2:4] + all_edges[0][6:7]:
                copy.start()

    @pl.when(me_z == 0)
    def _():
        enter(2, (down_z, up_z))

    over(0, 2 * tiles, first_part)

    for step in range(1, STEPS):
        def place(position):
            tile = tile_at(position)
            await_pieces(step - 1, position, tile)
            @pl.when(position == 0)
            def _():
                for copy in all_edges[step - 1]:
                    copy.wait_recv()
            if step >= 2:
                for copy in faces(step - 2, tile):
                    copy.wait_send()
                @pl.when(position == 0)
                def _():
                    for copy in all_edges[step - 2]:
                        copy.wait_send()
            collide_faces(step, tile)
            start_faces(step, position, tile)
            collide_inner(step, tile)
            start_rows(step, position)

        over(0, tiles, place)

    last = STEPS - 1
    def finish_inner(position):
        @pl.when(position == tiles - 2)
        def _():
            for copy in all_edges[last]:
                copy.wait_recv()
        tile = tile_at(tiles - 1 - position)
        over(1, ny - 1, lambda y: finish_tile(y, tile))

    over(0, tiles, finish_inner)

    def finish_faces(position):
        tile = tile_at(position)
        await_pieces(last, position, tile)
        over(0, 2, lambda index: finish_tile(index * (ny - 1), tile))

    over(0, tiles, finish_faces)

    def await_sends(tile):
        for step in (last - 1, last):
            for copy in faces(step, tile):
                copy.wait_send()

    over(0, tiles, await_sends)
    for step in (last - 1, last):
        for copy in all_edges[step]:
            copy.wait_send()


def output_kernel(final_in, density_in, velocity_in, final_ref, density_ref, velocity_ref, copy_sem):
    copies = []
    for first in range(0, final_in.shape[1], 2):
        planes = pl.ds(first, 2)
        pairs = [(final_in.at[pop_id, planes], final_ref.at[pop_id, planes]) for pop_id in range(19)]
        pairs += [(velocity_in.at[axis, planes], velocity_ref.at[axis, planes]) for axis in range(3)]
        pairs.append((density_in.at[planes], density_ref.at[planes]))
        for source, target in pairs:
            copies.append(pltpu.make_async_copy(source, target, copy_sem.at[len(copies)]))
            copies[-1].start()
    for copy in copies:
        copy.wait()


def solution(mesh):
    size_y = mesh.shape["py"]
    size_z = mesh.shape["pz"]
    field_spec = P(None, None, "py", "pz")

    def local_steps(populations, relax_time, body_force):
        field = jnp.transpose(populations, (0, 2, 3, 1))
        _, ny, nz, nx = field.shape
        tau = jnp.reshape(relax_time, (1,))
        state_shape = (19, ny + 2, 2, nz + 2 * ROWS, LANES)
        vmem = pl.BlockSpec(memory_space=pltpu.VMEM)
        anywhere = pl.BlockSpec(memory_space=pl.ANY)
        results = pl.pallas_call(
            functools.partial(step_kernel, size_y, size_z, ny, nz),
            name="lattice_steps",
            out_shape=(
                pltpu.VMEM((19, ny, nz, nx), jnp.float32),
                pltpu.VMEM((ny, nz, nx), jnp.float32),
                pltpu.VMEM((3, ny, nz, nx), jnp.float32),
            ),
            in_specs=[anywhere, anywhere, anywhere],
            out_specs=(vmem, vmem, vmem),
            scratch_shapes=[
                pltpu.VMEM(state_shape, jnp.float32),
                pltpu.VMEM(state_shape, jnp.float32),
                pltpu.SMEM((1,), jnp.float32),
                pltpu.SMEM((3,), jnp.float32),
                pltpu.SemaphoreType.DMA((2,)),
                pltpu.SemaphoreType.DMA((nz // ROWS,)),
                pltpu.SemaphoreType.DMA((2, nz // ROWS)),
                pltpu.SemaphoreType.DMA((2, 2, nz // ROWS)),
                pltpu.SemaphoreType.DMA((2, 2, nz // ROWS)),
                pltpu.SemaphoreType.DMA((2, EDGE_COPIES)),
                pltpu.SemaphoreType.DMA((2, EDGE_COPIES)),
            ],
            compiler_params=pltpu.CompilerParams(collective_id=0, has_side_effects=True, vmem_limit_bytes=46 * 2**20),
        )(tau, body_force, field)
        final, density, velocity = pl.pallas_call(
            output_kernel,
            name="lattice_output",
            out_shape=tuple(jax.ShapeDtypeStruct(result.shape, result.dtype) for result in results),
            in_specs=[vmem, vmem, vmem],
            out_specs=(anywhere, anywhere, anywhere),
            scratch_shapes=[pltpu.SemaphoreType.DMA((23 * ny // 2,))],
            compiler_params=pltpu.CompilerParams(vmem_limit_bytes=2**20),
        )(*results)
        return jnp.transpose(final, (0, 3, 1, 2)), jnp.transpose(density, (2, 0, 1)), jnp.transpose(velocity, (0, 3, 1, 2))

    return jax.shard_map(local_steps, mesh=mesh, in_specs=(field_spec, P(), P()), out_specs=(field_spec, P(None, "py", "pz"), field_spec), check_vma=False)
```

```python
import functools

import jax
import jax.numpy as jnp
from jax import lax
from jax.experimental import pallas as pl
from jax.experimental.pallas import tpu as pltpu
from jax.sharding import PartitionSpec as P

STEPS = 4
VELOCITIES = ((0, 0, 0), (1, 0, 0), (-1, 0, 0), (0, 1, 0), (0, -1, 0), (0, 0, 1), (0, 0, -1), (1, 1, 0), (-1, -1, 0), (1, -1, 0), (-1, 1, 0), (1, 0, 1), (-1, 0, -1), (1, 0, -1), (-1, 0, 1), (0, 1, 1), (0, -1, -1), (0, 1, -1), (0, -1, 1))
ORDER = (17, 3, 7, 10, 15, 5, 11, 14, 18, 4, 8, 9, 16, 6, 12, 13, 0, 1, 2)
SLOT = {pop_id: slot for slot, pop_id in enumerate(ORDER)}
MESH = pl.DeviceIdType.MESH
LANES = 128
ROWS = 8
EDGE_COPIES = 7


def moment_sums(load):
    rest = load(0)
    total = rest
    diff = {}
    for plus in range(1, 19, 2):
        upper, lower = load(plus), load(plus + 1)
        total = total + (upper + lower)
        diff[plus] = upper - lower
    mom_x = (diff[1] + diff[7]) + (diff[9] + (diff[11] + diff[13]))
    mom_y = (diff[3] + diff[7]) - (diff[9] - (diff[15] + diff[17]))
    mom_z = (diff[5] + diff[11]) - (diff[13] - (diff[15] - diff[17]))
    return total, (mom_x, mom_y, mom_z)


def tile_terms(load, force, rate36):
    density, momentum = moment_sums(load)
    inverse = 1.0 / density
    half = [(momentum[axis] + force[axis]) * inverse * 1.5 for axis in range(3)]
    square = half[0] * half[0] + half[1] * half[1] + half[2] * half[2]
    scale = density * rate36
    even = scale * (1.0 - square * (2.0 / 3.0))
    twice = scale + scale
    odd = [twice * half[axis] for axis in range(3)]
    return even, odd, half


def relaxed(load, terms, keep, plus):
    even, odd, half = terms
    axes = [(axis, shift) for axis, shift in enumerate(VELOCITIES[plus]) if shift != 0]
    if len(axes) == 1:
        axis = axes[0][0]
        odd_part = odd[axis] + odd[axis]
        even_part = (even + even) + odd_part * half[axis]
    else:
        (first, _), (second, sign) = axes
        if sign > 0:
            odd_part = odd[first] + odd[second]
            projection = half[first] + half[second]
        else:
            odd_part = odd[first] - odd[second]
            projection = half[first] - half[second]
        even_part = even + odd_part * projection
    return load(plus) * keep + (even_part + odd_part), load(plus + 1) * keep + (even_part - odd_part)


def rolled(halves, shift, lane):
    if shift == 0:
        return halves
    moved = [pltpu.roll(part, shift % LANES, 1) for part in halves]
    edge = lane == (0 if shift > 0 else LANES - 1)
    return [jnp.where(edge, moved[1], moved[0]), jnp.where(edge, moved[0], moved[1])]


def step_kernel(size_y, size_z, ny, nz, tau_in, force_in, field_ref, stage, density_ref, velocity_ref, buffer_0, buffer_1, tau_ref, force_ref, param_sem, load_sem, first_sem, face_send, face_recv, edge_send, edge_recv):
    me_y, me_z = lax.axis_index("py"), lax.axis_index("pz")
    up_y, down_y = lax.rem(me_y + 1, size_y), lax.rem(me_y + size_y - 1, size_y)
    up_z, down_z = lax.rem(me_z + 1, size_z), lax.rem(me_z + size_z - 1, size_z)

    def device(dev_y, dev_z):
        return {"py": dev_y, "pz": dev_z}

    barrier = pltpu.get_barrier_semaphore()
    beside = [(dev_y, dev_z) for dev_z in (down_z, up_z) for dev_y in (down_y, me_y, up_y)]

    def signal(dev_y, dev_z):
        pl.semaphore_signal(barrier, inc=1, device_id=device(dev_y, dev_z), device_id_type=MESH)

    signal(up_y, me_z)
    signal(down_y, me_z)
    for dev_y, dev_z in beside:
        @pl.when(jnp.logical_and(me_z != 0, dev_z != 0))
        def _():
            signal(dev_y, dev_z)

    def enter(count, targets):
        pl.semaphore_wait(barrier, count)
        for dev_z in targets:
            signal(me_y, dev_z)

    tiles = nz // ROWS
    params = [pltpu.make_async_copy(tau_in, tau_ref, param_sem.at[0]), pltpu.make_async_copy(force_in, force_ref, param_sem.at[1])]
    for copy in params:
        copy.start()

    def first_loads(tile):
        rows = pl.ds(pl.multiple_of(tile * ROWS, ROWS), ROWS)
        return [pltpu.make_async_copy(field_ref.at[:, y, rows], stage.at[:, y, rows], first_sem.at[face, tile]) for face, y in enumerate((0, ny - 1))]

    def inner_load(tile):
        rows = pl.ds(pl.multiple_of(tile * ROWS, ROWS), ROWS)
        planes = pl.ds(1, ny - 2)
        return pltpu.make_async_copy(field_ref.at[:, planes, rows], stage.at[:, planes, rows], load_sem.at[tile])

    order = [position // 2 if position % 2 == 0 else tiles - 1 - position // 2 for position in range(tiles)]
    for positions in (order[:2], order[2:]):
        for tile in positions:
            for copy in first_loads(tile):
                copy.start()
        for tile in positions:
            inner_load(tile).start()
    for copy in params:
        copy.wait()

    tau = jnp.full((ROWS, LANES), tau_ref[0], jnp.float32)
    rate = 1.0 / tau
    keep = 1.0 - rate
    rate36 = rate * (1.0 / 36.0)
    force = [tau * force_ref[axis] for axis in range(3)]
    lane = lax.broadcasted_iota(jnp.int32, (ROWS, LANES), 1)
    buffers = (buffer_0, buffer_1)

    def collide_tile(step, y, tile):
        row = pl.multiple_of(tile * ROWS, ROWS)
        target = buffers[step % 2]
        source = buffers[(step + 1) % 2]

        def load(half, pop_id):
            if step == 0:
                return stage[pop_id, y, pl.ds(row, ROWS), pl.ds(half * LANES, LANES)]
            _, shift_y, shift_z = VELOCITIES[pop_id]
            return source[SLOT[pop_id], y + 1 - shift_y, half, pl.ds(row + (ROWS - shift_z), ROWS), :]

        def store(pop_id, halves):
            halves = rolled(halves, VELOCITIES[pop_id][0], lane)
            for half in range(2):
                target[SLOT[pop_id], y + 1, half, pl.ds(row + ROWS, ROWS), :] = halves[half]

        loaders = [functools.partial(load, half) for half in range(2)]
        terms = [tile_terms(loaders[half], force, rate36) for half in range(2)]
        store(0, [loaders[half](0) * keep + terms[half][0] * 12.0 for half in range(2)])
        for plus in range(1, 19, 2):
            pairs = [relaxed(loaders[half], terms[half], keep, plus) for half in range(2)]
            store(plus, [pair[0] for pair in pairs])
            store(plus + 1, [pair[1] for pair in pairs])

    def faces(step, tile):
        state, parity = buffers[step % 2], step % 2
        rows = pl.ds(pl.multiple_of(tile * ROWS + ROWS, ROWS), ROWS)
        result = []
        for face, (slots, source, target, dev_y) in enumerate(((pl.ds(0, 5), ny, 0, up_y), (pl.ds(8, 5), 1, ny + 1, down_y))):
            result.append(pltpu.make_async_remote_copy(
                src_ref=state.at[slots, source, :, rows, :], dst_ref=state.at[slots, target, :, rows, :],
                send_sem=face_send.at[parity, face, tile], recv_sem=face_recv.at[parity, face, tile],
                device_id=device(dev_y, me_z), device_id_type=MESH))
        return result

    def edges(step):
        state, parity = buffers[step % 2], step % 2
        planes = pl.ds(1, ny)
        low, high, below, above = (pl.ds(row, 1) for row in (ROWS, ROWS + nz - 1, ROWS - 1, ROWS + nz))
        parts = (
            (0, ny, low, 0, above, up_y, down_z),
            (12, 1, low, ny + 1, above, down_y, down_z),
            (pl.ds(12, 4), planes, low, planes, above, me_y, down_z),
            (0, planes, low, planes, above, me_y, down_z),
            (4, ny, high, 0, below, up_y, up_z),
            (8, 1, high, ny + 1, below, down_y, up_z),
            (pl.ds(4, 5), planes, high, planes, below, me_y, up_z),
        )
        return [pltpu.make_async_remote_copy(
            src_ref=state.at[slots, source, :, source_row, :], dst_ref=state.at[slots, target, :, target_row, :],
            send_sem=edge_send.at[parity, number], recv_sem=edge_recv.at[parity, number],
            device_id=device(dev_y, dev_z), device_id_type=MESH)
            for number, (slots, source, source_row, target, target_row, dev_y, dev_z) in enumerate(parts)]

    def over(start, stop, body, unroll=False):
        def run(index, carry):
            body(index)
            return carry
        lax.fori_loop(start, stop, run, 0, unroll=unroll)

    def finish_tile(y, tile):
        row = pl.multiple_of(tile * ROWS, ROWS)
        source = buffers[(STEPS - 1) % 2]
        for half in range(2):
            place = (y, pl.ds(row, ROWS), pl.ds(half * LANES, LANES))

            def load(pop_id):
                _, shift_y, shift_z = VELOCITIES[pop_id]
                value = source[SLOT[pop_id], y + 1 - shift_y, half, pl.ds(row + (ROWS - shift_z), ROWS), :]
                stage[(pop_id, *place)] = value
                return value

            density, momentum = moment_sums(load)
            density_ref[place] = density
            for axis in range(3):
                velocity_ref[(axis, *place)] = (momentum[axis] + force[axis]) / density

    def tile_at(position):
        return jnp.where(position % 2 == 0, position // 2, tiles - 1 - position // 2)

    def at_position(position, number, copies):
        @pl.when(position == number)
        def _():
            for copy in copies:
                copy.start()

    all_edges = [edges(step) for step in range(STEPS)]

    def collide_faces(step, tile):
        over(0, 2, lambda index: collide_tile(step, index * (ny - 1), tile), True)

    def collide_inner(step, tile):
        over(1, ny - 1, lambda index: collide_tile(step, index, tile), True)

    def start_faces(step, position, tile):
        at_position(position, 0, all_edges[step][0:2])
        at_position(position, 1, all_edges[step][4:6])
        for copy in faces(step, tile):
            copy.start()

    def start_rows(step, position):
        at_position(position, 0, all_edges[step][2:4])
        at_position(position, 1, all_edges[step][6:7])

    def await_pieces(step, position, tile):
        def await_piece(number):
            for copy in faces(step, number):
                copy.wait_recv()

        @pl.when(position < 2)
        def _():
            await_piece(tile)
        @pl.when(position < tiles - 2)
        def _():
            await_piece(jnp.where(position % 2 == 0, tile + 1, tile - 1))

    def first_faces(position):
        tile = tile_at(position)
        for copy in first_loads(tile):
            copy.wait()
        collide_faces(0, tile)
        @pl.when(position == 0)
        def _():
            @pl.when(jnp.logical_and(me_z != 0, jnp.logical_and(down_z != 0, up_z != 0)))
            def _():
                enter(8, ())
            @pl.when(jnp.logical_and(me_z != 0, down_z == 0))
            def _():
                enter(6, (down_z,))
            @pl.when(jnp.logical_and(me_z != 0, up_z == 0))
            def _():
                enter(6, (up_z,))
        for number, corners in enumerate((all_edges[0][0:2], all_edges[0][4:6])):
            @pl.when(jnp.logical_and(position == number, me_z != 0))
            def _():
                for copy in corners:
                    copy.start()
        for copy in faces(0, tile):
            copy.start()

    def first_inner(position):
        tile = tile_at(position)
        inner_load(tile).wait()
        collide_inner(0, tile)

    split = jnp.where(me_z == 0, tiles // 2, 2)

    def first_part(number):
        early = number < 2 * split
        local = jnp.where(early, number, number - 2 * split)
        length = jnp.where(early, split, tiles - split)
        position = jnp.where(early, 0, split) + jnp.where(local < length, local, local - length)
        @pl.when(local < length)
        def _():
            first_faces(position)
        @pl.when(local >= length)
        def _():
            first_inner(position)
        @pl.when(number == 2 * split - 1)
        def _():
            @pl.when(me_z == 0)
            def _():
                pl.semaphore_wait(barrier, 2)
                for copy in all_edges[0][0:2] + all_edges[0][4:6]:
                    copy.start()
            for copy in all_edges[0][2:4] + all_edges[0][6:7]:
                copy.start()

    @pl.when(me_z == 0)
    def _():
        enter(2, (down_z, up_z))

    over(0, 2 * tiles, first_part)

    for step in range(1, STEPS):
        def place(position):
            tile = tile_at(position)
            await_pieces(step - 1, position, tile)
            @pl.when(position == 0)
            def _():
                for copy in all_edges[step - 1]:
                    copy.wait_recv()
            if step >= 2:
                for copy in faces(step - 2, tile):
                    copy.wait_send()
                @pl.when(position == 0)
                def _():
                    for copy in all_edges[step - 2]:
                        copy.wait_send()
            collide_faces(step, tile)
            start_faces(step, position, tile)
            collide_inner(step, tile)
            start_rows(step, position)

        over(0, tiles, place)

    last = STEPS - 1
    def finish_inner(position):
        @pl.when(position == tiles - 2)
        def _():
            for copy in all_edges[last]:
                copy.wait_recv()
        tile = tile_at(tiles - 1 - position)
        over(1, ny - 1, lambda y: finish_tile(y, tile))

    over(0, tiles, finish_inner)

    def finish_faces(position):
        tile = tile_at(position)
        await_pieces(last, position, tile)
        over(0, 2, lambda index: finish_tile(index * (ny - 1), tile))

    over(0, tiles, finish_faces)

    def await_sends(tile):
        for step in (last - 1, last):
            for copy in faces(step, tile):
                copy.wait_send()

    over(0, tiles, await_sends)
    for step in (last - 1, last):
        for copy in all_edges[step]:
            copy.wait_send()


def output_kernel(final_in, density_in, velocity_in, final_ref, density_ref, velocity_ref, copy_sem):
    pairs = [(final_in.at[pl.ds(first, count)], final_ref.at[pl.ds(first, count)]) for first, count in ((0, 4), (4, 4), (8, 4), (12, 4), (16, 3))]
    pairs += [(velocity_in, velocity_ref), (density_in, density_ref)]
    copies = [pltpu.make_async_copy(source, target, copy_sem.at[number]) for number, (source, target) in enumerate(pairs)]
    for copy in copies:
        copy.start()
    for copy in copies:
        copy.wait()


def solution(mesh):
    size_y = mesh.shape["py"]
    size_z = mesh.shape["pz"]
    field_spec = P(None, None, "py", "pz")

    def local_steps(populations, relax_time, body_force):
        field = jnp.transpose(populations, (0, 2, 3, 1))
        _, ny, nz, nx = field.shape
        tau = jnp.reshape(relax_time, (1,))
        state_shape = (19, ny + 2, 2, nz + 2 * ROWS, LANES)
        vmem = pl.BlockSpec(memory_space=pltpu.VMEM)
        anywhere = pl.BlockSpec(memory_space=pl.ANY)
        results = pl.pallas_call(
            functools.partial(step_kernel, size_y, size_z, ny, nz),
            name="lattice_steps",
            out_shape=(
                pltpu.VMEM((19, ny, nz, nx), jnp.float32),
                pltpu.VMEM((ny, nz, nx), jnp.float32),
                pltpu.VMEM((3, ny, nz, nx), jnp.float32),
            ),
            in_specs=[anywhere, anywhere, anywhere],
            out_specs=(vmem, vmem, vmem),
            scratch_shapes=[
                pltpu.VMEM(state_shape, jnp.float32),
                pltpu.VMEM(state_shape, jnp.float32),
                pltpu.SMEM((1,), jnp.float32),
                pltpu.SMEM((3,), jnp.float32),
                pltpu.SemaphoreType.DMA((2,)),
                pltpu.SemaphoreType.DMA((nz // ROWS,)),
                pltpu.SemaphoreType.DMA((2, nz // ROWS)),
                pltpu.SemaphoreType.DMA((2, 2, nz // ROWS)),
                pltpu.SemaphoreType.DMA((2, 2, nz // ROWS)),
                pltpu.SemaphoreType.DMA((2, EDGE_COPIES)),
                pltpu.SemaphoreType.DMA((2, EDGE_COPIES)),
            ],
            compiler_params=pltpu.CompilerParams(collective_id=0, has_side_effects=True, vmem_limit_bytes=46 * 2**20),
        )(tau, body_force, field)
        final, density, velocity = pl.pallas_call(
            output_kernel,
            name="lattice_output",
            out_shape=tuple(jax.ShapeDtypeStruct(result.shape, result.dtype) for result in results),
            in_specs=[vmem, vmem, vmem],
            out_specs=(anywhere, anywhere, anywhere),
            scratch_shapes=[pltpu.SemaphoreType.DMA((7,))],
            compiler_params=pltpu.CompilerParams(vmem_limit_bytes=2**20),
        )(*results)
        return jnp.transpose(final, (0, 3, 1, 2)), jnp.transpose(density, (2, 0, 1)), jnp.transpose(velocity, (0, 3, 1, 2))

    return jax.shard_map(local_steps, mesh=mesh, in_specs=(field_spec, P(), P()), out_specs=(field_spec, P(None, "py", "pz"), field_spec), check_vma=False)
```
